8 devices in a mesh: fsdp: 8 (over z, y, x, core).
Axes of the slice: x: 2, y: 2, z: 1, core: 2. Of those that a mesh axis runs over, the one named last changes fastest.
Arguments:
- x_layers: bfloat16 [2, 8, 2048, 768], P(None, 'fsdp')
- dy_top: bfloat16 [8, 2048, 768], P('fsdp')
- x_next: bfloat16 [8, 2048, 768], P('fsdp')
- w_up: bfloat16 [2, 768, 3072], replicated
- w_down: bfloat16 [2, 3072, 768], replicated
- acc_up: float32 [2, 768, 3072], P(None, 'fsdp')
- acc_down: float32 [2, 3072, 768], P(None, 'fsdp')
- master_up: float32 [2, 768, 3072], P(None, 'fsdp')
- master_down: float32 [2, 3072, 768], P(None, 'fsdp')
- mom_up: float32 [2, 768, 3072], P(None, 'fsdp')
- mom_down: float32 [2, 3072, 768], P(None, 'fsdp')
- var_up: float32 [2, 768, 3072], P(None, 'fsdp')
- var_down: float32 [2, 3072, 768], P(None, 'fsdp')
Outputs:
- output 1: float32 [2, 768, 3072], P(None, 'fsdp')
- output 2: float32 [2, 3072, 768], P(None, 'fsdp')
- output 3: float32 [2, 768, 3072], P(None, 'fsdp')
- output 4: float32 [2, 3072, 768], P(None, 'fsdp')
- output 5: float32 [2, 768, 3072], P(None, 'fsdp')
- output 6: float32 [2, 3072, 768], P(None, 'fsdp')
- output 7: bfloat16 [8, 2048, 768], P('fsdp')
All inputs are finite; a program needn't handle non-finite values.
Results may differ from the reference program's by a relative error of at most 0.00889.
Values are sent between devices in bfloat16 or wider.
A program may use at most 1 GiB of HBM per device.

```python
import jax
import jax.numpy as jnp
from jax import lax

D = 768
FF = 3072
LAYERS = 2
GROUP_SIZE = 8
BATCH_DEV = 1
SEQ_LEN = 2048
MICRO_STEPS = 2
STEP_COUNT = 3

BETA_MOM = 0.9
BETA_VAR = 0.999
ADAM_EPS = 1e-6
WEIGHT_DECAY = 0.01
LEARN_RATE = 0.06

BATCH = GROUP_SIZE * BATCH_DEV


def row_profile(rng_key, row_count):
    increments = jax.random.normal(rng_key, (LAYERS, row_count, 1), jnp.float32)
    log_scale = jnp.cumsum(increments, axis=1) * row_count ** -0.5
    scales = jnp.exp(log_scale)
    return scales / jnp.sqrt(jnp.mean(scales * scales, axis=1, keepdims=True))


def setup_inputs(seed: int = 0) -> dict:
    key_list = jax.random.split(jax.random.key(seed), 16)
    tok_count = BATCH * SEQ_LEN
    tok_shape = (BATCH, SEQ_LEN, D)
    up_shape = (LAYERS, D, FF)
    down_shape = (LAYERS, FF, D)
    x_layers = jax.random.normal(key_list[0], (LAYERS,) + tok_shape, jnp.float32)
    dy_top = jax.random.normal(key_list[1], tok_shape, jnp.float32) * tok_count ** -0.5
    x_next = jax.random.normal(key_list[2], tok_shape, jnp.float32)
    master_up = jax.random.normal(key_list[3], up_shape, jnp.float32) * row_profile(key_list[4], D) * D ** -0.5
    master_down = jax.random.normal(key_list[5], down_shape, jnp.float32) * row_profile(key_list[6], FF) * FF ** -0.5
    acc_up = 0.6 * jax.random.normal(key_list[7], up_shape, jnp.float32)
    acc_down = 0.6 * jax.random.normal(key_list[8], down_shape, jnp.float32)
    mom_up = 0.08 * jax.random.normal(key_list[9], up_shape, jnp.float32)
    mom_down = 0.08 * jax.random.normal(key_list[10], down_shape, jnp.float32)
    sq_up = jnp.sum(jnp.square(jax.random.normal(key_list[11], (2,) + up_shape, jnp.float32)), axis=0)
    sq_down = jnp.sum(jnp.square(jax.random.normal(key_list[12], (2,) + down_shape, jnp.float32)), axis=0)
    var_up = 0.0003 * (0.5 + sq_up)
    var_down = 0.0003 * (0.5 + sq_down)
    return {
        'x_layers': x_layers.astype(jnp.bfloat16),
        'dy_top': dy_top.astype(jnp.bfloat16),
        'x_next': x_next.astype(jnp.bfloat16),
        'w_up': master_up.astype(jnp.bfloat16),
        'w_down': master_down.astype(jnp.bfloat16),
        'acc_up': acc_up,
        'acc_down': acc_down,
        'master_up': master_up,
        'master_down': master_down,
        'mom_up': mom_up,
        'mom_down': mom_down,
        'var_up': var_up,
        'var_down': var_down,
    }


def lamb_step(grad_sum, acc_prev, master, mom_prev, var_prev):
    grad_full = (acc_prev + grad_sum) / MICRO_STEPS
    mom_new = BETA_MOM * mom_prev + (1.0 - BETA_MOM) * grad_full
    var_new = BETA_VAR * var_prev + (1.0 - BETA_VAR) * grad_full * grad_full
    update = (mom_new / (1.0 - BETA_MOM ** STEP_COUNT)) / (jnp.sqrt(var_new / (1.0 - BETA_VAR ** STEP_COUNT)) + ADAM_EPS) + WEIGHT_DECAY * master
    w_norm = jnp.sqrt(jnp.sum(master * master, axis=(1, 2), keepdims=True))
    u_norm = jnp.sqrt(jnp.sum(update * update, axis=(1, 2), keepdims=True))
    return master - LEARN_RATE * (w_norm / u_norm) * update, mom_new, var_new


def reference(x_layers, dy_top, x_next, w_up, w_down, acc_up, acc_down, master_up, master_down, mom_up, mom_down, var_up, var_down):
    x_dev = jnp.moveaxis(x_layers, 0, 1).reshape(GROUP_SIZE, BATCH_DEV, LAYERS, SEQ_LEN, D)
    dy_dev = dy_top.reshape(GROUP_SIZE, BATCH_DEV, SEQ_LEN, D)
    zero_init = (jnp.zeros((LAYERS, D, FF), jnp.float32), jnp.zeros((LAYERS, FF, D), jnp.float32))

    def seq_grads(carry_sum, seq_item):
        x_seq, d_cur = seq_item
        grads_up = [None] * LAYERS
        grads_down = [None] * LAYERS
        for layer_id in reversed(range(LAYERS)):
            x_cur = x_seq[layer_id]
            pre_act = jnp.dot(x_cur, w_up[layer_id], preferred_element_type=jnp.float32)
            act_f32, gelu_vjp = jax.vjp(jax.nn.gelu, pre_act)
            act_bf = act_f32.astype(jnp.bfloat16)
            d_act = jnp.dot(d_cur, w_down[layer_id].T, preferred_element_type=jnp.float32)
            d_pre = gelu_vjp(d_act)[0].astype(jnp.bfloat16)
            grads_down[layer_id] = jnp.dot(act_bf.T, d_cur, preferred_element_type=jnp.float32)
            grads_up[layer_id] = jnp.dot(x_cur.T, d_pre, preferred_element_type=jnp.float32)
            if layer_id > 0:
                d_cur = (d_cur.astype(jnp.float32) + jnp.dot(d_pre, w_up[layer_id].T, preferred_element_type=jnp.float32)).astype(jnp.bfloat16)
        return (carry_sum[0] + jnp.stack(grads_up), carry_sum[1] + jnp.stack(grads_down)), None

    def device_grads(carry_sum, dev_item):
        part_sum, _ = lax.scan(seq_grads, zero_init, dev_item)
        return (carry_sum[0] + part_sum[0].astype(jnp.bfloat16).astype(jnp.float32), carry_sum[1] + part_sum[1].astype(jnp.bfloat16).astype(jnp.float32)), None

    grad_total, _ = lax.scan(device_grads, zero_init, (x_dev, dy_dev))
    up_new, up_mom, up_var = lamb_step(grad_total[0], acc_up, master_up, mom_up, var_up)
    down_new, down_mom, down_var = lamb_step(grad_total[1], acc_down, master_down, mom_down, var_down)
    w_up_new = up_new.astype(jnp.bfloat16)
    w_down_new = down_new.astype(jnp.bfloat16)

    def forward_seq(x_seq):
        for layer_id in range(LAYERS):
            pre_act = jnp.dot(x_seq, w_up_new[layer_id], preferred_element_type=jnp.float32)
            act_bf = jax.nn.gelu(pre_act).astype(jnp.bfloat16)
            mlp_out = jnp.dot(act_bf, w_down_new[layer_id], preferred_element_type=jnp.float32)
            x_seq = (x_seq.astype(jnp.float32) + mlp_out).astype(jnp.bfloat16)
        return x_seq

    x_out = lax.map(forward_seq, x_next)
    return (up_new, down_new, up_mom, down_mom, up_var, down_var, x_out)
```

```python
import functools

import jax
import jax.numpy as jnp
from jax import lax
from jax.experimental import pallas as pl
from jax.experimental.pallas import tpu as pltpu
from jax.sharding import PartitionSpec as P

MICRO_STEPS = 2
STEP_COUNT = 3
BETA_MOM = 0.9
BETA_VAR = 0.999
ADAM_EPS = 1e-6
WEIGHT_DECAY = 0.01
LEARN_RATE = 0.06

C0 = 0.7978845608028654
C1 = C0 * 0.044715
MESH = pl.DeviceIdType.MESH
BF16 = jnp.bfloat16
F32 = jnp.float32
VMEM_MAX = 67043328

TOK = 2048
D = 768
FF = 3072
SUB = 128
CH = 8 * SUB
TT = 256
NT_DIMS = (((1,), (1,)), ((), ()))
NN_DIMS = (((1,), (0,)), ((), ()))


def position():
    me = lax.axis_index('fsdp')
    y, x, c = me // 4, (me // 2) % 2, me % 2
    return me, y, x, c, me + 1 - 2 * c, me + 2 - 4 * x, me + 4 - 8 * y


def entry_barrier(targets):
    barrier = pltpu.get_barrier_semaphore()
    for dev in targets:
        pl.semaphore_signal(barrier, inc=1, device_id=(dev,), device_id_type=MESH)
    pl.semaphore_wait(barrier, len(targets))


def dot(a, b, dims=NN_DIMS):
    return lax.dot_general(a, b, dims, preferred_element_type=F32)


def backward_kernel(x_hbm, dy_hbm, w1_hbm, w2_hbm, g1_ref, g2_ref,
                    xb, dyb, xt, dxacc, w1b, w2b, at, dhb, p1, p2, r01, r02, r1a1, r1b1, r1a2, r1b2, r2a1, r2b1, r2a2, r2b2,
                    ld_sem, w_sem, snd, rcv):
    me, y, x, c, partner, xn, yn = position()

    def w_copies(g, slot):
        layer = 1 - g // 3
        k = g % 3
        out = []
        for cc in range(2):
            for q in range(4):
                i = cc * 4 + q
                f0 = pl.multiple_of((2 * q + cc) * 384 + k * SUB, SUB)
                out.append(pltpu.make_async_copy(w1_hbm.at[layer, :, pl.ds(f0, SUB)], w1b.at[slot, :, pl.ds(i * SUB, SUB)], w_sem.at[slot, i]))
                out.append(pltpu.make_async_copy(w2_hbm.at[layer, pl.ds(f0, SUB), :], w2b.at[slot, pl.ds(i * SUB, SUB), :], w_sem.at[slot, 8 + i]))
        return out

    loads = [pltpu.make_async_copy(x_hbm.at[1], xb.at[1], ld_sem.at[0]),
             pltpu.make_async_copy(dy_hbm, dyb, ld_sem.at[1]),
             pltpu.make_async_copy(x_hbm.at[0], xb.at[0], ld_sem.at[2])]
    for cp in loads[:2]:
        cp.start()
    for cp in w_copies(0, 0):
        cp.start()
    loads[2].start()

    entry_barrier((partner, xn, yn))

    units = ((p1, r01, r1a1, r1b1, r2a1, r2b1, 48), (p2, r02, r1a2, r1b2, r2a2, r2b2, 64))

    def remote(src, dst, u, slot, stage, dev):
        return pltpu.make_async_remote_copy(src_ref=src, dst_ref=dst, send_sem=snd.at[u, slot, stage], recv_sem=rcv.at[u, slot, stage], device_id=(dev,), device_id_type=MESH)

    def s0(u, slot):
        p, r0, r1a, r1b, r2a, r2b, hr = units[u]
        return remote(p.at[slot, 1 - c], r0.at[slot], u, slot, 0, partner)

    def s1(u, slot):
        p, r0, r1a, r1b, r2a, r2b, hr = units[u]
        return (remote(p.at[slot, c, :, 1 - x, pl.ds(0, hr)], r1a.at[slot], u, slot, 1, xn),
                remote(p.at[slot, c, 1 - y, :, pl.ds(hr, hr)], r1b.at[slot], u, slot, 2, yn))

    def s2(u, slot):
        p, r0, r1a, r1b, r2a, r2b, hr = units[u]
        return (remote(p.at[slot, c, 1 - y, x, pl.ds(0, hr)], r2a.at[slot], u, slot, 3, yn),
                remote(p.at[slot, c, y, 1 - x, pl.ds(hr, hr)], r2b.at[slot], u, slot, 4, xn))

    def start_s0(u, slot):
        s0(u, slot).start()

    def to_s1(u, slot):
        p, r0, r1a, r1b, r2a, r2b, hr = units[u]
        s0(u, slot).wait()

        @pl.loop(0, 2)
        def _(yy):
            for xx in range(2):
                p[slot, c, yy, xx] = (p[slot, c, yy, xx].astype(F32) + r0[slot, yy, xx].astype(F32)).astype(BF16)

        for cp in s1(u, slot):
            cp.start()

    def to_s2(u, slot):
        p, r0, r1a, r1b, r2a, r2b, hr = units[u]
        ca, cb = s1(u, slot)
        ca.wait()
        for i in range(2):
            p[slot, c, i, x, 0:hr] = (p[slot, c, i, x, 0:hr].astype(F32) + r1a[slot, i].astype(F32)).astype(BF16)
        cb.wait()
        for i in range(2):
            p[slot, c, y, i, hr:2 * hr] = (p[slot, c, y, i, hr:2 * hr].astype(F32) + r1b[slot, i].astype(F32)).astype(BF16)
        for cp in s2(u, slot):
            cp.start()

    def finish(u, slot, g):
        p, r0, r1a, r1b, r2a, r2b, hr = units[u]
        layer = 1 - g // 3
        k = g % 3
        ca, cb = s2(u, slot)
        for half, (cp, r2) in enumerate(((ca, r2a), (cb, r2b))):
            cp.wait()
            rows = slice(half * hr, half * hr + hr)
            total = p[slot, c, y, x, rows].astype(F32) + r2[slot].astype(F32)
            if u == 1:
                g2_ref[layer, pl.ds(pl.multiple_of(k * SUB + half * hr, 64), hr), :] = total
            else:
                for cc in range(2):
                    for q in range(4):
                        i = cc * 4 + q
                        f0 = pl.multiple_of((2 * q + cc) * 384 + k * SUB, SUB)
                        g1_ref[layer, rows, pl.ds(f0, SUB)] = total[:, i * SUB:(i + 1) * SUB]

    loads[0].wait()
    loads[1].wait()

    @pl.loop(0, 6)
    def _(g):
        slot = g % 2
        prev = 1 - slot
        layer = 1 - g // 3
        k = g % 3
        for cp in w_copies(g, slot):
            cp.wait()

        @pl.when(g < 5)
        def _():
            for cp in w_copies(g + 1, prev):
                cp.start()

        @pl.when(g == 3)
        def _():
            loads[2].wait()

        @pl.loop(0, TOK // TT)
        def _(t):
            @pl.when((g > 0) & (t == 2))
            def _():
                to_s1(0, prev)

            @pl.when((g > 0) & (t == 5))
            def _():
                to_s2(1, prev)

            rows = pl.ds(pl.multiple_of(t * TT, TT), TT)
            xv = xb[layer, rows, :]
            dyv = dyb[rows, :]
            xt[:, rows] = xv.T
            for n in range(CH // 256):
                cs = slice(n * 256, n * 256 + 256)
                h = dot(xv, w1b[slot, :, cs])
                da = dot(dyv, w2b[slot, cs, :], NT_DIMS)
                sq = h * h
                s = 0.5 * jnp.tanh(h * (C0 + C1 * sq)) + 0.5
                a = h * s
                gp = s + a * (1.0 - s) * (2.0 * C0 + (6.0 * C1) * sq)
                at[cs, rows] = a.astype(BF16).T
                dhb[rows, cs] = (da * gp).astype(BF16)

            @pl.when(layer == 1)
            def _():
                base = jnp.where(k > 0, dxacc[rows, :], dyv.astype(F32))
                dxacc[rows, :] = base + dot(dhb[rows, :], w1b[slot], NT_DIMS)

        @pl.when(g > 0)
        def _():
            to_s2(0, prev)

        @pl.loop(0, CH // 256)
        def _(n):
            fs = pl.ds(pl.multiple_of(n * 256, 256), 256)
            res = dot(at[fs, :], dyb[...]).astype(BF16)
            p2[slot, n // 2, n % 2] = res.reshape(2, SUB, D)

        start_s0(1, slot)

        @pl.when(g > 0)
        def _():
            finish(1, prev, g - 1)

        @pl.loop(0, CH // 256)
        def _(n):
            fs = pl.ds(pl.multiple_of(n * 256, 256), 256)
            res = dot(xt[...], dhb[:, fs]).astype(BF16)
            for b in range(8):
                p1[slot, b % 2, b // 4, (b // 2) % 2, :, fs] = res[b * 96:(b + 1) * 96]

        to_s1(1, slot)
        start_s0(0, slot)

        @pl.when(g > 0)
        def _():
            finish(0, prev, g - 1)

        @pl.when(g == 2)
        def _():
            @pl.loop(0, TOK // TT)
            def _(t):
                rows = pl.ds(pl.multiple_of(t * TT, TT), TT)
                dyb[rows, :] = dxacc[rows, :].astype(BF16)

    to_s1(0, 1)
    to_s2(1, 1)
    to_s2(0, 1)
    finish(1, 1, 5)
    finish(0, 1, 5)


def run_backward(x, dy, w1, w2):
    any_spec = pl.BlockSpec(memory_space=pl.ANY)
    vm = pltpu.VMEM
    return pl.pallas_call(
        backward_kernel,
        out_shape=(jax.ShapeDtypeStruct((2, 96, FF), F32), jax.ShapeDtypeStruct((2, 384, D), F32)),
        in_specs=[any_spec] * 4,
        out_specs=(pl.BlockSpec(memory_space=vm),) * 2,
        scratch_shapes=[
            vm((2, TOK, D), BF16), vm((TOK, D), BF16), vm((D, TOK), BF16), vm((TOK, D), F32),
            vm((2, D, CH), BF16), vm((2, CH, D), BF16), vm((CH, TOK), BF16), vm((TOK, CH), BF16),
            vm((2, 2, 2, 2, 96, CH), BF16), vm((2, 2, 2, 2, SUB, D), BF16),
            vm((2, 2, 2, 96, CH), BF16), vm((2, 2, 2, SUB, D), BF16),
            vm((2, 2, 48, CH), BF16), vm((2, 2, 48, CH), BF16), vm((2, 2, 64, D), BF16), vm((2, 2, 64, D), BF16),
            vm((2, 48, CH), BF16), vm((2, 48, CH), BF16), vm((2, 64, D), BF16), vm((2, 64, D), BF16),
            pltpu.SemaphoreType.DMA((3,)), pltpu.SemaphoreType.DMA((2, 16)),
            pltpu.SemaphoreType.DMA((2, 2, 5)), pltpu.SemaphoreType.DMA((2, 2, 5)),
        ],
        compiler_params=pltpu.CompilerParams(collective_id=0, has_side_effects=True, vmem_limit_bytes=VMEM_MAX),
        name='backward',
    )(x, dy, w1, w2)


def moments_kernel(g1, a1, w1, m1, v1, g2, a2, w2, m2, v2, m1o, v1o, u1o, m2o, v2o, u2o, sq):
    first = pl.program_id(1) == 0

    @pl.when(first)
    def _():
        sq[...] = jnp.zeros_like(sq)

    def part(kind, g, acc, w, m, v, mo, vo, uo):
        grad = (acc[0] + g[0]) / MICRO_STEPS
        master = w[0]
        mom = BETA_MOM * m[0] + (1.0 - BETA_MOM) * grad
        var = BETA_VAR * v[0] + (1.0 - BETA_VAR) * grad * grad
        upd = (mom / (1.0 - BETA_MOM ** STEP_COUNT)) / (jnp.sqrt(var / (1.0 - BETA_VAR ** STEP_COUNT)) + ADAM_EPS) + WEIGHT_DECAY * master
        mo[0] = mom
        vo[0] = var
        uo[0] = upd
        for i, val in enumerate((master, upd)):
            folded = jnp.sum((val * val).reshape(-1, 8, val.shape[-1]), axis=0)
            lanes = folded[:, 0:128]
            for j in range(1, val.shape[-1] // 128):
                lanes = lanes + folded[:, j * 128:(j + 1) * 128]
            sq[0, kind * 2 + i] += lanes

    part(0, g1, a1, w1, m1, v1, m1o, v1o, u1o)
    part(1, g2, a2, w2, m2, v2, m2o, v2o, u2o)


def run_moments(g1, a1, w1, m1, v1, g2, a2, w2, m2, v2):
    up = pl.BlockSpec((1, 96, 768), lambda l, j: (l, 0, j))
    down = pl.BlockSpec((1, 96, 768), lambda l, j: (l, j, 0))
    s1 = jax.ShapeDtypeStruct((2, 96, FF), F32)
    s2 = jax.ShapeDtypeStruct((2, 384, D), F32)
    return pl.pallas_call(
        moments_kernel,
        grid=(2, 4),
        out_shape=(s1, s1, s1, s2, s2, s2, jax.ShapeDtypeStruct((2, 4, 8, 128), F32)),
        in_specs=[up] * 5 + [down] * 5,
        out_specs=(up, up, up, down, down, down, pl.BlockSpec((1, 4, 8, 128), lambda l, j: (l, 0, 0, 0))),
        name='moments',
    )(g1, a1, w1, m1, v1, g2, a2, w2, m2, v2)


def sums_kernel(sq_ref, out_ref, mine, got, snd, rcv):
    me = position()[0]
    mine[...] = jnp.sum(sq_ref[...], axis=1)
    others = [lax.rem(me + i, 8) for i in range(1, 8)]
    entry_barrier(others)
    copies = []
    for i, dev in enumerate(others):
        copies.append(pltpu.make_async_remote_copy(src_ref=mine, dst_ref=got.at[i], send_sem=snd.at[i], recv_sem=rcv.at[i], device_id=(dev,), device_id_type=MESH))
        copies[-1].start()
    got[7] = mine[...]
    for cp in copies:
        cp.wait()
    total = got[lax.rem(me + 7, 8)]
    for dev in range(1, 8):
        total = total + got[lax.rem(me + 7 - dev + 8, 8)]
    out_ref[...] = jnp.broadcast_to(jnp.sum(total, axis=1, keepdims=True), (8, 128))


def run_sums(sq):
    vmem = pl.BlockSpec(memory_space=pltpu.VMEM)
    return pl.pallas_call(
        sums_kernel,
        out_shape=jax.ShapeDtypeStruct((8, 128), F32),
        in_specs=[vmem],
        out_specs=vmem,
        scratch_shapes=[pltpu.VMEM((8, 128), F32), pltpu.VMEM((8, 8, 128), F32), pltpu.SemaphoreType.DMA((7,)), pltpu.SemaphoreType.DMA((7,))],
        compiler_params=pltpu.CompilerParams(collective_id=1, has_side_effects=True),
        name='sums',
    )(sq.reshape(8, 8, 128))


def forward_kernel(w1_hbm, w2_hbm, x_hbm, o_ref, wf1, wf2, ab, xb, ld_sem, snd, rcv):
    me, y, x, c, partner, xn, yn = position()
    fulls = (wf1.at[0], wf2.at[0], wf1.at[1], wf2.at[1])
    halves = (48, 192, 48, 192)
    srcs = (w1_hbm.at[0], w2_hbm.at[0], w1_hbm.at[1], w2_hbm.at[1])
    loads = [pltpu.make_async_copy(srcs[m], fulls[m].at[y, x, c], ld_sem.at[m]) for m in range(4)]
    loads.append(pltpu.make_async_copy(x_hbm, xb, ld_sem.at[4]))
    for cp in loads:
        cp.start()
    entry_barrier((partner, xn, yn))

    def same(ref, m, i, dev):
        return pltpu.make_async_remote_copy(src_ref=ref, dst_ref=ref, send_sem=snd.at[m, i], recv_sem=rcv.at[m, i], device_id=(dev,), device_id_type=MESH)

    def parts(m, name):
        f, h = fulls[m], halves[m]
        lo, hi = pl.ds(0, h), pl.ds(h, h)
        if name == 's1':
            return same(f.at[y, x, c, lo], m, 0, xn), same(f.at[y, x, c, hi], m, 1, yn)
        if name == 's2':
            return same(f.at[y, :, c, lo], m, 2, yn), same(f.at[:, x, c, hi], m, 3, xn)
        if name == 'd1':
            return (same(f.at[y, x, c], m, 4, partner),)
        if name == 'd2':
            return same(f.at[y, 1 - x, c, lo], m, 5, partner), same(f.at[1 - y, x, c, hi], m, 6, partner)
        return same(f.at[1 - y, :, c, lo], m, 7, partner), same(f.at[:, 1 - x, c, hi], m, 8, partner)

    def start(m, *names):
        for name in names:
            for cp in parts(m, name):
                cp.start()

    def wait(m, *names):
        for name in names:
            for cp in parts(m, name):
                cp.wait()

    def first(m):
        start(m, 's1', 'd1')

    def second(m):
        wait(m, 's1')
        start(m, 's2', 'd2')

    def third(m):
        wait(m, 's2')
        start(m, 'd3')

    def done(m):
        wait(m, 'd1', 'd2', 'd3')

    def up(layer, hook):
        @pl.loop(0, TOK // TT)
        def _(t):
            hook(t)
            rows = pl.ds(pl.multiple_of(t * TT, TT), TT)
            xv = xb[rows, :]
            for n in range(4):
                cs = slice(n * 768, n * 768 + 768)
                h = dot(xv, wf1[layer, :, :, :, :, cs].reshape(D, 768))
                s = 0.5 * jnp.tanh(h * (C0 + C1 * (h * h))) + 0.5
                ab[rows, cs] = (h * s).astype(BF16)

    def down(layer, hook):
        @pl.loop(0, TOK // TT)
        def _(t):
            hook(t)
            rows = pl.ds(pl.multiple_of(t * TT, TT), TT)
            res = xb[rows, :].astype(F32) + dot(ab[rows, :], wf2[layer].reshape(FF, D))
            if layer == 0:
                xb[rows, :] = res.astype(BF16)
            else:
                o_ref[rows, :] = res.astype(BF16)

    def no_hook(t):
        pass

    def at_step(step, fn):
        def hook(t):
            @pl.when(t == step)
            def _():
                fn()
        return hook

    def second_and_next(m):
        def fn():
            second(m)
            if m < 3:
                first(m + 1)
        return fn

    loads[0].wait()
    first(0)
    for cp in loads[1:]:
        cp.wait()
    second_and_next(0)()
    third(0)
    second_and_next(1)()
    done(0)
    up(0, no_hook)
    third(1)
    done(1)
    down(0, at_step(3, second_and_next(2)))
    third(2)
    second_and_next(3)()
    done(2)
    up(1, no_hook)
    third(3)
    done(3)
    down(1, no_hook)


def run_forward(w1, w2, x):
    any_spec = pl.BlockSpec(memory_space=pl.ANY)
    vm = pltpu.VMEM
    return pl.pallas_call(
        forward_kernel,
        out_shape=jax.ShapeDtypeStruct((TOK, D), BF16),
        in_specs=[any_spec] * 3,
        out_specs=pl.BlockSpec(memory_space=vm),
        scratch_shapes=[
            vm((2, 2, 2, 2, 96, FF), BF16), vm((2, 2, 2, 2, 384, D), BF16), vm((TOK, FF), BF16), vm((TOK, D), BF16),
            pltpu.SemaphoreType.DMA((5,)), pltpu.SemaphoreType.DMA((4, 9)), pltpu.SemaphoreType.DMA((4, 9)),
        ],
        compiler_params=pltpu.CompilerParams(collective_id=2, has_side_effects=True, vmem_limit_bytes=VMEM_MAX),
        name='forward',
    )(w1, w2, x)


def solution(mesh):
    shard_rows = P(None, 'fsdp')
    shard_batch = P('fsdp')
    spec_whole = P()

    def local_step(x_layers, dy_top, x_next, w_up, w_down, acc_up, acc_down, master_up, master_down, mom_up, mom_down, var_up, var_down):
        g1, g2 = run_backward(x_layers.reshape(2, TOK, D), dy_top.reshape(TOK, D), w_up, w_down)
        m1, v1, u1, m2, v2, u2, sq = run_moments(g1, acc_up, master_up, mom_up, var_up, g2, acc_down, master_down, mom_down, var_down)
        tot = run_sums(sq)[:, 0].reshape(2, 4)
        ratio = LEARN_RATE * jnp.sqrt(tot[:, 0::2] / tot[:, 1::2])
        up_new = master_up - ratio[:, 0][:, None, None] * u1
        down_new = master_down - ratio[:, 1][:, None, None] * u2
        out = run_forward(up_new.astype(BF16), down_new.astype(BF16), x_next.reshape(TOK, D))
        return up_new, down_new, m1, m2, v1, v2, out.reshape(1, TOK, D)

    return jax.shard_map(local_step, mesh=mesh, in_specs=(shard_rows, shard_batch, shard_batch, spec_whole, spec_whole) + (shard_rows,) * 8, out_specs=(shard_rows,) * 6 + (shard_batch,), check_vma=False)
```

```python
import functools

import jax
import jax.numpy as jnp
from jax import lax
from jax.experimental import pallas as pl
from jax.experimental.pallas import tpu as pltpu
from jax.sharding import PartitionSpec as P

MICRO_STEPS = 2
STEP_COUNT = 3
BETA_MOM = 0.9
BETA_VAR = 0.999
ADAM_EPS = 1e-6
WEIGHT_DECAY = 0.01
LEARN_RATE = 0.06

C0 = 0.7978845608028654
C1 = C0 * 0.044715
MESH = pl.DeviceIdType.MESH
BF16 = jnp.bfloat16
F32 = jnp.float32
VMEM_MAX = 67043328

TOK = 2048
D = 768
FF = 3072
SUB = 128
CH = 8 * SUB
TT = 256
NT_DIMS = (((1,), (1,)), ((), ()))
NN_DIMS = (((1,), (0,)), ((), ()))


def position():
    me = lax.axis_index('fsdp')
    y, x, c = me // 4, (me // 2) % 2, me % 2
    return me, y, x, c, me + 1 - 2 * c, me + 2 - 4 * x, me + 4 - 8 * y


def entry_barrier(targets):
    barrier = pltpu.get_barrier_semaphore()
    for dev in targets:
        pl.semaphore_signal(barrier, inc=1, device_id=(dev,), device_id_type=MESH)
    pl.semaphore_wait(barrier, len(targets))


def dot(a, b, dims=NN_DIMS):
    return lax.dot_general(a, b, dims, preferred_element_type=F32)


def moments(grad_sum, acc, master, mom_prev, var_prev):
    grad = (acc + grad_sum) / MICRO_STEPS
    mom = BETA_MOM * mom_prev + (1.0 - BETA_MOM) * grad
    var = BETA_VAR * var_prev + (1.0 - BETA_VAR) * grad * grad
    upd = (mom / (1.0 - BETA_MOM ** STEP_COUNT)) / (jnp.sqrt(var / (1.0 - BETA_VAR ** STEP_COUNT)) + ADAM_EPS) + WEIGHT_DECAY * master
    return mom, var, upd


def backward_kernel(x_hbm, dy_hbm, w1_hbm, w2_hbm, acc1, acc2, mas1, mas2, mom1, mom2, var1, var2,
                    g1_ref, g2_ref, tot_ref, ws1, ws2, wg1,
                    xb, dyb, xt, dxacc, w1b, w2b, at, dhb, p1, p2, r01, r02, r1a1, r1b1, r1a2, r1b2, r2a1, r2b1, r2a2, r2b2,
                    mb, sqb, smine, sgot,
                    ld_sem, w_sem, snd, rcv, l_sem, x_snd, x_rcv, a_snd, a_rcv):
    me, y, x, c, partner, xn, yn = position()
    others = [lax.rem(me + i, 8) for i in range(1, 8)]

    def w_copies(g, slot):
        layer = 1 - g // 3
        k = g % 3
        out = []
        for cc in range(2):
            for q in range(4):
                i = cc * 4 + q
                f0 = pl.multiple_of((2 * q + cc) * 384 + k * SUB, SUB)
                out.append(pltpu.make_async_copy(w1_hbm.at[layer, :, pl.ds(f0, SUB)], w1b.at[slot, :, pl.ds(i * SUB, SUB)], w_sem.at[slot, i]))
                out.append(pltpu.make_async_copy(w2_hbm.at[layer, pl.ds(f0, SUB), :], w2b.at[slot, pl.ds(i * SUB, SUB), :], w_sem.at[slot, 8 + i]))
        return out

    loads = [pltpu.make_async_copy(x_hbm.at[1], xb.at[1], ld_sem.at[0]),
             pltpu.make_async_copy(dy_hbm, dyb, ld_sem.at[1]),
             pltpu.make_async_copy(x_hbm.at[0], xb.at[0], ld_sem.at[2])]
    for cp in loads[:2]:
        cp.start()
    for cp in w_copies(0, 0):
        cp.start()
    loads[2].start()

    sqb[...] = jnp.zeros_like(sqb)
    smine[...] = jnp.zeros_like(smine)
    entry_barrier(others)

    def lamb_loads(layer):
        out = []
        for a, (up, down) in enumerate(((acc1, acc2), (mom1, mom2), (var1, var2), (mas1, mas2))):
            for j in range(8):
                src = up.at[layer, :, pl.ds(j * 768, 768)] if j < 4 else down.at[layer, pl.ds((j - 4) * 96, 96), :]
                dst = dxacc.at[pl.ds((a * 8 + j) * 96, 96), :] if a < 3 else mb.at[pl.ds(j * 96, 96), :]
                out.append(pltpu.make_async_copy(src, dst, l_sem.at[a * 8 + j]))
        return out

    def lamb_moments(layer):
        for cp in lamb_loads(layer):
            cp.wait()
        for kind in range(2):
            @pl.loop(0, 4)
            def _(j):
                spans = [pl.ds(pl.multiple_of((a * 8 + kind * 4 + j) * 96, 96), 96) for a in range(3)]
                grad_sum = g1_ref[layer, :, pl.ds(pl.multiple_of(j * 768, 768), 768)] if kind == 0 else g2_ref[layer, pl.ds(pl.multiple_of(j * 96, 96), 96), :]
                master = mb[spans[0], :] if kind == 0 else mb[pl.ds(pl.multiple_of((4 + j) * 96, 96), 96), :]
                upd = moments(grad_sum, dxacc[spans[0], :], master, dxacc[spans[1], :], dxacc[spans[2], :])[2]
                dxacc[spans[0], :] = upd
                for i, val in enumerate((master, upd)):
                    folded = jnp.sum((val * val).reshape(12, 8, 768), axis=0)
                    lanes = folded[:, 0:128]
                    for b in range(1, 6):
                        lanes = lanes + folded[:, b * 128:(b + 1) * 128]
                    sqb[layer, kind * 2 + i] += lanes

    def lamb_copies(layer):
        return [pltpu.make_async_remote_copy(src_ref=smine.at[layer], dst_ref=sgot.at[layer, i], send_sem=x_snd.at[layer, i], recv_sem=x_rcv.at[layer, i], device_id=(dev,), device_id_type=MESH) for i, dev in enumerate(others)]

    def lamb_send(layer):
        for i in range(4):
            smine[layer, i:i + 1, :] = jnp.sum(sqb[layer, i], axis=0, keepdims=True)
        for cp in lamb_copies(layer):
            cp.start()

    def lamb_apply(layer):
        sgot[layer, 7] = smine[layer]
        for cp in lamb_copies(layer):
            cp.wait()
        total = sgot[layer, lax.rem(me + 7, 8)]
        for dev in range(1, 8):
            total = total + sgot[layer, lax.rem(me + 7 - dev + 8, 8)]
        tot_ref[layer] = jnp.broadcast_to(jnp.sum(total, axis=1, keepdims=True), (8, 128))
        for kind in range(2):
            scale = LEARN_RATE * jnp.sqrt(tot_ref[layer, 2 * kind:2 * kind + 1, 0:1] / tot_ref[layer, 2 * kind + 1:2 * kind + 2, 0:1])

            @pl.loop(0, 4)
            def _(j):
                span = pl.ds(pl.multiple_of((kind * 4 + j) * 96, 96), 96)
                new = (mb[span, :] - scale * dxacc[span, :]).astype(BF16)
                if kind == 0:
                    ws1[layer, :, pl.ds(pl.multiple_of(j * 768, 768), 768)] = new
                else:
                    ws2[layer, pl.ds(pl.multiple_of(j * 96, 96), 96), :] = new

    lo, hi = pl.ds(0, 48), pl.ds(48, 48)

    def gather_copy(src, dst, i, dev):
        return pltpu.make_async_remote_copy(src_ref=src, dst_ref=dst, send_sem=a_snd.at[i], recv_sem=a_rcv.at[i], device_id=(dev,), device_id_type=MESH)

    def gather_local():
        return pltpu.make_async_copy(ws1.at[1], wg1.at[y, x, c], ld_sem.at[3])

    def gather_parts(name):
        def same(ref, i, dev):
            return gather_copy(ref, ref, i, dev)
        if name == 's1':
            return (gather_copy(ws1.at[1, lo], wg1.at[y, x, c, lo], 0, xn), gather_copy(ws1.at[1, hi], wg1.at[y, x, c, hi], 1, yn))
        if name == 's2':
            return same(wg1.at[y, :, c, lo], 2, yn), same(wg1.at[:, x, c, hi], 3, xn)
        if name == 'd1':
            return (gather_copy(ws1.at[1], wg1.at[y, x, c], 4, partner),)
        if name == 'd2':
            return same(wg1.at[y, 1 - x, c, lo], 5, partner), same(wg1.at[1 - y, x, c, hi], 6, partner)
        return same(wg1.at[1 - y, :, c, lo], 7, partner), same(wg1.at[:, 1 - x, c, hi], 8, partner)

    def gather_start(*names):
        for name in names:
            for cp in gather_parts(name):
                cp.start()

    def gather_wait(*names):
        for name in names:
            for cp in gather_parts(name):
                cp.wait()

    units = ((p1, r01, r1a1, r1b1, r2a1, r2b1, 48), (p2, r02, r1a2, r1b2, r2a2, r2b2, 64))

    def remote(src, dst, u, slot, stage, dev):
        return pltpu.make_async_remote_copy(src_ref=src, dst_ref=dst, send_sem=snd.at[u, slot, stage], recv_sem=rcv.at[u, slot, stage], device_id=(dev,), device_id_type=MESH)

    def s0(u, slot):
        p, r0, r1a, r1b, r2a, r2b, hr = units[u]
        return remote(p.at[slot, 1 - c], r0.at[slot], u, slot, 0, partner)

    def s1(u, slot):
        p, r0, r1a, r1b, r2a, r2b, hr = units[u]
        return (remote(p.at[slot, c, :, 1 - x, pl.ds(0, hr)], r1a.at[slot], u, slot, 1, xn),
                remote(p.at[slot, c, 1 - y, :, pl.ds(hr, hr)], r1b.at[slot], u, slot, 2, yn))

    def s2(u, slot):
        p, r0, r1a, r1b, r2a, r2b, hr = units[u]
        return (remote(p.at[slot, c, 1 - y, x, pl.ds(0, hr)], r2a.at[slot], u, slot, 3, yn),
                remote(p.at[slot, c, y, 1 - x, pl.ds(hr, hr)], r2b.at[slot], u, slot, 4, xn))

    def start_s0(u, slot):
        s0(u, slot).start()

    def to_s1(u, slot):
        p, r0, r1a, r1b, r2a, r2b, hr = units[u]
        s0(u, slot).wait()

        @pl.loop(0, 2)
        def _(yy):
            for xx in range(2):
                p[slot, c, yy, xx] = (p[slot, c, yy, xx].astype(F32) + r0[slot, yy, xx].astype(F32)).astype(BF16)

        for cp in s1(u, slot):
            cp.start()

    def to_s2(u, slot):
        p, r0, r1a, r1b, r2a, r2b, hr = units[u]
        ca, cb = s1(u, slot)
        ca.wait()
        for i in range(2):
            p[slot, c, i, x, 0:hr] = (p[slot, c, i, x, 0:hr].astype(F32) + r1a[slot, i].astype(F32)).astype(BF16)
        cb.wait()
        for i in range(2):
            p[slot, c, y, i, hr:2 * hr] = (p[slot, c, y, i, hr:2 * hr].astype(F32) + r1b[slot, i].astype(F32)).astype(BF16)
        for cp in s2(u, slot):
            cp.start()

    def finish(u, slot, g):
        p, r0, r1a, r1b, r2a, r2b, hr = units[u]
        layer = 1 - g // 3
        k = g % 3
        ca, cb = s2(u, slot)
        for half, (cp, r2) in enumerate(((ca, r2a), (cb, r2b))):
            cp.wait()
            rows = slice(half * hr, half * hr + hr)
            total = p[slot, c, y, x, rows].astype(F32) + r2[slot].astype(F32)
            if u == 1:
                g2_ref[layer, pl.ds(pl.multiple_of(k * SUB + half * hr, 64), hr), :] = total
            else:
                for cc in range(2):
                    for q in range(4):
                        i = cc * 4 + q
                        f0 = pl.multiple_of((2 * q + cc) * 384 + k * SUB, SUB)
                        g1_ref[layer, rows, pl.ds(f0, SUB)] = total[:, i * SUB:(i + 1) * SUB]

    loads[0].wait()
    loads[1].wait()

    @pl.loop(0, 6)
    def _(g):
        slot = g % 2
        prev = 1 - slot
        layer = 1 - g // 3
        k = g % 3
        for cp in w_copies(g, slot):
            cp.wait()

        @pl.when(g < 5)
        def _():
            for cp in w_copies(g + 1, prev):
                cp.start()

        @pl.when(g == 3)
        def _():
            loads[2].wait()
            for cp in lamb_loads(1):
                cp.start()

        @pl.when(g == 5)
        def _():
            for cp in lamb_loads(0):
                cp.start()

        def tile(rows):
            xv = xb[layer, rows, :]
            dyv = dyb[rows, :]
            xt[:, rows] = xv.T
            for n in range(CH // 256):
                cs = slice(n * 256, n * 256 + 256)
                h = dot(xv, w1b[slot, :, cs])
                da = dot(dyv, w2b[slot, cs, :], NT_DIMS)
                sq = h * h
                s = 0.5 * jnp.tanh(h * (C0 + C1 * sq)) + 0.5
                a = h * s
                gp = s + a * (1.0 - s) * (2.0 * C0 + (6.0 * C1) * sq)
                at[cs, rows] = a.astype(BF16).T
                dhb[rows, cs] = (da * gp).astype(BF16)

        def token_loop(with_dx):
            @pl.loop(0, TOK // (2 * TT))
            def _(t):
                @pl.when((g > 0) & (t == 1))
                def _():
                    to_s1(0, prev)

                if not with_dx:
                    @pl.when((g == 4) & (t == 2))
                    def _():
                        lamb_apply(1)
                        gather_start('s1', 'd1')
                        gather_local().start()

                @pl.when((g > 0) & (t == 3))
                def _():
                    to_s2(1, prev)

                base = pl.multiple_of(t * (2 * TT), 2 * TT)
                spans = [pl.ds(base + i * TT, TT) for i in range(2)]
                for rows in spans:
                    tile(rows)
                if with_dx:
                    for rows in spans:
                        dxacc[rows, :] += dot(dhb[rows, :], w1b[slot], NT_DIMS)

        @pl.when(layer == 1)
        def _():
            @pl.when(k == 0)
            def _():
                @pl.loop(0, TOK // 128)
                def _(t):
                    rows = pl.ds(pl.multiple_of(t * 128, 128), 128)
                    dxacc[rows, :] = dyb[rows, :].astype(F32)

            token_loop(True)

        @pl.when(layer == 0)
        def _():
            token_loop(False)

        @pl.when(g > 0)
        def _():
            to_s2(0, prev)

        @pl.loop(0, CH // 256)
        def _(n):
            fs = pl.ds(pl.multiple_of(n * 256, 256), 256)
            res = dot(at[fs, :], dyb[...]).astype(BF16)
            p2[slot, n // 2, n % 2] = res.reshape(2, SUB, D)

        start_s0(1, slot)

        @pl.when(g > 0)
        def _():
            finish(1, prev, g - 1)

        @pl.loop(0, CH // 256)
        def _(n):
            fs = pl.ds(pl.multiple_of(n * 256, 256), 256)
            res = dot(xt[...], dhb[:, fs]).astype(BF16)
            for b in range(8):
                p1[slot, b % 2, b // 4, (b // 2) % 2, :, fs] = res[b * 96:(b + 1) * 96]

        to_s1(1, slot)
        start_s0(0, slot)

        @pl.when(g > 0)
        def _():
            finish(0, prev, g - 1)

        @pl.when(g == 2)
        def _():
            @pl.loop(0, TOK // TT)
            def _(t):
                rows = pl.ds(pl.multiple_of(t * TT, TT), TT)
                dyb[rows, :] = dxacc[rows, :].astype(BF16)

        @pl.when(g == 3)
        def _():
            lamb_moments(1)
            lamb_send(1)

        @pl.when(g == 4)
        def _():
            gather_local().wait()
            gather_wait('s1')
            gather_start('s2', 'd2')

    to_s1(0, 1)
    to_s2(1, 1)
    to_s2(0, 1)
    gather_wait('s2')
    gather_start('d3')
    finish(1, 1, 5)
    finish(0, 1, 5)
    lamb_moments(0)
    lamb_send(0)
    lamb_apply(0)
    gather_wait('d1', 'd2', 'd3')


def run_backward(*args):
    any_spec = pl.BlockSpec(memory_space=pl.ANY)
    vm = pltpu.VMEM
    return pl.pallas_call(
        backward_kernel,
        out_shape=(jax.ShapeDtypeStruct((2, 96, FF), F32), jax.ShapeDtypeStruct((2, 384, D), F32), jax.ShapeDtypeStruct((2, 8, 128), F32),
                   jax.ShapeDtypeStruct((2, 96, FF), BF16), jax.ShapeDtypeStruct((2, 384, D), BF16), jax.ShapeDtypeStruct((2, 2, 2, 96, FF), BF16)),
        in_specs=[any_spec] * 12,
        out_specs=(pl.BlockSpec(memory_space=vm),) * 5 + (any_spec,),
        scratch_shapes=[
            vm((2, TOK, D), BF16), vm((TOK, D), BF16), vm((D, TOK), BF16), vm((24 * 96, D), F32),
            vm((2, D, CH), BF16), vm((2, CH, D), BF16), vm((CH, TOK), BF16), vm((TOK, CH), BF16),
            vm((2, 2, 2, 2, 96, CH), BF16), vm((2, 2, 2, 2, SUB, D), BF16),
            vm((2, 2, 2, 96, CH), BF16), vm((2, 2, 2, SUB, D), BF16),
            vm((2, 2, 48, CH), BF16), vm((2, 2, 48, CH), BF16), vm((2, 2, 64, D), BF16), vm((2, 2, 64, D), BF16),
            vm((2, 48, CH), BF16), vm((2, 48, CH), BF16), vm((2, 64, D), BF16), vm((2, 64, D), BF16),
            vm((768, 768), F32), vm((2, 4, 8, 128), F32), vm((2, 8, 128), F32), vm((2, 8, 8, 128), F32),
            pltpu.SemaphoreType.DMA((4,)), pltpu.SemaphoreType.DMA((2, 16)),
            pltpu.SemaphoreType.DMA((2, 2, 5)), pltpu.SemaphoreType.DMA((2, 2, 5)),
            pltpu.SemaphoreType.DMA((32,)), pltpu.SemaphoreType.DMA((2, 7)), pltpu.SemaphoreType.DMA((2, 7)),
            pltpu.SemaphoreType.DMA((9,)), pltpu.SemaphoreType.DMA((9,)),
        ],
        compiler_params=pltpu.CompilerParams(collective_id=0, has_side_effects=True, vmem_limit_bytes=VMEM_MAX),
        name='backward',
    )(*args)


def finalize_kernel(tot, g1, a1, w1, m1, v1, g2, a2, w2, m2, v2, w1o, m1o, v1o, w2o, m2o, v2o):
    def part(kind, g, acc, w, m, v, wo, mo, vo):
        scale = LEARN_RATE * jnp.sqrt(tot[0, 2 * kind:2 * kind + 1, 0:1] / tot[0, 2 * kind + 1:2 * kind + 2, 0:1])
        mo[0], vo[0], upd = moments(g[0], acc[0], w[0], m[0], v[0])
        wo[0] = w[0] - scale * upd

    part(0, g1, a1, w1, m1, v1, w1o, m1o, v1o)
    part(1, g2, a2, w2, m2, v2, w2o, m2o, v2o)


def run_finalize(*args):
    up = pl.BlockSpec((1, 96, 768), lambda l, j: (l, 0, j))
    down = pl.BlockSpec((1, 96, 768), lambda l, j: (l, j, 0))
    s1 = jax.ShapeDtypeStruct((2, 96, FF), F32)
    s2 = jax.ShapeDtypeStruct((2, 384, D), F32)
    return pl.pallas_call(
        finalize_kernel,
        grid=(2, 4),
        out_shape=(s1, s1, s1, s2, s2, s2),
        in_specs=[pl.BlockSpec((1, 8, 128), lambda l, j: (l, 0, 0))] + [up] * 5 + [down] * 5,
        out_specs=(up, up, up, down, down, down),
        name='finalize',
    )(*args)


def forward_kernel(w1_hbm, w2_hbm, wg1_hbm, x_hbm, o_ref, wf1, wf2, ab, xb, ld_sem, snd, rcv):
    me, y, x, c, partner, xn, yn = position()
    fulls = (wf1.at[0], wf2.at[0], wf2.at[1])
    halves = (48, 192, 192)
    srcs = (w1_hbm.at[0], w2_hbm.at[0], w2_hbm.at[1])
    loads = [pltpu.make_async_copy(srcs[m], fulls[m].at[y, x, c], ld_sem.at[m]) for m in range(3)]
    loads.append(pltpu.make_async_copy(x_hbm, xb, ld_sem.at[3]))
    loads.append(pltpu.make_async_copy(wg1_hbm, wf1.at[1], ld_sem.at[4]))
    for cp in loads:
        cp.start()
    entry_barrier((partner, xn, yn))

    def same(ref, m, i, dev):
        return pltpu.make_async_remote_copy(src_ref=ref, dst_ref=ref, send_sem=snd.at[m, i], recv_sem=rcv.at[m, i], device_id=(dev,), device_id_type=MESH)

    def parts(m, name):
        f, h = fulls[m], halves[m]
        lo, hi = pl.ds(0, h), pl.ds(h, h)
        if name == 's1':
            return same(f.at[y, x, c, lo], m, 0, xn), same(f.at[y, x, c, hi], m, 1, yn)
        if name == 's2':
            return same(f.at[y, :, c, lo], m, 2, yn), same(f.at[:, x, c, hi], m, 3, xn)
        if name == 'd1':
            return (same(f.at[y, x, c], m, 4, partner),)
        if name == 'd2':
            return same(f.at[y, 1 - x, c, lo], m, 5, partner), same(f.at[1 - y, x, c, hi], m, 6, partner)
        return same(f.at[1 - y, :, c, lo], m, 7, partner), same(f.at[:, 1 - x, c, hi], m, 8, partner)

    def start(m, *names):
        for name in names:
            for cp in parts(m, name):
                cp.start()

    def wait(m, *names):
        for name in names:
            for cp in parts(m, name):
                cp.wait()

    def first(m):
        start(m, 's1', 'd1')

    def second(m):
        wait(m, 's1')
        start(m, 's2', 'd2')

    def third(m):
        wait(m, 's2')
        start(m, 'd3')

    def done(m):
        wait(m, 'd1', 'd2', 'd3')

    def up(layer, hook):
        @pl.loop(0, TOK // TT)
        def _(t):
            hook(t)
            rows = pl.ds(pl.multiple_of(t * TT, TT), TT)
            xv = xb[rows, :]
            for n in range(4):
                cs = slice(n * 768, n * 768 + 768)
                h = dot(xv, wf1[layer, :, :, :, :, cs].reshape(D, 768))
                s = 0.5 * jnp.tanh(h * (C0 + C1 * (h * h))) + 0.5
                ab[rows, cs] = (h * s).astype(BF16)

    def down(layer, hook):
        @pl.loop(0, TOK // TT)
        def _(t):
            hook(t)
            rows = pl.ds(pl.multiple_of(t * TT, TT), TT)
            res = xb[rows, :].astype(F32) + dot(ab[rows, :], wf2[layer].reshape(FF, D))
            if layer == 0:
                xb[rows, :] = res.astype(BF16)
            else:
                o_ref[rows, :] = res.astype(BF16)

    def no_hook(t):
        pass

    def at_step(step, fn):
        def hook(t):
            @pl.when(t == step)
            def _():
                fn()
        return hook

    loads[0].wait()
    first(0)
    for cp in loads[1:3]:
        cp.wait()
    second(0)
    first(1)
    third(0)
    second(1)
    first(2)
    loads[3].wait()
    loads[4].wait()
    done(0)
    up(0, no_hook)
    third(1)
    done(1)
    down(0, at_step(1, lambda: second(2)))
    up(1, at_step(4, lambda: third(2)))
    done(2)
    down(1, no_hook)


def run_forward(*args):
    any_spec = pl.BlockSpec(memory_space=pl.ANY)
    vm = pltpu.VMEM
    return pl.pallas_call(
        forward_kernel,
        out_shape=jax.ShapeDtypeStruct((TOK, D), BF16),
        in_specs=[any_spec] * 4,
        out_specs=pl.BlockSpec(memory_space=vm),
        scratch_shapes=[
            vm((2, 2, 2, 2, 96, FF), BF16), vm((2, 2, 2, 2, 384, D), BF16), vm((TOK, FF), BF16), vm((TOK, D), BF16),
            pltpu.SemaphoreType.DMA((5,)), pltpu.SemaphoreType.DMA((3, 9)), pltpu.SemaphoreType.DMA((3, 9)),
        ],
        compiler_params=pltpu.CompilerParams(collective_id=1, has_side_effects=True, vmem_limit_bytes=VMEM_MAX),
        name='forward',
    )(*args)


def solution(mesh):
    shard_rows = P(None, 'fsdp')
    shard_batch = P('fsdp')
    spec_whole = P()

    def local_step(x_layers, dy_top, x_next, w_up, w_down, acc_up, acc_down, master_up, master_down, mom_up, mom_down, var_up, var_down):
        g1, g2, tot, ws1, ws2, wg1 = run_backward(x_layers.reshape(2, TOK, D), dy_top.reshape(TOK, D), w_up, w_down, acc_up, acc_down, master_up, master_down, mom_up, mom_down, var_up, var_down)
        out = run_forward(ws1, ws2, wg1, x_next.reshape(TOK, D))
        up_new, m1, v1, down_new, m2, v2 = run_finalize(tot, g1, acc_up, master_up, mom_up, var_up, g2, acc_down, master_down, mom_down, var_down)
        return up_new, down_new, m1, m2, v1, v2, out.reshape(1, TOK, D)

    return jax.shard_map(local_step, mesh=mesh, in_specs=(shard_rows, shard_batch, shard_batch, spec_whole, spec_whole) + (shard_rows,) * 8, out_specs=(shard_rows,) * 6 + (shard_batch,), check_vma=False)
```

```python
import functools

import jax
import jax.numpy as jnp
from jax import lax
from jax.experimental import pallas as pl
from jax.experimental.pallas import tpu as pltpu
from jax.sharding import PartitionSpec as P

MICRO_STEPS = 2
STEP_COUNT = 3
BETA_MOM = 0.9
BETA_VAR = 0.999
ADAM_EPS = 1e-6
WEIGHT_DECAY = 0.01
LEARN_RATE = 0.06

C0 = 0.7978845608028654
C1 = C0 * 0.044715
MESH = pl.DeviceIdType.MESH
BF16 = jnp.bfloat16
F32 = jnp.float32
VMEM_MAX = 67043328

TOK = 2048
D = 768
FF = 3072
SUB = 128
CH = 8 * SUB
TT = 256
NT_DIMS = (((1,), (1,)), ((), ()))
NN_DIMS = (((1,), (0,)), ((), ()))


def position():
    me = lax.axis_index('fsdp')
    y, x, c = me // 4, (me // 2) % 2, me % 2
    return me, y, x, c, me + 1 - 2 * c, me + 2 - 4 * x, me + 4 - 8 * y


def entry_barrier(targets):
    barrier = pltpu.get_barrier_semaphore()
    for dev in targets:
        pl.semaphore_signal(barrier, inc=1, device_id=(dev,), device_id_type=MESH)
    pl.semaphore_wait(barrier, len(targets))


def dot(a, b, dims=NN_DIMS):
    return lax.dot_general(a, b, dims, preferred_element_type=F32)


def moments(grad_sum, acc, master, mom_prev, var_prev):
    grad = (acc + grad_sum) / MICRO_STEPS
    mom = BETA_MOM * mom_prev + (1.0 - BETA_MOM) * grad
    var = BETA_VAR * var_prev + (1.0 - BETA_VAR) * grad * grad
    upd = (mom / (1.0 - BETA_MOM ** STEP_COUNT)) / (jnp.sqrt(var / (1.0 - BETA_VAR ** STEP_COUNT)) + ADAM_EPS) + WEIGHT_DECAY * master
    return mom, var, upd


def step_kernel(x_hbm, dy_hbm, xn_hbm, w1_hbm, w2_hbm, acc1, acc2, mas1, mas2, mom1, mom2, var1, var2,
                wo1, wo2, mo1, mo2, vo1, vo2, out, wg1, wg2,
                xb, dyb, xt, dxacc, w1b, w2b, at, dhb, p1, p2, r01, r02, r1a1, r1b1, r1a2, r1b2, r2a1, r2b1, r2a2, r2b2,
                g1, g2, mb, sqb, smine, sgot, tot, ws1, ws2,
                ld_sem, w_sem, snd, rcv, l_sem, o_sem, x_snd, x_rcv, a_snd, a_rcv, b_snd, b_rcv, f_sem, out_sem):
    me, y, x, c, partner, xn, yn = position()
    others = [lax.rem(me + i, 8) for i in range(1, 8)]

    def column(q, cc, k):
        return pl.ds(pl.multiple_of((2 * q + cc) * 384 + k * SUB, SUB), SUB)

    def w_copies(g):
        layer = 1 - g // 3
        k = g % 3
        res = []
        for cc in range(2):
            for q in range(4):
                i = cc * 4 + q
                res.append(pltpu.make_async_copy(w1_hbm.at[layer, :, :, :, :, column(q, cc, k)], w1b.at[k, :, :, :, :, pl.ds(i * SUB, SUB)], w_sem.at[k, i]))
            res.append(pltpu.make_async_copy(w2_hbm.at[layer, :, :, cc, k], w2b.at[k, cc], w_sem.at[k, 8 + cc]))
        return res

    loads = [pltpu.make_async_copy(x_hbm.at[1], xb.at[1], ld_sem.at[0]),
             pltpu.make_async_copy(dy_hbm, dyb, ld_sem.at[1]),
             pltpu.make_async_copy(x_hbm.at[0], xb.at[0], ld_sem.at[2]),
             pltpu.make_async_copy(xn_hbm, xb.at[1], ld_sem.at[3])]
    for cp in loads[:2]:
        cp.start()
    for cp in w_copies(0):
        cp.start()
    loads[2].start()

    sqb[...] = jnp.zeros_like(sqb)
    smine[...] = jnp.zeros_like(smine)
    entry_barrier(others)

    def area(a, kind, j):
        return pl.ds(pl.multiple_of(a * 768 + j * 96, 96), 96) if kind == 0 else pl.ds(pl.multiple_of(a * 768 + 384 + j * SUB, SUB), SUB)

    def shard_pairs(up, down, layer, buf, a):
        res = [(up.at[layer, :, pl.ds(j * 768, 768)], buf.at[pl.ds(a * 768 + j * 96, 96), :]) for j in range(4)]
        res.append((down.at[layer], buf.at[pl.ds(a * 768 + 384, 384), :]))
        return res

    def lamb_loads(layer):
        res = []
        for a, (up, down) in enumerate(((acc1, acc2), (mom1, mom2), (var1, var2), (mas1, mas2))):
            for i, (src, dst) in enumerate(shard_pairs(up, down, layer, dxacc if a < 3 else mb, a % 3)):
                res.append(pltpu.make_async_copy(src, dst, l_sem.at[a, i]))
        return res

    def lamb_outs(layer, kinds, arrays):
        res = []
        for a, (up, down) in ((0, (wo1, wo2)), (1, (mo1, mo2)), (2, (vo1, vo2))):
            for i, (dst, src) in enumerate(shard_pairs(up, down, layer, mb if a == 0 else dxacc, a)):
                if a in arrays and i // 4 in kinds:
                    res.append(pltpu.make_async_copy(src, dst, o_sem.at[a, i]))
        return res

    def run(copies):
        for cp in copies:
            cp.start()

    def settle(copies):
        for cp in copies:
            cp.wait()

    def lamb_moments(layer, kind):
        @pl.loop(0, 4 - kind)
        def _(j):
            spans = [area(a, kind, j) for a in range(3)]
            grad_sum = g1[:, pl.ds(pl.multiple_of(j * 768, 768), 768)] if kind == 0 else g2[pl.ds(pl.multiple_of(j * SUB, SUB), SUB), :]
            master = mb[spans[0], :]
            mom, var, upd = moments(grad_sum, dxacc[spans[0], :], master, dxacc[spans[1], :], dxacc[spans[2], :])
            dxacc[spans[0], :] = upd
            dxacc[spans[1], :] = mom
            dxacc[spans[2], :] = var
            for i, val in enumerate((master, upd)):
                folded = jnp.sum((val * val).reshape(-1, 8, 768), axis=0)
                lanes = folded[:, 0:128]
                for b in range(1, 6):
                    lanes = lanes + folded[:, b * 128:(b + 1) * 128]
                sqb[layer, kind, i] += lanes

        for i in range(2):
            smine[layer, kind, i:i + 1, :] = jnp.sum(sqb[layer, kind, i], axis=0, keepdims=True)
        run(sum_copies(layer, kind))
        run(lamb_outs(layer, (kind,), (1, 2)))

    def sum_copies(layer, kind):
        return [pltpu.make_async_remote_copy(src_ref=smine.at[layer, kind], dst_ref=sgot.at[layer, kind, i], send_sem=x_snd.at[layer, kind, i], recv_sem=x_rcv.at[layer, kind, i], device_id=(dev,), device_id_type=MESH) for i, dev in enumerate(others)]

    def lamb_apply(layer, kind):
        sgot[layer, kind, 7] = smine[layer, kind]
        settle(sum_copies(layer, kind))
        total = sgot[layer, kind, lax.rem(me + 7, 8)]
        for dev in range(1, 8):
            total = total + sgot[layer, kind, lax.rem(me + 7 - dev + 8, 8)]
        tot[...] = jnp.broadcast_to(jnp.sum(total, axis=1, keepdims=True), (8, 128))
        scale = LEARN_RATE * jnp.sqrt(tot[0:1, 0:1] / tot[1:2, 0:1])

        @pl.loop(0, 4 - kind)
        def _(j):
            span = area(0, kind, j)
            new = mb[span, :] - scale * dxacc[span, :]
            mb[span, :] = new
            half = new.astype(BF16)
            if kind == 1:
                if layer == 1:
                    ws2[j] = half
                else:
                    w2b[j, c, y, x] = half
            else:
                for cc in range(2):
                    lanes = pl.ds(pl.multiple_of((cc * 4 + j) * SUB, SUB), SUB)
                    for k in range(3):
                        piece = half[:, cc * 384 + k * SUB:cc * 384 + (k + 1) * SUB]
                        if layer == 1:
                            ws1[k, :, lanes] = piece
                        else:
                            w1b[k, y, x, c, :, lanes] = piece

        run(lamb_outs(layer, (kind,), (0,)))

    def remote_copy(src, dst, s_sem, r_sem, dev):
        return pltpu.make_async_remote_copy(src_ref=src, dst_ref=dst, send_sem=s_sem, recv_sem=r_sem, device_id=(dev,), device_id_type=MESH)

    lo, hi = pl.ds(0, 48), pl.ds(48, 48)

    def gather_local():
        return pltpu.make_async_copy(ws1, wg1.at[:, y, x, c], ld_sem.at[4])

    def gather2_local():
        return pltpu.make_async_copy(ws2, wg2.at[:, c, y, x], ld_sem.at[5])

    def gather_parts(name):
        def go(src, dst, i, dev):
            return remote_copy(src, dst, a_snd.at[i], a_rcv.at[i], dev)
        if name == 's1':
            return (go(ws1.at[:, lo], wg1.at[:, y, x, c, lo], 0, xn), go(ws1.at[:, hi], wg1.at[:, y, x, c, hi], 1, yn))
        if name == 's2':
            return go(wg1.at[:, y, :, c, lo], wg1.at[:, y, :, c, lo], 2, yn), go(wg1.at[:, :, x, c, hi], wg1.at[:, :, x, c, hi], 3, xn)
        if name == 'd1':
            return (go(ws1, wg1.at[:, y, x, c], 4, partner),)
        if name == 'd2':
            return (go(wg1.at[:, y, 1 - x, c, lo], wg1.at[:, y, 1 - x, c, lo], 5, partner), go(wg1.at[:, 1 - y, x, c, hi], wg1.at[:, 1 - y, x, c, hi], 6, partner))
        return (go(wg1.at[:, 1 - y, :, c, lo], wg1.at[:, 1 - y, :, c, lo], 7, partner), go(wg1.at[:, :, 1 - x, c, hi], wg1.at[:, :, 1 - x, c, hi], 8, partner))

    def gather_start(*names):
        for name in names:
            run(gather_parts(name))

    def gather_wait(*names):
        for name in names:
            settle(gather_parts(name))

    def piece_parts(m, name):
        if m < 6 and m % 2 == 0:
            ref = w1b.at[m // 2]
            h = 48

            def blk(yy, xx, rows):
                return ref.at[yy, xx, c, rows]
        else:
            ref = w2b.at[m // 2] if m < 6 else wg2.at[m - 6]
            h = 64

            def blk(yy, xx, rows):
                return ref.at[c, yy, xx, rows]
        first, last, every, both = pl.ds(0, h), pl.ds(h, h), pl.ds(0, 2 * h), slice(None)

        def go(part, i, dev):
            return remote_copy(part, part, b_snd.at[m, i], b_rcv.at[m, i], dev)
        if name == 's1':
            return go(blk(y, x, first), 0, xn), go(blk(y, x, last), 1, yn)
        if name == 's2':
            return go(blk(y, both, first), 2, yn), go(blk(both, x, last), 3, xn)
        if name == 'd1':
            return (go(blk(y, x, every), 4, partner),)
        if name == 'd2':
            return go(blk(y, 1 - x, first), 5, partner), go(blk(1 - y, x, last), 6, partner)
        return go(blk(1 - y, both, first), 7, partner), go(blk(both, 1 - x, last), 8, partner)

    def first(m):
        run(piece_parts(m, 's1'))
        run(piece_parts(m, 'd1'))

    def second(m):
        settle(piece_parts(m, 's1'))
        run(piece_parts(m, 's2'))
        run(piece_parts(m, 'd2'))

    def third(m):
        settle(piece_parts(m, 's2'))
        run(piece_parts(m, 'd3'))

    def done(m):
        for name in ('d1', 'd2', 'd3'):
            settle(piece_parts(m, name))

    units = ((p1, r01, r1a1, r1b1, r2a1, r2b1, 48), (p2, r02, r1a2, r1b2, r2a2, r2b2, 64))

    def remote(src, dst, u, slot, stage, dev):
        return pltpu.make_async_remote_copy(src_ref=src, dst_ref=dst, send_sem=snd.at[u, slot, stage], recv_sem=rcv.at[u, slot, stage], device_id=(dev,), device_id_type=MESH)

    def s0(u, slot):
        p, r0, r1a, r1b, r2a, r2b, hr = units[u]
        return remote(p.at[slot, 1 - c], r0.at[slot], u, slot, 0, partner)

    def s1(u, slot):
        p, r0, r1a, r1b, r2a, r2b, hr = units[u]
        return (remote(p.at[slot, c, :, 1 - x, pl.ds(0, hr)], r1a.at[slot], u, slot, 1, xn),
                remote(p.at[slot, c, 1 - y, :, pl.ds(hr, hr)], r1b.at[slot], u, slot, 2, yn))

    def s2(u, slot):
        p, r0, r1a, r1b, r2a, r2b, hr = units[u]
        return (remote(p.at[slot, c, 1 - y, x, pl.ds(0, hr)], r2a.at[slot], u, slot, 3, yn),
                remote(p.at[slot, c, y, 1 - x, pl.ds(hr, hr)], r2b.at[slot], u, slot, 4, xn))

    def start_s0(u, slot):
        s0(u, slot).start()

    def to_s1(u, slot):
        p, r0, r1a, r1b, r2a, r2b, hr = units[u]
        s0(u, slot).wait()

        @pl.loop(0, 2)
        def _(yy):
            for xx in range(2):
                p[slot, c, yy, xx] = (p[slot, c, yy, xx].astype(F32) + r0[slot, yy, xx].astype(F32)).astype(BF16)

        for cp in s1(u, slot):
            cp.start()

    def to_s2(u, slot):
        p, r0, r1a, r1b, r2a, r2b, hr = units[u]
        ca, cb = s1(u, slot)
        ca.wait()
        for i in range(2):
            p[slot, c, i, x, 0:hr] = (p[slot, c, i, x, 0:hr].astype(F32) + r1a[slot, i].astype(F32)).astype(BF16)
        cb.wait()
        for i in range(2):
            p[slot, c, y, i, hr:2 * hr] = (p[slot, c, y, i, hr:2 * hr].astype(F32) + r1b[slot, i].astype(F32)).astype(BF16)
        for cp in s2(u, slot):
            cp.start()

    def finish(u, slot, g):
        p, r0, r1a, r1b, r2a, r2b, hr = units[u]
        k = g % 3
        ca, cb = s2(u, slot)
        for half, (cp, r2) in enumerate(((ca, r2a), (cb, r2b))):
            cp.wait()
            rows = slice(half * hr, half * hr + hr)
            total = p[slot, c, y, x, rows].astype(F32) + r2[slot].astype(F32)
            if u == 1:
                g2[pl.ds(pl.multiple_of(k * SUB + half * hr, 64), hr), :] = total
            else:
                for cc in range(2):
                    for q in range(4):
                        i = cc * 4 + q
                        g1[rows, column(q, cc, k)] = total[:, i * SUB:(i + 1) * SUB]

    settle(loads[:2])

    @pl.loop(0, 6)
    def _(g):
        slot = g % 2
        prev = 1 - slot
        layer = 1 - g // 3
        k = g % 3
        settle(w_copies(g))

        @pl.when(g < 5)
        def _():
            run(w_copies(g + 1))

        @pl.when(g == 3)
        def _():
            loads[2].wait()
            loads[3].start()
            run(lamb_loads(1))

        @pl.when(g == 5)
        def _():
            settle(lamb_outs(1, (0, 1), (0, 1, 2)))
            run(lamb_loads(0))

        def tile(rows):
            xv = xb[layer, rows, :]
            dyv = dyb[rows, :]
            xt[:, rows] = xv.T
            for n in range(CH // 256):
                cs = slice(n * 256, n * 256 + 256)
                h = dot(xv, w1b[k, :, :, :, :, cs].reshape(D, 256))
                da = dot(dyv, w2b[k, n // 2, n % 2].reshape(256, D), NT_DIMS)
                sq = h * h
                s = 0.5 * jnp.tanh(h * (C0 + C1 * sq)) + 0.5
                a = h * s
                gp = s + a * (1.0 - s) * (2.0 * C0 + (6.0 * C1) * sq)
                at[cs, rows] = a.astype(BF16).T
                dhb[rows, cs] = (da * gp).astype(BF16)

        def token_loop(with_dx):
            @pl.loop(0, TOK // (2 * TT))
            def _(t):
                @pl.when((g > 0) & (t == 1))
                def _():
                    to_s1(1, prev)

                if not with_dx:
                    @pl.when((g == 4) & (t == 2))
                    def _():
                        lamb_apply(1, 0)
                        gather_start('s1', 'd1')
                        gather_local().start()
                        lamb_apply(1, 1)
                        gather2_local().start()

                @pl.when((g > 0) & (t == 3))
                def _():
                    to_s2(0, prev)

                base = pl.multiple_of(t * (2 * TT), 2 * TT)
                spans = [pl.ds(base + i * TT, TT) for i in range(2)]
                for rows in spans:
                    tile(rows)
                if with_dx:
                    for rows in spans:
                        dxacc[rows, :] += dot(dhb[rows, :], w1b[k].reshape(D, CH), NT_DIMS)

        @pl.when(layer == 1)
        def _():
            @pl.when(k == 0)
            def _():
                @pl.loop(0, TOK // 128)
                def _(t):
                    rows = pl.ds(pl.multiple_of(t * 128, 128), 128)
                    dxacc[rows, :] = dyb[rows, :].astype(F32)

            token_loop(True)

        @pl.when(layer == 0)
        def _():
            token_loop(False)

        @pl.when(g > 0)
        def _():
            to_s2(1, prev)

        @pl.loop(0, CH // 256)
        def _(n):
            fs = pl.ds(pl.multiple_of(n * 256, 256), 256)
            res = dot(xt[...], dhb[:, fs]).astype(BF16)
            for b in range(8):
                p1[slot, b % 2, b // 4, (b // 2) % 2, :, fs] = res[b * 96:(b + 1) * 96]

        start_s0(0, slot)

        @pl.when(g > 0)
        def _():
            finish(0, prev, g - 1)

        @pl.loop(0, CH // 256)
        def _(n):
            fs = pl.ds(pl.multiple_of(n * 256, 256), 256)
            res = dot(at[fs, :], dyb[...]).astype(BF16)
            p2[slot, n // 2, n % 2] = res.reshape(2, SUB, D)

        to_s1(0, slot)
        start_s0(1, slot)

        @pl.when(g > 0)
        def _():
            finish(1, prev, g - 1)

        @pl.when(g == 2)
        def _():
            @pl.loop(0, TOK // TT)
            def _(t):
                rows = pl.ds(pl.multiple_of(t * TT, TT), TT)
                dyb[rows, :] = dxacc[rows, :].astype(BF16)

        @pl.when(g == 3)
        def _():
            settle(lamb_loads(1))
            lamb_moments(1, 0)
            lamb_moments(1, 1)

        @pl.when(g == 4)
        def _():
            gather_local().wait()
            gather_wait('s1')
            gather_start('s2', 'd2')

    to_s1(1, 1)
    to_s2(0, 1)
    to_s2(1, 1)
    settle(lamb_loads(0))
    finish(0, 1, 5)
    lamb_moments(0, 0)
    finish(1, 1, 5)
    lamb_moments(0, 1)
    lamb_apply(0, 0)
    first(0)
    first(2)
    lamb_apply(0, 1)
    second(0)
    first(1)
    second(2)
    first(3)
    second(1)
    first(4)
    gather_wait('s2')
    gather_start('d3')
    third(0)
    first(5)
    second(3)
    gather2_local().wait()
    loads[3].wait()
    settle(lamb_outs(0, (0, 1), (1, 2)))
    third(1)
    third(2)
    done(0)
    done(1)
    gather_wait('d1', 'd2', 'd3')

    def chunk_load(k, kind):
        if kind == 0:
            return pltpu.make_async_copy(wg1.at[k], w1b.at[k], f_sem.at[k, 0])
        return pltpu.make_async_copy(wg2.at[k], w2b.at[k], f_sem.at[k, 1])

    def out_copy(t):
        rows = pl.ds(pl.multiple_of(t * 512, 512), 512)
        return pltpu.make_async_copy(dyb.at[rows, :], out.at[rows, :], out_sem.at[t])

    def before_1():
        chunk_load(0, 0).start()
        second(5)
        first(6)
        first(7)
        third(3)
        done(2)
        done(3)

    def before_2():
        chunk_load(1, 0).start()
        third(5)
        done(4)
        done(5)

    def before_3():
        chunk_load(2, 0).start()
        second(8)
        done(6)
        chunk_load(0, 1).start()
        chunk_load(0, 0).wait()
        chunk_load(0, 1).wait()

    def before_4():
        chunk_load(1, 0).wait()
        chunk_load(1, 1).wait()

    def before_5():
        chunk_load(2, 0).wait()
        chunk_load(2, 1).wait()

    def load_second(m):
        done(m)
        chunk_load(m - 6, 1).start()

    def six_and_eight():
        second(6)
        first(8)

    hooks = {
        (0, 0): lambda: second(4),
        (1, 2): lambda: third(4),
        (1, 3): six_and_eight,
        (2, 1): lambda: second(7),
        (2, 3): lambda: third(6),
        (3, 1): lambda: third(7),
        (3, 3): lambda: load_second(7),
        (4, 1): lambda: third(8),
        (4, 3): lambda: load_second(8),
    }

    @pl.loop(0, 6)
    def _(f):
        k = f % 3
        for i, fn in enumerate((before_1, before_2, before_3, before_4, before_5)):
            pl.when(f == i + 1)(fn)

        @pl.when(k == 0)
        def _():
            @pl.loop(0, TOK // 128)
            def _(t):
                rows = pl.ds(pl.multiple_of(t * 128, 128), 128)
                dxacc[rows, :] = xb[1, rows, :].astype(F32)

        @pl.loop(0, TOK // (2 * TT))
        def _(t):
            for (hf, ht), fn in hooks.items():
                pl.when((f == hf) & (t == ht))(fn)
            base = pl.multiple_of(t * (2 * TT), 2 * TT)
            spans = [pl.ds(base + i * TT, TT) for i in range(2)]
            for rows in spans:
                xv = xb[1, rows, :]
                for n in range(CH // 256):
                    cs = slice(n * 256, n * 256 + 256)
                    h = dot(xv, w1b[k, :, :, :, :, cs].reshape(D, 256))
                    s = 0.5 * jnp.tanh(h * (C0 + C1 * (h * h))) + 0.5
                    dhb[rows, cs] = (h * s).astype(BF16)
            for rows in spans:
                dxacc[rows, :] += dot(dhb[rows, :], w2b[k].reshape(CH, D))

            pair = pl.ds(base, 2 * TT)

            @pl.when(f == 2)
            def _():
                xb[1, pair, :] = dxacc[pair, :].astype(BF16)

            @pl.when(f == 5)
            def _():
                dyb[pair, :] = dxacc[pair, :].astype(BF16)
                out_copy(t).start()

    settle(lamb_outs(0, (0, 1), (0,)))
    for t in range(4):
        out_copy(t).wait()


def run_step(*args):
    any_spec = pl.BlockSpec(memory_space=pl.ANY)
    vm = pltpu.VMEM
    dma = pltpu.SemaphoreType.DMA
    up, down = jax.ShapeDtypeStruct((2, 96, FF), F32), jax.ShapeDtypeStruct((2, 384, D), F32)
    return pl.pallas_call(
        step_kernel,
        out_shape=(up, down, up, down, up, down, jax.ShapeDtypeStruct((TOK, D), BF16),
                   jax.ShapeDtypeStruct((3, 2, 2, 2, 96, CH), BF16), jax.ShapeDtypeStruct((3, 2, 2, 2, SUB, D), BF16)),
        in_specs=[any_spec] * 13,
        out_specs=(any_spec,) * 9,
        scratch_shapes=[
            vm((2, TOK, D), BF16), vm((TOK, D), BF16), vm((D, TOK), BF16), vm((3 * 768, D), F32),
            vm((3, 2, 2, 2, 96, CH), BF16), vm((3, 2, 2, 2, SUB, D), BF16), vm((CH, TOK), BF16), vm((TOK, CH), BF16),
            vm((2, 2, 2, 2, 96, CH), BF16), vm((2, 2, 2, 2, SUB, D), BF16),
            vm((2, 2, 2, 96, CH), BF16), vm((2, 2, 2, SUB, D), BF16),
            vm((2, 2, 48, CH), BF16), vm((2, 2, 48, CH), BF16), vm((2, 2, 64, D), BF16), vm((2, 2, 64, D), BF16),
            vm((2, 48, CH), BF16), vm((2, 48, CH), BF16), vm((2, 64, D), BF16), vm((2, 64, D), BF16),
            vm((96, FF), F32), vm((384, D), F32), vm((768, 768), F32), vm((2, 2, 2, 8, 128), F32), vm((2, 2, 8, 128), F32), vm((2, 2, 8, 8, 128), F32), vm((8, 128), F32),
            vm((3, 96, CH), BF16), vm((3, SUB, D), BF16),
            dma((6,)), dma((3, 10)), dma((2, 2, 5)), dma((2, 2, 5)), dma((4, 5)), dma((3, 5)),
            dma((2, 2, 7)), dma((2, 2, 7)), dma((9,)), dma((9,)), dma((9, 9)), dma((9, 9)), dma((3, 2)), dma((4,)),
        ],
        compiler_params=pltpu.CompilerParams(collective_id=0, has_side_effects=True, vmem_limit_bytes=VMEM_MAX),
        name='step',
    )(*args)


def solution(mesh):
    shard_rows = P(None, 'fsdp')
    shard_batch = P('fsdp')
    spec_whole = P()

    def local_step(x_layers, dy_top, x_next, w_up, w_down, acc_up, acc_down, master_up, master_down, mom_up, mom_down, var_up, var_down):
        res = run_step(x_layers.reshape(2, TOK, D), dy_top.reshape(TOK, D), x_next.reshape(TOK, D),
                       w_up.reshape(2, 2, 2, 2, 96, FF), w_down.reshape(2, 2, 2, 2, 3, SUB, D),
                       acc_up, acc_down, master_up, master_down, mom_up, mom_down, var_up, var_down)
        return res[:6] + (res[6].reshape(1, TOK, D),)

    return jax.shard_map(local_step, mesh=mesh, in_specs=(shard_rows, shard_batch, shard_batch, spec_whole, spec_whole) + (shard_rows,) * 8, out_specs=(shard_rows,) * 6 + (shard_batch,), check_vma=False)
```

```python
import functools

import jax
import jax.numpy as jnp
from jax import lax
from jax.experimental import pallas as pl
from jax.experimental.pallas import tpu as pltpu
from jax.sharding import PartitionSpec as P

MICRO_STEPS = 2
STEP_COUNT = 3
BETA_MOM = 0.9
BETA_VAR = 0.999
ADAM_EPS = 1e-6
WEIGHT_DECAY = 0.01
LEARN_RATE = 0.06

C0 = 0.7978845608028654
C1 = C0 * 0.044715
MESH = pl.DeviceIdType.MESH
BF16 = jnp.bfloat16
F32 = jnp.float32
VMEM_MAX = 67043328

TOK = 2048
D = 768
FF = 3072
SUB = 128
CH = 8 * SUB
TT = 256
NT_DIMS = (((1,), (1,)), ((), ()))
NN_DIMS = (((1,), (0,)), ((), ()))


def position():
    me = lax.axis_index('fsdp')
    y, x, c = me // 4, (me // 2) % 2, me % 2
    return me, y, x, c, me + 1 - 2 * c, me + 2 - 4 * x, me + 4 - 8 * y


def entry_barrier(targets):
    barrier = pltpu.get_barrier_semaphore()
    for dev in targets:
        pl.semaphore_signal(barrier, inc=1, device_id=(dev,), device_id_type=MESH)
    pl.semaphore_wait(barrier, len(targets))


def dot(a, b, dims=NN_DIMS):
    return lax.dot_general(a, b, dims, preferred_element_type=F32)


def moments(grad_sum, acc, master, mom_prev, var_prev):
    grad = (acc + grad_sum) / MICRO_STEPS
    mom = BETA_MOM * mom_prev + (1.0 - BETA_MOM) * grad
    var = BETA_VAR * var_prev + (1.0 - BETA_VAR) * grad * grad
    upd = (mom / (1.0 - BETA_MOM ** STEP_COUNT)) / (jnp.sqrt(var / (1.0 - BETA_VAR ** STEP_COUNT)) + ADAM_EPS) + WEIGHT_DECAY * master
    return mom, var, upd


def step_kernel(x_hbm, dy_hbm, xn_hbm, w1_hbm, w2_hbm, acc1, acc2, mas1, mas2, mom1, mom2, var1, var2,
                wo1, wo2, mo1, mo2, vo1, vo2, out, wg1, wg2,
                xb, dyb, xt, dxacc, w1b, w2b, at, dhb, p1, p2, r01, r02, r1a1, r1b1, r1a2, r1b2, r2a1, r2b1, r2a2, r2b2,
                g1, g2, mb, sqb, smine, sgot, tot, ws1, ws2,
                ld_sem, w_sem, snd, rcv, l_sem, o_sem, x_snd, x_rcv, b_snd, b_rcv, f_sem, out_sem):
    me, y, x, c, partner, xn, yn = position()
    others = [lax.rem(me + i, 8) for i in range(1, 8)]

    def column(q, cc, k):
        return pl.ds(pl.multiple_of((2 * q + cc) * 384 + k * SUB, SUB), SUB)

    def w_copies(g):
        layer = 1 - g // 3
        k = g % 3
        res = []
        for cc in range(2):
            for q in range(4):
                i = cc * 4 + q
                res.append(pltpu.make_async_copy(w1_hbm.at[layer, :, :, :, :, column(q, cc, k)], w1b.at[k, :, :, :, :, pl.ds(i * SUB, SUB)], w_sem.at[k, i]))
            res.append(pltpu.make_async_copy(w2_hbm.at[layer, :, :, cc, k], w2b.at[k, cc], w_sem.at[k, 8 + cc]))
        return res

    loads = [pltpu.make_async_copy(x_hbm.at[1], xb.at[1], ld_sem.at[0]),
             pltpu.make_async_copy(dy_hbm, dyb, ld_sem.at[1]),
             pltpu.make_async_copy(x_hbm.at[0], xb.at[0], ld_sem.at[2]),
             pltpu.make_async_copy(xn_hbm, xb.at[1], ld_sem.at[3])]
    for cp in loads[:2]:
        cp.start()
    for cp in w_copies(0):
        cp.start()
    loads[2].start()

    sqb[...] = jnp.zeros_like(sqb)
    smine[...] = jnp.zeros_like(smine)
    entry_barrier(others)

    def area(a, kind, j):
        return pl.ds(pl.multiple_of(a * 768 + j * 96, 96), 96) if kind == 0 else pl.ds(pl.multiple_of(a * 768 + 384 + j * SUB, SUB), SUB)

    def shard_pairs(up, down, layer, buf, a):
        res = [(up.at[layer, :, pl.ds(j * 768, 768)], buf.at[pl.ds(a * 768 + j * 96, 96), :]) for j in range(4)]
        res.append((down.at[layer], buf.at[pl.ds(a * 768 + 384, 384), :]))
        return res

    def lamb_loads(layer):
        res = []
        for a, (up, down) in enumerate(((acc1, acc2), (mom1, mom2), (var1, var2), (mas1, mas2))):
            for i, (src, dst) in enumerate(shard_pairs(up, down, layer, dxacc if a < 3 else mb, a % 3)):
                res.append(pltpu.make_async_copy(src, dst, l_sem.at[a, i]))
        return res

    def lamb_outs(layer, kinds, arrays):
        res = []
        for a, (up, down) in ((0, (wo1, wo2)), (1, (mo1, mo2)), (2, (vo1, vo2))):
            for i, (dst, src) in enumerate(shard_pairs(up, down, layer, mb if a == 0 else dxacc, a)):
                if a in arrays and i // 4 in kinds:
                    res.append(pltpu.make_async_copy(src, dst, o_sem.at[a, i]))
        return res

    def run(copies):
        for cp in copies:
            cp.start()

    def settle(copies):
        for cp in copies:
            cp.wait()

    def lamb_moments(layer, kind):
        @pl.loop(0, 4 - kind)
        def _(j):
            spans = [area(a, kind, j) for a in range(3)]
            grad_sum = g1[:, pl.ds(pl.multiple_of(j * 768, 768), 768)] if kind == 0 else g2[pl.ds(pl.multiple_of(j * SUB, SUB), SUB), :]
            master = mb[spans[0], :]
            mom, var, upd = moments(grad_sum, dxacc[spans[0], :], master, dxacc[spans[1], :], dxacc[spans[2], :])
            dxacc[spans[0], :] = upd
            dxacc[spans[1], :] = mom
            dxacc[spans[2], :] = var
            for i, val in enumerate((master, upd)):
                folded = jnp.sum((val * val).reshape(-1, 8, 768), axis=0)
                lanes = folded[:, 0:128]
                for b in range(1, 6):
                    lanes = lanes + folded[:, b * 128:(b + 1) * 128]
                sqb[layer, kind, i] += lanes

        for i in range(2):
            smine[layer, kind, i:i + 1, :] = jnp.sum(sqb[layer, kind, i], axis=0, keepdims=True)
        run(sum_copies(layer, kind))
        run(lamb_outs(layer, (kind,), (1, 2)))

    def sum_copies(layer, kind):
        return [pltpu.make_async_remote_copy(src_ref=smine.at[layer, kind], dst_ref=sgot.at[layer, kind, i], send_sem=x_snd.at[layer, kind, i], recv_sem=x_rcv.at[layer, kind, i], device_id=(dev,), device_id_type=MESH) for i, dev in enumerate(others)]

    def lamb_apply(layer, kind):
        sgot[layer, kind, 7] = smine[layer, kind]
        settle(sum_copies(layer, kind))
        total = sgot[layer, kind, lax.rem(me + 7, 8)]
        for dev in range(1, 8):
            total = total + sgot[layer, kind, lax.rem(me + 7 - dev + 8, 8)]
        tot[...] = jnp.broadcast_to(jnp.sum(total, axis=1, keepdims=True), (8, 128))
        scale = LEARN_RATE * jnp.sqrt(tot[0:1, 0:1] / tot[1:2, 0:1])

        @pl.loop(0, 4 - kind)
        def _(j):
            span = area(0, kind, j)
            new = mb[span, :] - scale * dxacc[span, :]
            mb[span, :] = new
            half = new.astype(BF16)
            if kind == 1:
                if layer == 1:
                    ws2[j] = half
                else:
                    w2b[j, c, y, x] = half
            else:
                for cc in range(2):
                    lanes = pl.ds(pl.multiple_of((cc * 4 + j) * SUB, SUB), SUB)
                    for k in range(3):
                        piece = half[:, cc * 384 + k * SUB:cc * 384 + (k + 1) * SUB]
                        if layer == 1:
                            ws1[k, :, lanes] = piece
                        else:
                            w1b[k, y, x, c, :, lanes] = piece

        run(lamb_outs(layer, (kind,), (0,)))

    def remote_copy(src, dst, s_sem, r_sem, dev):
        return pltpu.make_async_remote_copy(src_ref=src, dst_ref=dst, send_sem=s_sem, recv_sem=r_sem, device_id=(dev,), device_id_type=MESH)

    def gather_local():
        return pltpu.make_async_copy(ws1, wg1.at[:, y, x, c], ld_sem.at[4])

    def gather2_local():
        return pltpu.make_async_copy(ws2, wg2.at[:, c, y, x], ld_sem.at[5])

    def piece_parts(m, name):
        if m > 8 or (m < 6 and m % 2 == 0):
            ref = w1b.at[m // 2] if m < 6 else wg1.at[m - 9]
            h = 48

            def blk(yy, xx, rows):
                return ref.at[yy, xx, c, rows]
        else:
            ref = w2b.at[m // 2] if m < 6 else wg2.at[m - 6]
            h = 64

            def blk(yy, xx, rows):
                return ref.at[c, yy, xx, rows]
        first, last, every, both = pl.ds(0, h), pl.ds(h, h), pl.ds(0, 2 * h), slice(None)

        def go(part, i, dev):
            return remote_copy(part, part, b_snd.at[m, i], b_rcv.at[m, i], dev)
        if name == 's1':
            return go(blk(y, x, first), 0, xn), go(blk(y, x, last), 1, yn)
        if name == 's2':
            return go(blk(y, both, first), 2, yn), go(blk(both, x, last), 3, xn)
        if name == 'd1':
            return (go(blk(y, x, every), 4, partner),)
        if name == 'd2':
            return go(blk(y, 1 - x, first), 5, partner), go(blk(1 - y, x, last), 6, partner)
        return go(blk(1 - y, both, first), 7, partner), go(blk(both, 1 - x, last), 8, partner)

    def first(m):
        run(piece_parts(m, 's1'))
        run(piece_parts(m, 'd1'))

    def second(m):
        settle(piece_parts(m, 's1'))
        run(piece_parts(m, 's2'))
        run(piece_parts(m, 'd2'))

    def third(m):
        settle(piece_parts(m, 's2'))
        run(piece_parts(m, 'd3'))

    def done(m):
        for name in ('d1', 'd2', 'd3'):
            settle(piece_parts(m, name))

    units = ((p1, r01, r1a1, r1b1, r2a1, r2b1, 48), (p2, r02, r1a2, r1b2, r2a2, r2b2, 64))

    def remote(src, dst, u, slot, stage, dev):
        return pltpu.make_async_remote_copy(src_ref=src, dst_ref=dst, send_sem=snd.at[u, slot, stage], recv_sem=rcv.at[u, slot, stage], device_id=(dev,), device_id_type=MESH)

    def s0(u, slot):
        p, r0, r1a, r1b, r2a, r2b, hr = units[u]
        return remote(p.at[slot, 1 - c], r0.at[slot], u, slot, 0, partner)

    def s1(u, slot):
        p, r0, r1a, r1b, r2a, r2b, hr = units[u]
        return (remote(p.at[slot, c, :, 1 - x, pl.ds(0, hr)], r1a.at[slot], u, slot, 1, xn),
                remote(p.at[slot, c, 1 - y, :, pl.ds(hr, hr)], r1b.at[slot], u, slot, 2, yn))

    def s2(u, slot):
        p, r0, r1a, r1b, r2a, r2b, hr = units[u]
        return (remote(p.at[slot, c, 1 - y, x, pl.ds(0, hr)], r2a.at[slot], u, slot, 3, yn),
                remote(p.at[slot, c, y, 1 - x, pl.ds(hr, hr)], r2b.at[slot], u, slot, 4, xn))

    def start_s0(u, slot):
        s0(u, slot).start()

    def to_s1(u, slot):
        p, r0, r1a, r1b, r2a, r2b, hr = units[u]
        s0(u, slot).wait()

        @pl.loop(0, 2)
        def _(yy):
            for xx in range(2):
                p[slot, c, yy, xx] = (p[slot, c, yy, xx].astype(F32) + r0[slot, yy, xx].astype(F32)).astype(BF16)

        for cp in s1(u, slot):
            cp.start()

    def to_s2(u, slot):
        p, r0, r1a, r1b, r2a, r2b, hr = units[u]
        ca, cb = s1(u, slot)
        ca.wait()
        for i in range(2):
            p[slot, c, i, x, 0:hr] = (p[slot, c, i, x, 0:hr].astype(F32) + r1a[slot, i].astype(F32)).astype(BF16)
        cb.wait()
        for i in range(2):
            p[slot, c, y, i, hr:2 * hr] = (p[slot, c, y, i, hr:2 * hr].astype(F32) + r1b[slot, i].astype(F32)).astype(BF16)
        for cp in s2(u, slot):
            cp.start()

    def finish(u, slot, g):
        p, r0, r1a, r1b, r2a, r2b, hr = units[u]
        k = g % 3
        ca, cb = s2(u, slot)
        for half, (cp, r2) in enumerate(((ca, r2a), (cb, r2b))):
            cp.wait()
            rows = slice(half * hr, half * hr + hr)
            total = p[slot, c, y, x, rows].astype(F32) + r2[slot].astype(F32)
            if u == 1:
                g2[pl.ds(pl.multiple_of(k * SUB + half * hr, 64), hr), :] = total
            else:
                for cc in range(2):
                    for q in range(4):
                        i = cc * 4 + q
                        g1[rows, column(q, cc, k)] = total[:, i * SUB:(i + 1) * SUB]

    settle(loads[:2])

    @pl.loop(0, 6)
    def _(g):
        slot = g % 2
        prev = 1 - slot
        layer = 1 - g // 3
        k = g % 3
        settle(w_copies(g))

        @pl.when(g < 5)
        def _():
            run(w_copies(g + 1))

        @pl.when(g == 3)
        def _():
            loads[2].wait()
            loads[3].start()
            run(lamb_loads(1))

        @pl.when(g == 5)
        def _():
            settle(lamb_outs(1, (0, 1), (0, 1, 2)))
            run(lamb_loads(0))

        def tile(rows):
            xv = xb[layer, rows, :]
            dyv = dyb[rows, :]
            xt[:, rows] = xv.T
            for n in range(CH // 256):
                cs = slice(n * 256, n * 256 + 256)
                h = dot(xv, w1b[k, :, :, :, :, cs].reshape(D, 256))
                da = dot(dyv, w2b[k, n // 2, n % 2].reshape(256, D), NT_DIMS)
                sq = h * h
                s = 0.5 * jnp.tanh(h * (C0 + C1 * sq)) + 0.5
                a = h * s
                gp = s + a * (1.0 - s) * (2.0 * C0 + (6.0 * C1) * sq)
                at[cs, rows] = a.astype(BF16).T
                dhb[rows, cs] = (da * gp).astype(BF16)

        def token_loop(with_dx):
            @pl.loop(0, TOK // (2 * TT))
            def _(t):
                @pl.when((g > 0) & (t == 1))
                def _():
                    to_s1(1, prev)

                if not with_dx:
                    @pl.when((g == 4) & (t == 2))
                    def _():
                        lamb_apply(1, 0)
                        gather_local().start()
                        lamb_apply(1, 1)
                        gather2_local().start()

                    @pl.when((g == 5) & (t == 2))
                    def _():
                        second(9)

                @pl.when((g > 0) & (t == 3))
                def _():
                    to_s2(0, prev)

                base = pl.multiple_of(t * (2 * TT), 2 * TT)
                spans = [pl.ds(base + i * TT, TT) for i in range(2)]
                for rows in spans:
                    tile(rows)
                if with_dx:
                    for rows in spans:
                        dxacc[rows, :] += dot(dhb[rows, :], w1b[k].reshape(D, CH), NT_DIMS)

        @pl.when(layer == 1)
        def _():
            @pl.when(k == 0)
            def _():
                @pl.loop(0, TOK // 128)
                def _(t):
                    rows = pl.ds(pl.multiple_of(t * 128, 128), 128)
                    dxacc[rows, :] = dyb[rows, :].astype(F32)

            token_loop(True)

        @pl.when(layer == 0)
        def _():
            token_loop(False)

        @pl.when(g > 0)
        def _():
            to_s2(1, prev)

        @pl.when(g == 4)
        def _():
            gather_local().wait()
            gather2_local().wait()
            for m in (9, 10, 11):
                first(m)

        @pl.loop(0, CH // 256)
        def _(n):
            fs = pl.ds(pl.multiple_of(n * 256, 256), 256)
            res = dot(xt[...], dhb[:, fs]).astype(BF16)
            for b in range(8):
                p1[slot, b % 2, b // 4, (b // 2) % 2, :, fs] = res[b * 96:(b + 1) * 96]

        start_s0(0, slot)

        @pl.when(g > 0)
        def _():
            finish(0, prev, g - 1)

        @pl.loop(0, CH // 256)
        def _(n):
            fs = pl.ds(pl.multiple_of(n * 256, 256), 256)
            res = dot(at[fs, :], dyb[...]).astype(BF16)
            p2[slot, n // 2, n % 2] = res.reshape(2, SUB, D)

        to_s1(0, slot)
        start_s0(1, slot)

        @pl.when(g > 0)
        def _():
            finish(1, prev, g - 1)

        @pl.when(g == 2)
        def _():
            @pl.loop(0, TOK // TT)
            def _(t):
                rows = pl.ds(pl.multiple_of(t * TT, TT), TT)
                dyb[rows, :] = dxacc[rows, :].astype(BF16)

        @pl.when(g == 3)
        def _():
            settle(lamb_loads(1))
            lamb_moments(1, 0)
            lamb_moments(1, 1)

    to_s1(1, 1)
    to_s2(0, 1)
    to_s2(1, 1)
    first(6)
    settle(lamb_loads(0))
    finish(0, 1, 5)
    lamb_moments(0, 0)
    finish(1, 1, 5)
    lamb_moments(0, 1)
    lamb_apply(0, 0)
    first(0)
    lamb_apply(0, 1)
    first(1)
    second(0)
    first(2)
    second(1)
    first(3)
    first(4)
    third(0)
    second(2)
    first(5)
    third(9)
    loads[3].wait()
    settle(lamb_outs(0, (0, 1), (1, 2)))
    third(1)
    done(0)
    done(1)

    def chunk_load(k, kind):
        if kind == 0:
            return pltpu.make_async_copy(wg1.at[k], w1b.at[k], f_sem.at[k, 0])
        return pltpu.make_async_copy(wg2.at[k], w2b.at[k], f_sem.at[k, 1])

    def out_copy(t):
        rows = pl.ds(pl.multiple_of(t * 512, 512), 512)
        return pltpu.make_async_copy(dyb.at[rows, :], out.at[rows, :], out_sem.at[t])

    def load(k, kind):
        done(9 + k if kind == 0 else 6 + k)
        chunk_load(k, kind).start()

    def ready(k):
        chunk_load(k, 0).wait()
        chunk_load(k, 1).wait()

    def before_1():
        second(5)
        first(7)
        third(3)
        done(2)
        done(3)
        load(0, 0)

    def before_2():
        third(5)
        done(4)
        done(5)
        second(7)
        first(8)
        second(11)

    def before_3():
        load(0, 1)
        third(10)
        ready(0)

    def before_4():
        third(11)
        ready(1)

    def before_5():
        ready(2)

    def f1_t1():
        third(4)
        second(6)

    def f3_t3():
        second(8)
        load(1, 1)

    hooks = {
        (0, 0): lambda: second(3),
        (0, 1): lambda: second(4),
        (0, 3): lambda: third(2),
        (1, 1): f1_t1,
        (1, 2): lambda: second(10),
        (2, 2): lambda: third(6),
        (3, 1): lambda: third(7),
        (3, 2): lambda: load(1, 0),
        (3, 3): f3_t3,
        (4, 1): lambda: load(2, 0),
        (4, 2): lambda: third(8),
        (4, 3): lambda: load(2, 1),
    }

    @pl.loop(0, 6)
    def _(f):
        k = f % 3
        for i, fn in enumerate((before_1, before_2, before_3, before_4, before_5)):
            pl.when(f == i + 1)(fn)

        @pl.when(k == 0)
        def _():
            @pl.loop(0, TOK // 128)
            def _(t):
                rows = pl.ds(pl.multiple_of(t * 128, 128), 128)
                dxacc[rows, :] = xb[1, rows, :].astype(F32)

        @pl.loop(0, TOK // (2 * TT))
        def _(t):
            for (hf, ht), fn in hooks.items():
                pl.when((f == hf) & (t == ht))(fn)
            base = pl.multiple_of(t * (2 * TT), 2 * TT)
            spans = [pl.ds(base + i * TT, TT) for i in range(2)]
            for rows in spans:
                xv = xb[1, rows, :]
                for n in range(CH // 256):
                    cs = slice(n * 256, n * 256 + 256)
                    h = dot(xv, w1b[k, :, :, :, :, cs].reshape(D, 256))
                    s = 0.5 * jnp.tanh(h * (C0 + C1 * (h * h))) + 0.5
                    dhb[rows, cs] = (h * s).astype(BF16)
            for rows in spans:
                dxacc[rows, :] += dot(dhb[rows, :], w2b[k].reshape(CH, D))

            pair = pl.ds(base, 2 * TT)

            @pl.when(f == 2)
            def _():
                xb[1, pair, :] = dxacc[pair, :].astype(BF16)

            @pl.when(f == 5)
            def _():
                dyb[pair, :] = dxacc[pair, :].astype(BF16)
                out_copy(t).start()

    settle(lamb_outs(0, (0, 1), (0,)))
    for t in range(4):
        out_copy(t).wait()


def run_step(*args):
    any_spec = pl.BlockSpec(memory_space=pl.ANY)
    vm = pltpu.VMEM
    dma = pltpu.SemaphoreType.DMA
    up, down = jax.ShapeDtypeStruct((2, 96, FF), F32), jax.ShapeDtypeStruct((2, 384, D), F32)
    return pl.pallas_call(
        step_kernel,
        out_shape=(up, down, up, down, up, down, jax.ShapeDtypeStruct((TOK, D), BF16),
                   jax.ShapeDtypeStruct((3, 2, 2, 2, 96, CH), BF16), jax.ShapeDtypeStruct((3, 2, 2, 2, SUB, D), BF16)),
        in_specs=[any_spec] * 13,
        out_specs=(any_spec,) * 9,
        scratch_shapes=[
            vm((2, TOK, D), BF16), vm((TOK, D), BF16), vm((D, TOK), BF16), vm((3 * 768, D), F32),
            vm((3, 2, 2, 2, 96, CH), BF16), vm((3, 2, 2, 2, SUB, D), BF16), vm((CH, TOK), BF16), vm((TOK, CH), BF16),
            vm((2, 2, 2, 2, 96, CH), BF16), vm((2, 2, 2, 2, SUB, D), BF16),
            vm((2, 2, 2, 96, CH), BF16), vm((2, 2, 2, SUB, D), BF16),
            vm((2, 2, 48, CH), BF16), vm((2, 2, 48, CH), BF16), vm((2, 2, 64, D), BF16), vm((2, 2, 64, D), BF16),
            vm((2, 48, CH), BF16), vm((2, 48, CH), BF16), vm((2, 64, D), BF16), vm((2, 64, D), BF16),
            vm((96, FF), F32), vm((384, D), F32), vm((768, 768), F32), vm((2, 2, 2, 8, 128), F32), vm((2, 2, 8, 128), F32), vm((2, 2, 8, 8, 128), F32), vm((8, 128), F32),
            vm((3, 96, CH), BF16), vm((3, SUB, D), BF16),
            dma((6,)), dma((3, 10)), dma((2, 2, 5)), dma((2, 2, 5)), dma((4, 5)), dma((3, 5)),
            dma((2, 2, 7)), dma((2, 2, 7)), dma((12, 9)), dma((12, 9)), dma((3, 2)), dma((4,)),
        ],
        compiler_params=pltpu.CompilerParams(collective_id=0, has_side_effects=True, vmem_limit_bytes=VMEM_MAX),
        name='step',
    )(*args)


def copy_kernel(*refs):
    src, dst, buf, (sem_in, sem_out) = refs[:7], refs[7:14], refs[14:21], refs[21:]
    order = [(a, i) for i in range(2) for a in range(7)]

    def part(ref, a, i):
        return ref.at[pl.ds(i * (TOK // 2), TOK // 2)] if a == 6 else ref.at[i]

    ins = [pltpu.make_async_copy(part(src[a], a, i), part(buf[a], a, i), sem_in.at[a, i]) for a, i in order]
    outs = [pltpu.make_async_copy(part(buf[a], a, i), part(dst[a], a, i), sem_out.at[a, i]) for a, i in order]
    for cp in ins:
        cp.start()
    for cp, nxt in zip(ins, outs):
        cp.wait()
        nxt.start()
    for cp in outs:
        cp.wait()


def run_copy(arrays):
    any_spec = pl.BlockSpec(memory_space=pl.ANY)
    return pl.pallas_call(
        copy_kernel,
        out_shape=tuple(jax.ShapeDtypeStruct(a.shape, a.dtype) for a in arrays),
        in_specs=[any_spec] * 7,
        out_specs=(any_spec,) * 7,
        scratch_shapes=[pltpu.VMEM(a.shape, a.dtype) for a in arrays] + [pltpu.SemaphoreType.DMA((7, 2)), pltpu.SemaphoreType.DMA((7, 2))],
        compiler_params=pltpu.CompilerParams(vmem_limit_bytes=VMEM_MAX),
        name='copy_out',
    )(*arrays)


def solution(mesh):
    shard_rows = P(None, 'fsdp')
    shard_batch = P('fsdp')
    spec_whole = P()

    def local_step(x_layers, dy_top, x_next, w_up, w_down, acc_up, acc_down, master_up, master_down, mom_up, mom_down, var_up, var_down):
        res = run_step(x_layers.reshape(2, TOK, D), dy_top.reshape(TOK, D), x_next.reshape(TOK, D),
                       w_up.reshape(2, 2, 2, 2, 96, FF), w_down.reshape(2, 2, 2, 2, 3, SUB, D),
                       acc_up, acc_down, master_up, master_down, mom_up, mom_down, var_up, var_down)
        res = run_copy(res[:7])
        return tuple(res[:6]) + (res[6].reshape(1, TOK, D),)

    return jax.shard_map(local_step, mesh=mesh, in_specs=(shard_rows, shard_batch, shard_batch, spec_whole, spec_whole) + (shard_rows,) * 8, out_specs=(shard_rows,) * 6 + (shard_batch,), check_vma=False)
```

```python
import functools

import jax
import jax.numpy as jnp
from jax import lax
from jax.experimental import pallas as pl
from jax.experimental.pallas import tpu as pltpu
from jax.sharding import PartitionSpec as P

MICRO_STEPS = 2
STEP_COUNT = 3
BETA_MOM = 0.9
BETA_VAR = 0.999
ADAM_EPS = 1e-6
WEIGHT_DECAY = 0.01
LEARN_RATE = 0.06

C0 = 0.7978845608028654
C1 = C0 * 0.044715
MESH = pl.DeviceIdType.MESH
BF16 = jnp.bfloat16
F32 = jnp.float32
VMEM_MAX = 67043328

TOK = 2048
D = 768
FF = 3072
SUB = 128
CH = 8 * SUB
TT = 256
NT_DIMS = (((1,), (1,)), ((), ()))
NN_DIMS = (((1,), (0,)), ((), ()))


def position():
    me = lax.axis_index('fsdp')
    y, x, c = me // 4, (me // 2) % 2, me % 2
    return me, y, x, c, me + 1 - 2 * c, me + 2 - 4 * x, me + 4 - 8 * y


def entry_barrier(targets):
    barrier = pltpu.get_barrier_semaphore()
    for dev in targets:
        pl.semaphore_signal(barrier, inc=1, device_id=(dev,), device_id_type=MESH)
    pl.semaphore_wait(barrier, len(targets))


def dot(a, b, dims=NN_DIMS):
    return lax.dot_general(a, b, dims, preferred_element_type=F32)


def moments(grad_sum, acc, master, mom_prev, var_prev):
    grad = (acc + grad_sum) / MICRO_STEPS
    mom = BETA_MOM * mom_prev + (1.0 - BETA_MOM) * grad
    var = BETA_VAR * var_prev + (1.0 - BETA_VAR) * grad * grad
    upd = (mom / (1.0 - BETA_MOM ** STEP_COUNT)) / (jnp.sqrt(var / (1.0 - BETA_VAR ** STEP_COUNT)) + ADAM_EPS) + WEIGHT_DECAY * master
    return mom, var, upd


def step_kernel(x_hbm, dy_hbm, xn_hbm, w1_hbm, w2_hbm, acc1, acc2, mas1, mas2, mom1, mom2, var1, var2,
                wo1, wo2, mo1, mo2, vo1, vo2, out, wg1, wg2,
                xb, dyb, xt, dxacc, w1b, w2b, at, dhb, p1, p2, r01, r02, r1a1, r1b1, r1a2, r1b2, r2a1, r2b1, r2a2, r2b2,
                g1, g2, mb, sqb, smine, sgot, tot, ws1, ws2,
                ld_sem, w_sem, snd, rcv, l_sem, o_sem, x_snd, x_rcv, b_snd, b_rcv, f_sem, out_sem):
    me, y, x, c, partner, xn, yn = position()
    others = [lax.rem(me + i, 8) for i in range(1, 8)]

    def column(q, cc, k):
        return pl.ds(pl.multiple_of((2 * q + cc) * 384 + k * SUB, SUB), SUB)

    def w_copies(g):
        layer = 1 - g // 3
        k = g % 3
        res = []
        for cc in range(2):
            for q in range(4):
                i = cc * 4 + q
                res.append(pltpu.make_async_copy(w1_hbm.at[layer, :, :, :, :, column(q, cc, k)], w1b.at[k, :, :, :, :, pl.ds(i * SUB, SUB)], w_sem.at[k, i]))
            res.append(pltpu.make_async_copy(w2_hbm.at[layer, :, :, cc, k], w2b.at[k, cc], w_sem.at[k, 8 + cc]))
        return res

    loads = [pltpu.make_async_copy(x_hbm.at[1], xb.at[1], ld_sem.at[0]),
             pltpu.make_async_copy(dy_hbm, dyb, ld_sem.at[1]),
             pltpu.make_async_copy(x_hbm.at[0], xb.at[0], ld_sem.at[2]),
             pltpu.make_async_copy(xn_hbm, xb.at[1], ld_sem.at[3])]
    for cp in loads[:2]:
        cp.start()
    for cp in w_copies(0):
        cp.start()
    loads[2].start()

    sqb[...] = jnp.zeros_like(sqb)
    smine[...] = jnp.zeros_like(smine)
    entry_barrier(others)

    def area(a, kind, j):
        return pl.ds(pl.multiple_of(a * 768 + j * 96, 96), 96) if kind == 0 else pl.ds(pl.multiple_of(a * 768 + 384 + j * SUB, SUB), SUB)

    def shard_pairs(up, down, layer, buf, a):
        res = [(up.at[layer, :, pl.ds(j * 768, 768)], buf.at[pl.ds(a * 768 + j * 96, 96), :]) for j in range(4)]
        res.append((down.at[layer], buf.at[pl.ds(a * 768 + 384, 384), :]))
        return res

    def lamb_loads(layer):
        res = []
        for a, (up, down) in enumerate(((acc1, acc2), (mom1, mom2), (var1, var2), (mas1, mas2))):
            for i, (src, dst) in enumerate(shard_pairs(up, down, layer, dxacc if a < 3 else mb, a % 3)):
                res.append(pltpu.make_async_copy(src, dst, l_sem.at[a, i]))
        return res

    def lamb_outs(layer, kinds, arrays):
        res = []
        for a, (up, down) in ((0, (wo1, wo2)), (1, (mo1, mo2)), (2, (vo1, vo2))):
            for i, (dst, src) in enumerate(shard_pairs(up, down, layer, mb if a == 0 else dxacc, a)):
                if a in arrays and i // 4 in kinds:
                    res.append(pltpu.make_async_copy(src, dst, o_sem.at[a, i]))
        return res

    def run(copies):
        for cp in copies:
            cp.start()

    def settle(copies):
        for cp in copies:
            cp.wait()

    def lamb_moments(layer, kind):
        @pl.loop(0, 4 - kind)
        def _(j):
            spans = [area(a, kind, j) for a in range(3)]
            grad_sum = g1[:, pl.ds(pl.multiple_of(j * 768, 768), 768)] if kind == 0 else g2[pl.ds(pl.multiple_of(j * SUB, SUB), SUB), :]
            master = mb[spans[0], :]
            mom, var, upd = moments(grad_sum, dxacc[spans[0], :], master, dxacc[spans[1], :], dxacc[spans[2], :])
            dxacc[spans[0], :] = upd
            dxacc[spans[1], :] = mom
            dxacc[spans[2], :] = var
            for i, val in enumerate((master, upd)):
                folded = jnp.sum((val * val).reshape(-1, 8, 768), axis=0)
                lanes = folded[:, 0:128]
                for b in range(1, 6):
                    lanes = lanes + folded[:, b * 128:(b + 1) * 128]
                sqb[layer, kind, i] += lanes

        for i in range(2):
            smine[layer, kind, i:i + 1, :] = jnp.sum(sqb[layer, kind, i], axis=0, keepdims=True)
        run(sum_copies(layer, kind))
        run(lamb_outs(layer, (kind,), (1, 2)))

    def sum_copies(layer, kind):
        return [pltpu.make_async_remote_copy(src_ref=smine.at[layer, kind], dst_ref=sgot.at[layer, kind, i], send_sem=x_snd.at[layer, kind, i], recv_sem=x_rcv.at[layer, kind, i], device_id=(dev,), device_id_type=MESH) for i, dev in enumerate(others)]

    def lamb_apply(layer, kind):
        sgot[layer, kind, 7] = smine[layer, kind]
        settle(sum_copies(layer, kind))
        total = sgot[layer, kind, lax.rem(me + 7, 8)]
        for dev in range(1, 8):
            total = total + sgot[layer, kind, lax.rem(me + 7 - dev + 8, 8)]
        tot[...] = jnp.broadcast_to(jnp.sum(total, axis=1, keepdims=True), (8, 128))
        scale = LEARN_RATE * jnp.sqrt(tot[0:1, 0:1] / tot[1:2, 0:1])

        @pl.loop(0, 4 - kind)
        def _(j):
            span = area(0, kind, j)
            new = mb[span, :] - scale * dxacc[span, :]
            mb[span, :] = new
            half = new.astype(BF16)
            if kind == 1:
                if layer == 1:
                    ws2[j] = half
                else:
                    w2b[j, c, y, x] = half
            else:
                for cc in range(2):
                    lanes = pl.ds(pl.multiple_of((cc * 4 + j) * SUB, SUB), SUB)
                    for k in range(3):
                        piece = half[:, cc * 384 + k * SUB:cc * 384 + (k + 1) * SUB]
                        if layer == 1:
                            ws1[k, :, lanes] = piece
                        else:
                            w1b[k, y, x, c, :, lanes] = piece

        run(lamb_outs(layer, (kind,), (0,)))

    def remote_copy(src, dst, s_sem, r_sem, dev):
        return pltpu.make_async_remote_copy(src_ref=src, dst_ref=dst, send_sem=s_sem, recv_sem=r_sem, device_id=(dev,), device_id_type=MESH)

    def gather_local():
        return pltpu.make_async_copy(ws1, wg1.at[:, y, x, c], ld_sem.at[4])

    def gather2_local():
        return pltpu.make_async_copy(ws2, wg2.at[:, c, y, x], ld_sem.at[5])

    def piece_parts(m, name):
        if m > 8 or (m < 6 and m % 2 == 0):
            ref = w1b.at[m // 2] if m < 6 else wg1.at[m - 9]
            h = 48

            def blk(yy, xx, rows):
                return ref.at[yy, xx, c, rows]
        else:
            ref = w2b.at[m // 2] if m < 6 else wg2.at[m - 6]
            h = 64

            def blk(yy, xx, rows):
                return ref.at[c, yy, xx, rows]
        first, last, every, both = pl.ds(0, h), pl.ds(h, h), pl.ds(0, 2 * h), slice(None)

        def go(part, i, dev):
            return remote_copy(part, part, b_snd.at[m, i], b_rcv.at[m, i], dev)
        if name == 's1':
            return go(blk(y, x, first), 0, xn), go(blk(y, x, last), 1, yn)
        if name == 's2':
            return go(blk(y, both, first), 2, yn), go(blk(both, x, last), 3, xn)
        if name == 'd1':
            return (go(blk(y, x, every), 4, partner),)
        if name == 'd2':
            return go(blk(y, 1 - x, first), 5, partner), go(blk(1 - y, x, last), 6, partner)
        return go(blk(1 - y, both, first), 7, partner), go(blk(both, 1 - x, last), 8, partner)

    def first(m):
        run(piece_parts(m, 's1'))
        run(piece_parts(m, 'd1'))

    def second(m):
        settle(piece_parts(m, 's1'))
        run(piece_parts(m, 's2'))
        run(piece_parts(m, 'd2'))

    def third(m):
        settle(piece_parts(m, 's2'))
        run(piece_parts(m, 'd3'))

    def done(m):
        for name in ('d1', 'd2', 'd3'):
            settle(piece_parts(m, name))

    units = ((p1, r01, r1a1, r1b1, r2a1, r2b1, 48), (p2, r02, r1a2, r1b2, r2a2, r2b2, 64))

    def remote(src, dst, u, slot, stage, dev):
        return pltpu.make_async_remote_copy(src_ref=src, dst_ref=dst, send_sem=snd.at[u, slot, stage], recv_sem=rcv.at[u, slot, stage], device_id=(dev,), device_id_type=MESH)

    def s0(u, slot):
        p, r0, r1a, r1b, r2a, r2b, hr = units[u]
        return remote(p.at[slot, 1 - c], r0.at[slot], u, slot, 0, partner)

    def s1(u, slot):
        p, r0, r1a, r1b, r2a, r2b, hr = units[u]
        return (remote(p.at[slot, c, :, 1 - x, pl.ds(0, hr)], r1a.at[slot], u, slot, 1, xn),
                remote(p.at[slot, c, 1 - y, :, pl.ds(hr, hr)], r1b.at[slot], u, slot, 2, yn))

    def s2(u, slot):
        p, r0, r1a, r1b, r2a, r2b, hr = units[u]
        return (remote(p.at[slot, c, 1 - y, x, pl.ds(0, hr)], r2a.at[slot], u, slot, 3, yn),
                remote(p.at[slot, c, y, 1 - x, pl.ds(hr, hr)], r2b.at[slot], u, slot, 4, xn))

    def start_s0(u, slot):
        s0(u, slot).start()

    def to_s1(u, slot):
        p, r0, r1a, r1b, r2a, r2b, hr = units[u]
        s0(u, slot).wait()

        @pl.loop(0, 2)
        def _(yy):
            for xx in range(2):
                p[slot, c, yy, xx] = (p[slot, c, yy, xx].astype(F32) + r0[slot, yy, xx].astype(F32)).astype(BF16)

        for cp in s1(u, slot):
            cp.start()

    def to_s2(u, slot):
        p, r0, r1a, r1b, r2a, r2b, hr = units[u]
        ca, cb = s1(u, slot)
        ca.wait()
        for i in range(2):
            p[slot, c, i, x, 0:hr] = (p[slot, c, i, x, 0:hr].astype(F32) + r1a[slot, i].astype(F32)).astype(BF16)
        cb.wait()
        for i in range(2):
            p[slot, c, y, i, hr:2 * hr] = (p[slot, c, y, i, hr:2 * hr].astype(F32) + r1b[slot, i].astype(F32)).astype(BF16)
        for cp in s2(u, slot):
            cp.start()

    def finish(u, slot, g):
        p, r0, r1a, r1b, r2a, r2b, hr = units[u]
        k = g % 3
        ca, cb = s2(u, slot)
        for half, (cp, r2) in enumerate(((ca, r2a), (cb, r2b))):
            cp.wait()
            rows = slice(half * hr, half * hr + hr)
            total = p[slot, c, y, x, rows].astype(F32) + r2[slot].astype(F32)
            if u == 1:
                g2[pl.ds(pl.multiple_of(k * SUB + half * hr, 64), hr), :] = total
            else:
                for cc in range(2):
                    for q in range(4):
                        i = cc * 4 + q
                        g1[rows, column(q, cc, k)] = total[:, i * SUB:(i + 1) * SUB]

    settle(loads[:2])

    @pl.loop(0, 6)
    def _(g):
        slot = g % 2
        prev = 1 - slot
        layer = 1 - g // 3
        k = g % 3
        settle(w_copies(g))

        @pl.when(g < 5)
        def _():
            run(w_copies(g + 1))

        @pl.when(g == 3)
        def _():
            loads[2].wait()
            loads[3].start()
            run(lamb_loads(1))

        @pl.when(g == 5)
        def _():
            settle(lamb_outs(1, (0, 1), (0, 1, 2)))
            run(lamb_loads(0))

        def tile(rows):
            xv = xb[layer, rows, :]
            dyv = dyb[rows, :]
            xt[:, rows] = xv.T
            for n in range(CH // 256):
                cs = slice(n * 256, n * 256 + 256)
                h = dot(xv, w1b[k, :, :, :, :, cs].reshape(D, 256))
                da = dot(dyv, w2b[k, n // 2, n % 2].reshape(256, D), NT_DIMS)
                sq = h * h
                s = 0.5 * jnp.tanh(h * (C0 + C1 * sq)) + 0.5
                a = h * s
                gp = s + a * (1.0 - s) * (2.0 * C0 + (6.0 * C1) * sq)
                at[cs, rows] = a.astype(BF16).T
                dhb[rows, cs] = (da * gp).astype(BF16)

        def token_loop(with_dx):
            @pl.loop(0, TOK // (2 * TT))
            def _(t):
                @pl.when((g > 0) & (t == 1))
                def _():
                    to_s1(1, prev)

                if not with_dx:
                    @pl.when((g == 4) & (t == 2))
                    def _():
                        lamb_apply(1, 0)
                        gather_local().start()
                        lamb_apply(1, 1)
                        gather2_local().start()

                    @pl.when((g == 5) & (t == 2))
                    def _():
                        second(9)

                @pl.when((g > 0) & (t == 3))
                def _():
                    to_s2(0, prev)

                base = pl.multiple_of(t * (2 * TT), 2 * TT)
                spans = [pl.ds(base + i * TT, TT) for i in range(2)]
                for rows in spans:
                    tile(rows)
                if with_dx:
                    for rows in spans:
                        dxacc[rows, :] += dot(dhb[rows, :], w1b[k].reshape(D, CH), NT_DIMS)

        @pl.when(layer == 1)
        def _():
            @pl.when(k == 0)
            def _():
                @pl.loop(0, TOK // 128)
                def _(t):
                    rows = pl.ds(pl.multiple_of(t * 128, 128), 128)
                    dxacc[rows, :] = dyb[rows, :].astype(F32)

            token_loop(True)

        @pl.when(layer == 0)
        def _():
            token_loop(False)

        @pl.when(g > 0)
        def _():
            to_s2(1, prev)

        @pl.when(g == 4)
        def _():
            gather_local().wait()
            gather2_local().wait()
            for m in (9, 10, 11):
                first(m)

        for n in range(CH // 256):
            fs = slice(n * 256, n * 256 + 256)
            res = dot(xt[...], dhb[:, fs]).astype(BF16)
            for b in range(8):
                p1[slot, b % 2, b // 4, (b // 2) % 2, :, fs] = res[b * 96:(b + 1) * 96]

        start_s0(0, slot)

        for n in range(CH // 256):
            res = dot(at[n * 256:n * 256 + 256, :], dyb[...]).astype(BF16)
            p2[slot, n // 2, n % 2] = res.reshape(2, SUB, D)

        to_s1(0, slot)
        start_s0(1, slot)

        @pl.when(g > 0)
        def _():
            finish(0, prev, g - 1)
            finish(1, prev, g - 1)

        @pl.when(g == 2)
        def _():
            @pl.loop(0, TOK // TT)
            def _(t):
                rows = pl.ds(pl.multiple_of(t * TT, TT), TT)
                dyb[rows, :] = dxacc[rows, :].astype(BF16)

        @pl.when(g == 3)
        def _():
            settle(lamb_loads(1))
            lamb_moments(1, 0)
            lamb_moments(1, 1)

    to_s1(1, 1)
    to_s2(0, 1)
    to_s2(1, 1)
    first(6)
    settle(lamb_loads(0))
    finish(0, 1, 5)
    lamb_moments(0, 0)
    finish(1, 1, 5)
    lamb_moments(0, 1)
    lamb_apply(0, 0)
    first(0)
    lamb_apply(0, 1)
    first(1)
    second(0)
    first(2)
    second(1)
    first(3)
    first(4)
    third(0)
    second(2)
    first(5)
    third(9)
    loads[3].wait()
    settle(lamb_outs(0, (0, 1), (1, 2)))
    third(1)
    done(0)
    done(1)

    def chunk_load(k, kind):
        if kind == 0:
            return pltpu.make_async_copy(wg1.at[k], w1b.at[k], f_sem.at[k, 0])
        return pltpu.make_async_copy(wg2.at[k], w2b.at[k], f_sem.at[k, 1])

    def out_copy(t):
        rows = pl.ds(pl.multiple_of(t * 512, 512), 512)
        return pltpu.make_async_copy(dyb.at[rows, :], out.at[rows, :], out_sem.at[t])

    def load(k, kind):
        done(9 + k if kind == 0 else 6 + k)
        chunk_load(k, kind).start()

    def ready(k):
        chunk_load(k, 0).wait()
        chunk_load(k, 1).wait()

    def before_1():
        second(5)
        first(7)
        third(3)
        done(2)
        done(3)
        load(0, 0)

    def before_2():
        third(5)
        done(4)
        done(5)
        second(7)
        first(8)
        second(11)

    def before_3():
        load(0, 1)
        third(10)
        ready(0)

    def before_4():
        third(11)
        ready(1)

    def before_5():
        ready(2)

    def f1_t1():
        third(4)
        second(6)

    def f3_t3():
        second(8)
        load(1, 1)

    hooks = {
        (0, 0): lambda: second(3),
        (0, 1): lambda: second(4),
        (0, 3): lambda: third(2),
        (1, 1): f1_t1,
        (1, 2): lambda: second(10),
        (2, 2): lambda: third(6),
        (3, 1): lambda: third(7),
        (3, 2): lambda: load(1, 0),
        (3, 3): f3_t3,
        (4, 1): lambda: load(2, 0),
        (4, 2): lambda: third(8),
        (4, 3): lambda: load(2, 1),
    }

    @pl.loop(0, 6)
    def _(f):
        k = f % 3
        for i, fn in enumerate((before_1, before_2, before_3, before_4, before_5)):
            pl.when(f == i + 1)(fn)

        @pl.when(k == 0)
        def _():
            @pl.loop(0, TOK // 128)
            def _(t):
                rows = pl.ds(pl.multiple_of(t * 128, 128), 128)
                dxacc[rows, :] = xb[1, rows, :].astype(F32)

        @pl.loop(0, TOK // (2 * TT))
        def _(t):
            for (hf, ht), fn in hooks.items():
                pl.when((f == hf) & (t == ht))(fn)
            base = pl.multiple_of(t * (2 * TT), 2 * TT)
            spans = [pl.ds(base + i * TT, TT) for i in range(2)]
            for rows in spans:
                xv = xb[1, rows, :]
                for n in range(CH // 256):
                    cs = slice(n * 256, n * 256 + 256)
                    h = dot(xv, w1b[k, :, :, :, :, cs].reshape(D, 256))
                    s = 0.5 * jnp.tanh(h * (C0 + C1 * (h * h))) + 0.5
                    dhb[rows, cs] = (h * s).astype(BF16)
            for rows in spans:
                dxacc[rows, :] += dot(dhb[rows, :], w2b[k].reshape(CH, D))

            pair = pl.ds(base, 2 * TT)

            @pl.when(f == 2)
            def _():
                xb[1, pair, :] = dxacc[pair, :].astype(BF16)

            @pl.when(f == 5)
            def _():
                dyb[pair, :] = dxacc[pair, :].astype(BF16)
                out_copy(t).start()

    settle(lamb_outs(0, (0, 1), (0,)))
    for t in range(4):
        out_copy(t).wait()


def run_step(*args):
    any_spec = pl.BlockSpec(memory_space=pl.ANY)
    vm = pltpu.VMEM
    dma = pltpu.SemaphoreType.DMA
    up, down = jax.ShapeDtypeStruct((2, 96, FF), F32), jax.ShapeDtypeStruct((2, 384, D), F32)
    return pl.pallas_call(
        step_kernel,
        out_shape=(up, down, up, down, up, down, jax.ShapeDtypeStruct((TOK, D), BF16),
                   jax.ShapeDtypeStruct((3, 2, 2, 2, 96, CH), BF16), jax.ShapeDtypeStruct((3, 2, 2, 2, SUB, D), BF16)),
        in_specs=[any_spec] * 13,
        out_specs=(any_spec,) * 9,
        scratch_shapes=[
            vm((2, TOK, D), BF16), vm((TOK, D), BF16), vm((D, TOK), BF16), vm((3 * 768, D), F32),
            vm((3, 2, 2, 2, 96, CH), BF16), vm((3, 2, 2, 2, SUB, D), BF16), vm((CH, TOK), BF16), vm((TOK, CH), BF16),
            vm((2, 2, 2, 2, 96, CH), BF16), vm((2, 2, 2, 2, SUB, D), BF16),
            vm((2, 2, 2, 96, CH), BF16), vm((2, 2, 2, SUB, D), BF16),
            vm((2, 2, 48, CH), BF16), vm((2, 2, 48, CH), BF16), vm((2, 2, 64, D), BF16), vm((2, 2, 64, D), BF16),
            vm((2, 48, CH), BF16), vm((2, 48, CH), BF16), vm((2, 64, D), BF16), vm((2, 64, D), BF16),
            vm((96, FF), F32), vm((384, D), F32), vm((768, 768), F32), vm((2, 2, 2, 8, 128), F32), vm((2, 2, 8, 128), F32), vm((2, 2, 8, 8, 128), F32), vm((8, 128), F32),
            vm((3, 96, CH), BF16), vm((3, SUB, D), BF16),
            dma((6,)), dma((3, 10)), dma((2, 2, 5)), dma((2, 2, 5)), dma((4, 5)), dma((3, 5)),
            dma((2, 2, 7)), dma((2, 2, 7)), dma((12, 9)), dma((12, 9)), dma((3, 2)), dma((4,)),
        ],
        compiler_params=pltpu.CompilerParams(collective_id=0, has_side_effects=True, vmem_limit_bytes=VMEM_MAX),
        name='step',
    )(*args)


def copy_kernel(*refs):
    src, dst, buf, (sem_in, sem_out) = refs[:7], refs[7:14], refs[14:21], refs[21:]
    order = [(a, i) for i in range(2) for a in range(7)]

    def part(ref, a, i):
        return ref.at[pl.ds(i * (TOK // 2), TOK // 2)] if a == 6 else ref.at[i]

    ins = [pltpu.make_async_copy(part(src[a], a, i), part(buf[a], a, i), sem_in.at[a, i]) for a, i in order]
    outs = [pltpu.make_async_copy(part(buf[a], a, i), part(dst[a], a, i), sem_out.at[a, i]) for a, i in order]
    for cp in ins:
        cp.start()
    for cp, nxt in zip(ins, outs):
        cp.wait()
        nxt.start()
    for cp in outs:
        cp.wait()


def run_copy(arrays):
    any_spec = pl.BlockSpec(memory_space=pl.ANY)
    return pl.pallas_call(
        copy_kernel,
        out_shape=tuple(jax.ShapeDtypeStruct(a.shape, a.dtype) for a in arrays),
        in_specs=[any_spec] * 7,
        out_specs=(any_spec,) * 7,
        scratch_shapes=[pltpu.VMEM(a.shape, a.dtype) for a in arrays] + [pltpu.SemaphoreType.DMA((7, 2)), pltpu.SemaphoreType.DMA((7, 2))],
        compiler_params=pltpu.CompilerParams(vmem_limit_bytes=VMEM_MAX),
        name='copy_out',
    )(*arrays)


def solution(mesh):
    shard_rows = P(None, 'fsdp')
    shard_batch = P('fsdp')
    spec_whole = P()

    def local_step(x_layers, dy_top, x_next, w_up, w_down, acc_up, acc_down, master_up, master_down, mom_up, mom_down, var_up, var_down):
        res = run_step(x_layers.reshape(2, TOK, D), dy_top.reshape(TOK, D), x_next.reshape(TOK, D),
                       w_up.reshape(2, 2, 2, 2, 96, FF), w_down.reshape(2, 2, 2, 2, 3, SUB, D),
                       acc_up, acc_down, master_up, master_down, mom_up, mom_down, var_up, var_down)
        res = run_copy(res[:7])
        return tuple(res[:6]) + (res[6].reshape(1, TOK, D),)

    return jax.shard_map(local_step, mesh=mesh, in_specs=(shard_rows, shard_batch, shard_batch, spec_whole, spec_whole) + (shard_rows,) * 8, out_specs=(shard_rows,) * 6 + (shard_batch,), check_vma=False)
```

```python
import functools

import jax
import jax.numpy as jnp
from jax import lax
from jax.experimental import pallas as pl
from jax.experimental.pallas import tpu as pltpu
from jax.sharding import PartitionSpec as P

MICRO_STEPS = 2
STEP_COUNT = 3
BETA_MOM = 0.9
BETA_VAR = 0.999
ADAM_EPS = 1e-6
WEIGHT_DECAY = 0.01
LEARN_RATE = 0.06

C0 = 0.7978845608028654
C1 = C0 * 0.044715
MESH = pl.DeviceIdType.MESH
BF16 = jnp.bfloat16
F32 = jnp.float32
VMEM_MAX = 67043328

TOK = 2048
D = 768
FF = 3072
SUB = 128
CH = 8 * SUB
TT = 256
NT_DIMS = (((1,), (1,)), ((), ()))
NN_DIMS = (((1,), (0,)), ((), ()))


def position():
    me = lax.axis_index('fsdp')
    y, x, c = me // 4, (me // 2) % 2, me % 2
    return me, y, x, c, me + 1 - 2 * c, me + 2 - 4 * x, me + 4 - 8 * y


def entry_barrier(targets):
    barrier = pltpu.get_barrier_semaphore()
    for dev in targets:
        pl.semaphore_signal(barrier, inc=1, device_id=(dev,), device_id_type=MESH)
    pl.semaphore_wait(barrier, len(targets))


def dot(a, b, dims=NN_DIMS):
    return lax.dot_general(a, b, dims, preferred_element_type=F32)


def moments(grad_sum, acc, master, mom_prev, var_prev):
    grad = (acc + grad_sum) / MICRO_STEPS
    mom = BETA_MOM * mom_prev + (1.0 - BETA_MOM) * grad
    var = BETA_VAR * var_prev + (1.0 - BETA_VAR) * grad * grad
    upd = (mom / (1.0 - BETA_MOM ** STEP_COUNT)) / (jnp.sqrt(var / (1.0 - BETA_VAR ** STEP_COUNT)) + ADAM_EPS) + WEIGHT_DECAY * master
    return mom, var, upd


def step_kernel(x_hbm, dy_hbm, xn_hbm, w1_hbm, w2_hbm, acc1, acc2, mas1, mas2, mom1, mom2, var1, var2,
                wo1, wo2, mo1, mo2, vo1, vo2, out, wg1, wg2,
                xb, dyb, xt, dxacc, w1b, w2b, at, dhb, p1, p2, r01, r02, r1a1, r1b1, r1a2, r1b2, r2a1, r2b1, r2a2, r2b2,
                g1, g2, mb, sqb, smine, sgot, tot, ws1, ws2,
                ld_sem, w_sem, snd, rcv, l_sem, o_sem, x_snd, x_rcv, b_snd, b_rcv, f_sem, out_sem):
    me, y, x, c, partner, xn, yn = position()
    others = [lax.rem(me + i, 8) for i in range(1, 8)]

    def column(q, cc, k):
        return pl.ds(pl.multiple_of((2 * q + cc) * 384 + k * SUB, SUB), SUB)

    def w_copies(g):
        layer = 1 - g // 3
        k = g % 3
        res = []
        for cc in range(2):
            for q in range(4):
                i = cc * 4 + q
                res.append(pltpu.make_async_copy(w1_hbm.at[layer, :, :, :, :, column(q, cc, k)], w1b.at[k, :, :, :, :, pl.ds(i * SUB, SUB)], w_sem.at[k, i]))
            res.append(pltpu.make_async_copy(w2_hbm.at[layer, :, :, cc, k], w2b.at[k, cc], w_sem.at[k, 8 + cc]))
        return res

    loads = [pltpu.make_async_copy(x_hbm.at[1], xb.at[1], ld_sem.at[0]),
             pltpu.make_async_copy(dy_hbm, dyb, ld_sem.at[1]),
             pltpu.make_async_copy(x_hbm.at[0], xb.at[0], ld_sem.at[2]),
             pltpu.make_async_copy(xn_hbm, xb.at[1], ld_sem.at[3])]
    for cp in loads[:2]:
        cp.start()
    for cp in w_copies(0):
        cp.start()
    sqb[...] = jnp.zeros_like(sqb)
    smine[...] = jnp.zeros_like(smine)
    entry_barrier(others)

    def area(a, kind, j):
        return pl.ds(pl.multiple_of(a * 768 + j * 96, 96), 96) if kind == 0 else pl.ds(pl.multiple_of(a * 768 + 384 + j * SUB, SUB), SUB)

    def shard_pairs(up, down, layer, buf, a):
        res = [(up.at[layer, :, pl.ds(j * 768, 768)], buf.at[pl.ds(a * 768 + j * 96, 96), :]) for j in range(4)]
        res.append((down.at[layer], buf.at[pl.ds(a * 768 + 384, 384), :]))
        return res

    def lamb_loads(layer):
        res = []
        for a, (up, down) in enumerate(((acc1, acc2), (mom1, mom2), (var1, var2), (mas1, mas2))):
            for i, (src, dst) in enumerate(shard_pairs(up, down, layer, dxacc if a < 3 else mb, a % 3)):
                res.append(pltpu.make_async_copy(src, dst, l_sem.at[a, i]))
        return res

    def lamb_outs(layer, kinds, arrays):
        res = []
        for a, (up, down) in ((0, (wo1, wo2)), (1, (mo1, mo2)), (2, (vo1, vo2))):
            for i, (dst, src) in enumerate(shard_pairs(up, down, layer, mb if a == 0 else dxacc, a)):
                if a in arrays and i // 4 in kinds:
                    res.append(pltpu.make_async_copy(src, dst, o_sem.at[a, i]))
        return res

    def run(copies):
        for cp in copies:
            cp.start()

    def settle(copies):
        for cp in copies:
            cp.wait()

    def lamb_moments(layer, kind):
        @pl.loop(0, 4 - kind)
        def _(j):
            spans = [area(a, kind, j) for a in range(3)]
            grad_sum = g1[:, pl.ds(pl.multiple_of(j * 768, 768), 768)] if kind == 0 else g2[pl.ds(pl.multiple_of(j * SUB, SUB), SUB), :]
            master = mb[spans[0], :]
            mom, var, upd = moments(grad_sum, dxacc[spans[0], :], master, dxacc[spans[1], :], dxacc[spans[2], :])
            dxacc[spans[0], :] = upd
            dxacc[spans[1], :] = mom
            dxacc[spans[2], :] = var
            for i, val in enumerate((master, upd)):
                folded = jnp.sum((val * val).reshape(-1, 8, 768), axis=0)
                lanes = folded[:, 0:128]
                for b in range(1, 6):
                    lanes = lanes + folded[:, b * 128:(b + 1) * 128]
                sqb[layer, kind, i] += lanes

        for i in range(2):
            smine[layer, kind, i:i + 1, :] = jnp.sum(sqb[layer, kind, i], axis=0, keepdims=True)
        run(sum_copies(layer, kind))
        run(lamb_outs(layer, (kind,), (1, 2)))

    def sum_copies(layer, kind):
        return [pltpu.make_async_remote_copy(src_ref=smine.at[layer, kind], dst_ref=sgot.at[layer, kind, i], send_sem=x_snd.at[layer, kind, i], recv_sem=x_rcv.at[layer, kind, i], device_id=(dev,), device_id_type=MESH) for i, dev in enumerate(others)]

    def lamb_apply(layer, kind):
        sgot[layer, kind, 7] = smine[layer, kind]
        settle(sum_copies(layer, kind))
        total = sgot[layer, kind, lax.rem(me + 7, 8)]
        for dev in range(1, 8):
            total = total + sgot[layer, kind, lax.rem(me + 7 - dev + 8, 8)]
        tot[...] = jnp.broadcast_to(jnp.sum(total, axis=1, keepdims=True), (8, 128))
        scale = LEARN_RATE * jnp.sqrt(tot[0:1, 0:1] / tot[1:2, 0:1])

        @pl.loop(0, 4 - kind)
        def _(j):
            span = area(0, kind, j)
            new = mb[span, :] - scale * dxacc[span, :]
            mb[span, :] = new
            half = new.astype(BF16)
            if kind == 1:
                if layer == 1:
                    ws2[j] = half
                else:
                    w2b[j, c, y, x] = half
            else:
                for cc in range(2):
                    lanes = pl.ds(pl.multiple_of((cc * 4 + j) * SUB, SUB), SUB)
                    for k in range(3):
                        piece = half[:, cc * 384 + k * SUB:cc * 384 + (k + 1) * SUB]
                        if layer == 1:
                            ws1[k, :, lanes] = piece
                        else:
                            w1b[k, y, x, c, :, lanes] = piece

        run(lamb_outs(layer, (kind,), (0,)))

    def remote_copy(src, dst, s_sem, r_sem, dev):
        return pltpu.make_async_remote_copy(src_ref=src, dst_ref=dst, send_sem=s_sem, recv_sem=r_sem, device_id=(dev,), device_id_type=MESH)

    def gather_local():
        return pltpu.make_async_copy(ws1, wg1.at[:, y, x, c], ld_sem.at[4])

    def gather2_local():
        return pltpu.make_async_copy(ws2, wg2.at[:, c, y, x], ld_sem.at[5])

    def piece_parts(m, name):
        if m > 8 or (m < 6 and m % 2 == 0):
            ref = w1b.at[m // 2] if m < 6 else wg1.at[m - 9]
            h = 48

            def blk(yy, xx, rows):
                return ref.at[yy, xx, c, rows]
        else:
            ref = w2b.at[m // 2] if m < 6 else wg2.at[m - 6]
            h = 64

            def blk(yy, xx, rows):
                return ref.at[c, yy, xx, rows]
        first, last, every, both = pl.ds(0, h), pl.ds(h, h), pl.ds(0, 2 * h), slice(None)

        def go(part, i, dev):
            return remote_copy(part, part, b_snd.at[m, i], b_rcv.at[m, i], dev)
        if name == 's1':
            return go(blk(y, x, first), 0, xn), go(blk(y, x, last), 1, yn)
        if name == 's2':
            return go(blk(y, both, first), 2, yn), go(blk(both, x, last), 3, xn)
        if name == 'd1':
            return (go(blk(y, x, every), 4, partner),)
        if name == 'd2':
            return go(blk(y, 1 - x, first), 5, partner), go(blk(1 - y, x, last), 6, partner)
        return go(blk(1 - y, both, first), 7, partner), go(blk(both, 1 - x, last), 8, partner)

    def first(m):
        run(piece_parts(m, 's1'))
        run(piece_parts(m, 'd1'))

    def second(m):
        settle(piece_parts(m, 's1'))
        run(piece_parts(m, 's2'))
        run(piece_parts(m, 'd2'))

    def third(m):
        settle(piece_parts(m, 's2'))
        run(piece_parts(m, 'd3'))

    def done(m):
        for name in ('d1', 'd2', 'd3'):
            settle(piece_parts(m, name))

    units = ((p1, r01, r1a1, r1b1, r2a1, r2b1, 48), (p2, r02, r1a2, r1b2, r2a2, r2b2, 64))

    def remote(src, dst, u, slot, stage, dev):
        return pltpu.make_async_remote_copy(src_ref=src, dst_ref=dst, send_sem=snd.at[u, slot, stage], recv_sem=rcv.at[u, slot, stage], device_id=(dev,), device_id_type=MESH)

    def s0(u, slot):
        p, r0, r1a, r1b, r2a, r2b, hr = units[u]
        return remote(p.at[slot, 1 - c], r0.at[slot], u, slot, 0, partner)

    def s1(u, slot):
        p, r0, r1a, r1b, r2a, r2b, hr = units[u]
        return (remote(p.at[slot, c, :, 1 - x, pl.ds(0, hr)], r1a.at[slot], u, slot, 1, xn),
                remote(p.at[slot, c, 1 - y, :, pl.ds(hr, hr)], r1b.at[slot], u, slot, 2, yn))

    def s2(u, slot):
        p, r0, r1a, r1b, r2a, r2b, hr = units[u]
        return (remote(p.at[slot, c, 1 - y, x, pl.ds(0, hr)], r2a.at[slot], u, slot, 3, yn),
                remote(p.at[slot, c, y, 1 - x, pl.ds(hr, hr)], r2b.at[slot], u, slot, 4, xn))

    def start_s0(u, slot):
        s0(u, slot).start()

    def to_s1(u, slot):
        p, r0, r1a, r1b, r2a, r2b, hr = units[u]
        s0(u, slot).wait()

        @pl.loop(0, 2)
        def _(yy):
            for xx in range(2):
                p[slot, c, yy, xx] = (p[slot, c, yy, xx].astype(F32) + r0[slot, yy, xx].astype(F32)).astype(BF16)

        for cp in s1(u, slot):
            cp.start()

    def to_s2(u, slot):
        p, r0, r1a, r1b, r2a, r2b, hr = units[u]
        ca, cb = s1(u, slot)
        ca.wait()
        for i in range(2):
            p[slot, c, i, x, 0:hr] = (p[slot, c, i, x, 0:hr].astype(F32) + r1a[slot, i].astype(F32)).astype(BF16)
        cb.wait()
        for i in range(2):
            p[slot, c, y, i, hr:2 * hr] = (p[slot, c, y, i, hr:2 * hr].astype(F32) + r1b[slot, i].astype(F32)).astype(BF16)
        for cp in s2(u, slot):
            cp.start()

    def finish(u, slot, g):
        p, r0, r1a, r1b, r2a, r2b, hr = units[u]
        k = g % 3
        ca, cb = s2(u, slot)
        for half, (cp, r2) in enumerate(((ca, r2a), (cb, r2b))):
            cp.wait()
            rows = slice(half * hr, half * hr + hr)
            total = p[slot, c, y, x, rows].astype(F32) + r2[slot].astype(F32)
            if u == 1:
                g2[pl.ds(pl.multiple_of(k * SUB + half * hr, 64), hr), :] = total
            else:
                for cc in range(2):
                    for q in range(4):
                        i = cc * 4 + q
                        g1[rows, column(q, cc, k)] = total[:, i * SUB:(i + 1) * SUB]

    settle(loads[:2])

    @pl.loop(0, 6)
    def _(g):
        slot = g % 2
        prev = 1 - slot
        layer = 1 - g // 3
        k = g % 3
        settle(w_copies(g))

        @pl.when(g < 5)
        def _():
            run(w_copies(g + 1))

        @pl.when(g == 1)
        def _():
            loads[2].start()

        @pl.when(g == 3)
        def _():
            loads[2].wait()
            loads[3].start()
            run(lamb_loads(1))

        @pl.when(g == 5)
        def _():
            settle(lamb_outs(1, (0, 1), (0, 1, 2)))
            run(lamb_loads(0))

        def tile(rows):
            xv = xb[layer, rows, :]
            dyv = dyb[rows, :]
            xt[:, rows] = xv.T
            for n in range(CH // 256):
                cs = slice(n * 256, n * 256 + 256)
                h = dot(xv, w1b[k, :, :, :, :, cs].reshape(D, 256))
                da = dot(dyv, w2b[k, n // 2, n % 2].reshape(256, D), NT_DIMS)
                sq = h * h
                s = 0.5 * jnp.tanh(h * (C0 + C1 * sq)) + 0.5
                a = h * s
                gp = s + a * (1.0 - s) * (2.0 * C0 + (6.0 * C1) * sq)
                at[cs, rows] = a.astype(BF16).T
                dhb[rows, cs] = (da * gp).astype(BF16)

        def token_loop(with_dx):
            @pl.loop(0, TOK // (4 * TT))
            def _(t):
                @pl.when((g > 0) & (t == 1))
                def _():
                    to_s1(1, prev)

                if not with_dx:
                    @pl.when((g == 4) & (t == 1))
                    def _():
                        lamb_apply(1, 0)
                        gather_local().start()
                        lamb_apply(1, 1)
                        gather2_local().start()

                base = pl.multiple_of(t * (4 * TT), 4 * TT)
                spans = [pl.ds(base + i * TT, TT) for i in range(4)]
                for rows in spans:
                    tile(rows)
                if with_dx:
                    for rows in spans:
                        dxacc[rows, :] += dot(dhb[rows, :], w1b[k].reshape(D, CH), NT_DIMS)

        @pl.when(layer == 1)
        def _():
            @pl.when(k == 0)
            def _():
                @pl.loop(0, TOK // 128)
                def _(t):
                    rows = pl.ds(pl.multiple_of(t * 128, 128), 128)
                    dxacc[rows, :] = dyb[rows, :].astype(F32)

            token_loop(True)

        @pl.when(layer == 0)
        def _():
            token_loop(False)

        @pl.when(g > 0)
        def _():
            to_s2(0, prev)

        @pl.when(g == 4)
        def _():
            gather_local().wait()
            gather2_local().wait()
            for m in (9, 10, 11):
                first(m)

        for n in range(CH // 256):
            if n == 2:
                @pl.when(g > 0)
                def _():
                    to_s2(1, prev)
            fs = slice(n * 256, n * 256 + 256)
            res = dot(xt[...], dhb[:, fs]).astype(BF16)
            for b in range(8):
                p1[slot, b % 2, b // 4, (b // 2) % 2, :, fs] = res[b * 96:(b + 1) * 96]

        start_s0(0, slot)

        for n in range(CH // 256):
            res = dot(at[n * 256:n * 256 + 256, :], dyb[...]).astype(BF16)
            p2[slot, n // 2, n % 2] = res.reshape(2, SUB, D)

        to_s1(0, slot)
        start_s0(1, slot)

        @pl.when(g > 0)
        def _():
            finish(0, prev, g - 1)
            finish(1, prev, g - 1)

        @pl.when(g == 2)
        def _():
            @pl.loop(0, TOK // TT)
            def _(t):
                rows = pl.ds(pl.multiple_of(t * TT, TT), TT)
                dyb[rows, :] = dxacc[rows, :].astype(BF16)

        @pl.when(g == 3)
        def _():
            settle(lamb_loads(1))
            lamb_moments(1, 0)
            lamb_moments(1, 1)

    to_s1(1, 1)
    to_s2(0, 1)
    to_s2(1, 1)
    first(6)
    settle(lamb_loads(0))
    finish(0, 1, 5)
    lamb_moments(0, 0)
    finish(1, 1, 5)
    lamb_moments(0, 1)
    lamb_apply(0, 0)
    first(0)
    lamb_apply(0, 1)
    first(1)
    second(0)
    first(2)
    second(1)
    first(3)
    first(4)
    third(0)
    second(2)
    first(5)
    loads[3].wait()
    settle(lamb_outs(0, (0, 1), (1, 2)))
    third(1)
    done(0)
    done(1)

    def chunk_load(k, kind):
        if kind == 0:
            return pltpu.make_async_copy(wg1.at[k], w1b.at[k], f_sem.at[k, 0])
        return pltpu.make_async_copy(wg2.at[k], w2b.at[k], f_sem.at[k, 1])

    def out_copy(t):
        rows = pl.ds(pl.multiple_of(t * 512, 512), 512)
        return pltpu.make_async_copy(dyb.at[rows, :], out.at[rows, :], out_sem.at[t])

    def load(k, kind):
        done(9 + k if kind == 0 else 6 + k)
        chunk_load(k, kind).start()

    def ready(k):
        chunk_load(k, 0).wait()
        chunk_load(k, 1).wait()

    def before_1():
        second(5)
        second(9)
        first(7)
        third(3)
        done(2)
        done(3)

    def before_2():
        third(5)
        third(9)
        done(4)
        done(5)
        second(7)
        first(8)
        second(11)

    def before_3():
        load(0, 0)
        load(0, 1)
        third(10)
        ready(0)

    def before_4():
        third(11)
        ready(1)

    def before_5():
        ready(2)

    def f1_t1():
        third(4)
        second(6)

    def f3_t3():
        second(8)
        load(1, 1)

    hooks = {
        (0, 0): lambda: second(3),
        (0, 1): lambda: second(4),
        (0, 3): lambda: third(2),
        (1, 1): f1_t1,
        (1, 2): lambda: second(10),
        (2, 2): lambda: third(6),
        (3, 1): lambda: third(7),
        (3, 2): lambda: load(1, 0),
        (3, 3): f3_t3,
        (4, 1): lambda: load(2, 0),
        (4, 2): lambda: third(8),
        (4, 3): lambda: load(2, 1),
    }

    @pl.loop(0, 6)
    def _(f):
        k = f % 3
        for i, fn in enumerate((before_1, before_2, before_3, before_4, before_5)):
            pl.when(f == i + 1)(fn)

        @pl.when(k == 0)
        def _():
            @pl.loop(0, TOK // 128)
            def _(t):
                rows = pl.ds(pl.multiple_of(t * 128, 128), 128)
                dxacc[rows, :] = xb[1, rows, :].astype(F32)

        @pl.loop(0, TOK // (2 * TT))
        def _(t):
            for (hf, ht), fn in hooks.items():
                pl.when((f == hf) & (t == ht))(fn)
            base = pl.multiple_of(t * (2 * TT), 2 * TT)
            spans = [pl.ds(base + i * TT, TT) for i in range(2)]
            for rows in spans:
                xv = xb[1, rows, :]
                for n in range(CH // 256):
                    cs = slice(n * 256, n * 256 + 256)
                    h = dot(xv, w1b[k, :, :, :, :, cs].reshape(D, 256))
                    s = 0.5 * jnp.tanh(h * (C0 + C1 * (h * h))) + 0.5
                    dhb[rows, cs] = (h * s).astype(BF16)
            for rows in spans:
                dxacc[rows, :] += dot(dhb[rows, :], w2b[k].reshape(CH, D))

            pair = pl.ds(base, 2 * TT)

            @pl.when(f == 2)
            def _():
                xb[1, pair, :] = dxacc[pair, :].astype(BF16)

            @pl.when(f == 5)
            def _():
                dyb[pair, :] = dxacc[pair, :].astype(BF16)
                out_copy(t).start()

    settle(lamb_outs(0, (0, 1), (0,)))
    for t in range(4):
        out_copy(t).wait()


def run_step(*args):
    any_spec = pl.BlockSpec(memory_space=pl.ANY)
    vm = pltpu.VMEM
    dma = pltpu.SemaphoreType.DMA
    up, down = jax.ShapeDtypeStruct((2, 96, FF), F32), jax.ShapeDtypeStruct((2, 384, D), F32)
    return pl.pallas_call(
        step_kernel,
        out_shape=(up, down, up, down, up, down, jax.ShapeDtypeStruct((TOK, D), BF16),
                   jax.ShapeDtypeStruct((3, 2, 2, 2, 96, CH), BF16), jax.ShapeDtypeStruct((3, 2, 2, 2, SUB, D), BF16)),
        in_specs=[any_spec] * 13,
        out_specs=(any_spec,) * 9,
        scratch_shapes=[
            vm((2, TOK, D), BF16), vm((TOK, D), BF16), vm((D, TOK), BF16), vm((3 * 768, D), F32),
            vm((3, 2, 2, 2, 96, CH), BF16), vm((3, 2, 2, 2, SUB, D), BF16), vm((CH, TOK), BF16), vm((TOK, CH), BF16),
            vm((2, 2, 2, 2, 96, CH), BF16), vm((2, 2, 2, 2, SUB, D), BF16),
            vm((2, 2, 2, 96, CH), BF16), vm((2, 2, 2, SUB, D), BF16),
            vm((2, 2, 48, CH), BF16), vm((2, 2, 48, CH), BF16), vm((2, 2, 64, D), BF16), vm((2, 2, 64, D), BF16),
            vm((2, 48, CH), BF16), vm((2, 48, CH), BF16), vm((2, 64, D), BF16), vm((2, 64, D), BF16),
            vm((96, FF), F32), vm((384, D), F32), vm((768, 768), F32), vm((2, 2, 2, 8, 128), F32), vm((2, 2, 8, 128), F32), vm((2, 2, 8, 8, 128), F32), vm((8, 128), F32),
            vm((3, 96, CH), BF16), vm((3, SUB, D), BF16),
            dma((6,)), dma((3, 10)), dma((2, 2, 5)), dma((2, 2, 5)), dma((4, 5)), dma((3, 5)),
            dma((2, 2, 7)), dma((2, 2, 7)), dma((12, 9)), dma((12, 9)), dma((3, 2)), dma((4,)),
        ],
        compiler_params=pltpu.CompilerParams(collective_id=0, has_side_effects=True, vmem_limit_bytes=VMEM_MAX),
        name='step',
    )(*args)


def copy_kernel(*refs):
    src, dst, buf, (sem_in, sem_out) = refs[:7], refs[7:14], refs[14:21], refs[21:]
    order = [(a, i) for i in range(2) for a in range(7)]

    def part(ref, a, i):
        return ref.at[pl.ds(i * (TOK // 2), TOK // 2)] if a == 6 else ref.at[i]

    ins = [pltpu.make_async_copy(part(src[a], a, i), part(buf[a], a, i), sem_in.at[a, i]) for a, i in order]
    outs = [pltpu.make_async_copy(part(buf[a], a, i), part(dst[a], a, i), sem_out.at[a, i]) for a, i in order]
    for cp in ins:
        cp.start()
    for cp, nxt in zip(ins, outs):
        cp.wait()
        nxt.start()
    for cp in outs:
        cp.wait()


def run_copy(arrays):
    any_spec = pl.BlockSpec(memory_space=pl.ANY)
    return pl.pallas_call(
        copy_kernel,
        out_shape=tuple(jax.ShapeDtypeStruct(a.shape, a.dtype) for a in arrays),
        in_specs=[any_spec] * 7,
        out_specs=(any_spec,) * 7,
        scratch_shapes=[pltpu.VMEM(a.shape, a.dtype) for a in arrays] + [pltpu.SemaphoreType.DMA((7, 2)), pltpu.SemaphoreType.DMA((7, 2))],
        compiler_params=pltpu.CompilerParams(vmem_limit_bytes=VMEM_MAX),
        name='copy_out',
    )(*arrays)


def solution(mesh):
    shard_rows = P(None, 'fsdp')
    shard_batch = P('fsdp')
    spec_whole = P()

    def local_step(x_layers, dy_top, x_next, w_up, w_down, acc_up, acc_down, master_up, master_down, mom_up, mom_down, var_up, var_down):
        res = run_step(x_layers.reshape(2, TOK, D), dy_top.reshape(TOK, D), x_next.reshape(TOK, D),
                       w_up.reshape(2, 2, 2, 2, 96, FF), w_down.reshape(2, 2, 2, 2, 3, SUB, D),
                       acc_up, acc_down, master_up, master_down, mom_up, mom_down, var_up, var_down)
        res = run_copy(res[:7])
        return tuple(res[:6]) + (res[6].reshape(1, TOK, D),)

    return jax.shard_map(local_step, mesh=mesh, in_specs=(shard_rows, shard_batch, shard_batch, spec_whole, spec_whole) + (shard_rows,) * 8, out_specs=(shard_rows,) * 6 + (shard_batch,), check_vma=False)
```

```python
import functools

import jax
import jax.numpy as jnp
from jax import lax
from jax.experimental import pallas as pl
from jax.experimental.pallas import tpu as pltpu
from jax.sharding import PartitionSpec as P

MICRO_STEPS = 2
STEP_COUNT = 3
BETA_MOM = 0.9
BETA_VAR = 0.999
ADAM_EPS = 1e-6
WEIGHT_DECAY = 0.01
LEARN_RATE = 0.06

C0 = 0.7978845608028654
C1 = C0 * 0.044715
MESH = pl.DeviceIdType.MESH
BF16 = jnp.bfloat16
F32 = jnp.float32
VMEM_MAX = 67043328

TOK = 2048
D = 768
FF = 3072
SUB = 128
CH = 8 * SUB
TT = 256
NT_DIMS = (((1,), (1,)), ((), ()))
NN_DIMS = (((1,), (0,)), ((), ()))


def position():
    me = lax.axis_index('fsdp')
    y, x, c = me // 4, (me // 2) % 2, me % 2
    return me, y, x, c, me + 1 - 2 * c, me + 2 - 4 * x, me + 4 - 8 * y


def entry_barrier(targets):
    barrier = pltpu.get_barrier_semaphore()
    for dev in targets:
        pl.semaphore_signal(barrier, inc=1, device_id=(dev,), device_id_type=MESH)
    pl.semaphore_wait(barrier, len(targets))


def dot(a, b, dims=NN_DIMS):
    return lax.dot_general(a, b, dims, preferred_element_type=F32)


def moments(grad_sum, acc, master, mom_prev, var_prev):
    grad = (acc + grad_sum) / MICRO_STEPS
    mom = BETA_MOM * mom_prev + (1.0 - BETA_MOM) * grad
    var = BETA_VAR * var_prev + (1.0 - BETA_VAR) * grad * grad
    upd = (mom / (1.0 - BETA_MOM ** STEP_COUNT)) / (jnp.sqrt(var / (1.0 - BETA_VAR ** STEP_COUNT)) + ADAM_EPS) + WEIGHT_DECAY * master
    return mom, var, upd


def step_kernel(x_hbm, dy_hbm, xn_hbm, w1_hbm, w2_hbm, acc1, acc2, mas1, mas2, mom1, mom2, var1, var2,
                wo1, wo2, mo1, mo2, vo1, vo2, out, wg1, wg2,
                xb, dyb, xt, dxacc, w1b, w2b, at, dhb, p1, p2, r01, r02, r1a1, r1b1, r1a2, r1b2, r2a1, r2b1, r2a2, r2b2,
                g1, g2, mb, sqb, smine, sgot, tot, ws1, ws2,
                ld_sem, w_sem, snd, rcv, l_sem, o_sem, x_snd, x_rcv, b_snd, b_rcv, f_sem, out_sem):
    me, y, x, c, partner, xn, yn = position()
    others = [lax.rem(me + i, 8) for i in range(1, 8)]

    def column(q, cc, k):
        return pl.ds(pl.multiple_of((2 * q + cc) * 384 + k * SUB, SUB), SUB)

    def w_copies(g):
        layer = 1 - g // 3
        k = g % 3
        res = []
        for cc in range(2):
            for q in range(4):
                i = cc * 4 + q
                res.append(pltpu.make_async_copy(w1_hbm.at[layer, :, :, :, :, column(q, cc, k)], w1b.at[k, :, :, :, :, pl.ds(i * SUB, SUB)], w_sem.at[k, i]))
            res.append(pltpu.make_async_copy(w2_hbm.at[layer, :, :, cc, k], w2b.at[k, cc], w_sem.at[k, 8 + cc]))
        return res

    loads = [pltpu.make_async_copy(x_hbm.at[1], xb.at[1], ld_sem.at[0]),
             pltpu.make_async_copy(dy_hbm, dyb, ld_sem.at[1]),
             pltpu.make_async_copy(x_hbm.at[0], xb.at[0], ld_sem.at[2]),
             pltpu.make_async_copy(xn_hbm, xb.at[1], ld_sem.at[3])]
    for cp in loads[:2]:
        cp.start()
    for cp in w_copies(0):
        cp.start()
    sqb[...] = jnp.zeros_like(sqb)
    smine[...] = jnp.zeros_like(smine)
    entry_barrier(others)

    def area(a, kind, j):
        return pl.ds(pl.multiple_of(a * 768 + j * 96, 96), 96) if kind == 0 else pl.ds(pl.multiple_of(a * 768 + 384 + j * SUB, SUB), SUB)

    def shard_pairs(up, down, layer, buf, a):
        res = [(up.at[layer, :, pl.ds(j * 768, 768)], buf.at[pl.ds(a * 768 + j * 96, 96), :]) for j in range(4)]
        res.append((down.at[layer], buf.at[pl.ds(a * 768 + 384, 384), :]))
        return res

    def lamb_loads(layer):
        res = []
        for a, (up, down) in enumerate(((acc1, acc2), (mom1, mom2), (var1, var2), (mas1, mas2))):
            for i, (src, dst) in enumerate(shard_pairs(up, down, layer, dxacc if a < 3 else mb, a % 3)):
                res.append(pltpu.make_async_copy(src, dst, l_sem.at[a, i]))
        return res

    def lamb_outs(layer, kinds, arrays):
        res = []
        for a, (up, down) in ((0, (wo1, wo2)), (1, (mo1, mo2)), (2, (vo1, vo2))):
            for i, (dst, src) in enumerate(shard_pairs(up, down, layer, mb if a == 0 else dxacc, a)):
                if a in arrays and i // 4 in kinds:
                    res.append(pltpu.make_async_copy(src, dst, o_sem.at[a, i]))
        return res

    def run(copies):
        for cp in copies:
            cp.start()

    def settle(copies):
        for cp in copies:
            cp.wait()

    def lamb_moments(layer, kind):
        @pl.loop(0, 4 - kind)
        def _(j):
            spans = [area(a, kind, j) for a in range(3)]
            grad_sum = g1[:, pl.ds(pl.multiple_of(j * 768, 768), 768)] if kind == 0 else g2[pl.ds(pl.multiple_of(j * SUB, SUB), SUB), :]
            master = mb[spans[0], :]
            mom, var, upd = moments(grad_sum, dxacc[spans[0], :], master, dxacc[spans[1], :], dxacc[spans[2], :])
            dxacc[spans[0], :] = upd
            dxacc[spans[1], :] = mom
            dxacc[spans[2], :] = var
            for i, val in enumerate((master, upd)):
                folded = jnp.sum((val * val).reshape(-1, 8, 768), axis=0)
                lanes = folded[:, 0:128]
                for b in range(1, 6):
                    lanes = lanes + folded[:, b * 128:(b + 1) * 128]
                sqb[layer, kind, i] += lanes

        for i in range(2):
            smine[layer, kind, i:i + 1, :] = jnp.sum(sqb[layer, kind, i], axis=0, keepdims=True)
        run(sum_copies(layer, kind))
        run(lamb_outs(layer, (kind,), (1, 2)))

    def sum_copies(layer, kind):
        return [pltpu.make_async_remote_copy(src_ref=smine.at[layer, kind], dst_ref=sgot.at[layer, kind, i], send_sem=x_snd.at[layer, kind, i], recv_sem=x_rcv.at[layer, kind, i], device_id=(dev,), device_id_type=MESH) for i, dev in enumerate(others)]

    def lamb_apply(layer, kind):
        sgot[layer, kind, 7] = smine[layer, kind]
        settle(sum_copies(layer, kind))
        total = sgot[layer, kind, lax.rem(me + 7, 8)]
        for dev in range(1, 8):
            total = total + sgot[layer, kind, lax.rem(me + 7 - dev + 8, 8)]
        tot[...] = jnp.broadcast_to(jnp.sum(total, axis=1, keepdims=True), (8, 128))
        scale = LEARN_RATE * jnp.sqrt(tot[0:1, 0:1] / tot[1:2, 0:1])

        @pl.loop(0, 4 - kind)
        def _(j):
            span = area(0, kind, j)
            new = mb[span, :] - scale * dxacc[span, :]
            mb[span, :] = new
            half = new.astype(BF16)
            if kind == 1:
                if layer == 1:
                    ws2[j] = half
                else:
                    w2b[j, c, y, x] = half
            else:
                for cc in range(2):
                    lanes = pl.ds(pl.multiple_of((cc * 4 + j) * SUB, SUB), SUB)
                    for k in range(3):
                        piece = half[:, cc * 384 + k * SUB:cc * 384 + (k + 1) * SUB]
                        if layer == 1:
                            ws1[k, :, lanes] = piece
                        else:
                            w1b[k, y, x, c, :, lanes] = piece

        run(lamb_outs(layer, (kind,), (0,)))

    def remote_copy(src, dst, s_sem, r_sem, dev):
        return pltpu.make_async_remote_copy(src_ref=src, dst_ref=dst, send_sem=s_sem, recv_sem=r_sem, device_id=(dev,), device_id_type=MESH)

    def gather_local():
        return pltpu.make_async_copy(ws1, wg1.at[:, y, x, c], ld_sem.at[4])

    def gather2_local():
        return pltpu.make_async_copy(ws2, wg2.at[:, c, y, x], ld_sem.at[5])

    def piece_parts(m, name):
        if m > 8 or (m < 6 and m % 2 == 0):
            ref = w1b.at[m // 2] if m < 6 else wg1.at[m - 9]
            h = 48

            def blk(yy, xx, rows):
                return ref.at[yy, xx, c, rows]
        else:
            ref = w2b.at[m // 2] if m < 6 else wg2.at[m - 6]
            h = 64

            def blk(yy, xx, rows):
                return ref.at[c, yy, xx, rows]
        first, last, every, both = pl.ds(0, h), pl.ds(h, h), pl.ds(0, 2 * h), slice(None)

        def go(part, i, dev):
            return remote_copy(part, part, b_snd.at[m, i], b_rcv.at[m, i], dev)
        if name == 's1':
            return go(blk(y, x, first), 0, xn), go(blk(y, x, last), 1, yn)
        if name == 's2':
            return go(blk(y, both, first), 2, yn), go(blk(both, x, last), 3, xn)
        if name == 'd1':
            return (go(blk(y, x, every), 4, partner),)
        if name == 'd2':
            return go(blk(y, 1 - x, first), 5, partner), go(blk(1 - y, x, last), 6, partner)
        return go(blk(1 - y, both, first), 7, partner), go(blk(both, 1 - x, last), 8, partner)

    def first(m):
        run(piece_parts(m, 's1'))
        run(piece_parts(m, 'd1'))

    def second(m):
        settle(piece_parts(m, 's1'))
        run(piece_parts(m, 's2'))
        run(piece_parts(m, 'd2'))

    def third(m):
        settle(piece_parts(m, 's2'))
        run(piece_parts(m, 'd3'))

    def done(m):
        for name in ('d1', 'd2', 'd3'):
            settle(piece_parts(m, name))

    units = ((p1, r01, r1a1, r1b1, r2a1, r2b1, 48), (p2, r02, r1a2, r1b2, r2a2, r2b2, 64))

    def remote(src, dst, u, slot, stage, dev):
        return pltpu.make_async_remote_copy(src_ref=src, dst_ref=dst, send_sem=snd.at[u, slot, stage], recv_sem=rcv.at[u, slot, stage], device_id=(dev,), device_id_type=MESH)

    def s0(u, slot):
        p, r0, r1a, r1b, r2a, r2b, hr = units[u]
        return remote(p.at[slot, 1 - c], r0.at[slot], u, slot, 0, partner)

    def s1(u, slot):
        p, r0, r1a, r1b, r2a, r2b, hr = units[u]
        return (remote(p.at[slot, c, :, 1 - x, pl.ds(0, hr)], r1a.at[slot], u, slot, 1, xn),
                remote(p.at[slot, c, 1 - y, :, pl.ds(hr, hr)], r1b.at[slot], u, slot, 2, yn))

    def s2(u, slot):
        p, r0, r1a, r1b, r2a, r2b, hr = units[u]
        return (remote(p.at[slot, c, 1 - y, x, pl.ds(0, hr)], r2a.at[slot], u, slot, 3, yn),
                remote(p.at[slot, c, y, 1 - x, pl.ds(hr, hr)], r2b.at[slot], u, slot, 4, xn))

    def start_s0(u, slot):
        s0(u, slot).start()

    def to_s1(u, slot):
        p, r0, r1a, r1b, r2a, r2b, hr = units[u]
        s0(u, slot).wait()

        @pl.loop(0, 2)
        def _(yy):
            for xx in range(2):
                p[slot, c, yy, xx] = (p[slot, c, yy, xx].astype(F32) + r0[slot, yy, xx].astype(F32)).astype(BF16)

        for cp in s1(u, slot):
            cp.start()

    def to_s2(u, slot):
        p, r0, r1a, r1b, r2a, r2b, hr = units[u]
        ca, cb = s1(u, slot)
        ca.wait()
        for i in range(2):
            p[slot, c, i, x, 0:hr] = (p[slot, c, i, x, 0:hr].astype(F32) + r1a[slot, i].astype(F32)).astype(BF16)
        cb.wait()
        for i in range(2):
            p[slot, c, y, i, hr:2 * hr] = (p[slot, c, y, i, hr:2 * hr].astype(F32) + r1b[slot, i].astype(F32)).astype(BF16)
        for cp in s2(u, slot):
            cp.start()

    def finish(u, slot, g):
        p, r0, r1a, r1b, r2a, r2b, hr = units[u]
        k = g % 3
        ca, cb = s2(u, slot)
        for half, (cp, r2) in enumerate(((ca, r2a), (cb, r2b))):
            cp.wait()
            rows = slice(half * hr, half * hr + hr)
            total = p[slot, c, y, x, rows].astype(F32) + r2[slot].astype(F32)
            if u == 1:
                g2[pl.ds(pl.multiple_of(k * SUB + half * hr, 64), hr), :] = total
            else:
                for cc in range(2):
                    for q in range(4):
                        i = cc * 4 + q
                        g1[rows, column(q, cc, k)] = total[:, i * SUB:(i + 1) * SUB]

    settle(loads[:2])

    @pl.loop(0, 6)
    def _(g):
        slot = g % 2
        prev = 1 - slot
        layer = 1 - g // 3
        k = g % 3
        settle(w_copies(g))

        @pl.when(g < 5)
        def _():
            run(w_copies(g + 1))

        @pl.when(g == 1)
        def _():
            loads[2].start()

        @pl.when(g == 3)
        def _():
            loads[2].wait()
            loads[3].start()
            run(lamb_loads(1))

        @pl.when(g == 5)
        def _():
            settle(lamb_outs(1, (0, 1), (0, 1, 2)))
            run(lamb_loads(0))

        def tile(rows):
            xv = xb[layer, rows, :]
            dyv = dyb[rows, :]
            xt[:, rows] = xv.T
            for n in range(CH // 256):
                cs = slice(n * 256, n * 256 + 256)
                h = dot(xv, w1b[k, :, :, :, :, cs].reshape(D, 256))
                da = dot(dyv, w2b[k, n // 2, n % 2].reshape(256, D), NT_DIMS)
                sq = h * h
                s = 0.5 * jnp.tanh(h * (C0 + C1 * sq)) + 0.5
                a = h * s
                gp = s + a * (1.0 - s) * (2.0 * C0 + (6.0 * C1) * sq)
                at[cs, rows] = a.astype(BF16).T
                dhb[rows, cs] = (da * gp).astype(BF16)

        def token_loop(with_dx):
            @pl.loop(0, TOK // (4 * TT))
            def _(t):
                @pl.when((g > 0) & (t == 1))
                def _():
                    to_s1(1, prev)

                if not with_dx:
                    @pl.when((g == 5) & (t == 1))
                    def _():
                        second(9)

                    @pl.when((g == 4) & (t == 1))
                    def _():
                        lamb_apply(1, 0)
                        gather_local().start()
                        lamb_apply(1, 1)
                        gather2_local().start()

                base = pl.multiple_of(t * (4 * TT), 4 * TT)
                spans = [pl.ds(base + i * TT, TT) for i in range(4)]
                for rows in spans:
                    tile(rows)
                if with_dx:
                    for rows in spans:
                        dxacc[rows, :] += dot(dhb[rows, :], w1b[k].reshape(D, CH), NT_DIMS)

        @pl.when(layer == 1)
        def _():
            @pl.when(k == 0)
            def _():
                @pl.loop(0, TOK // 128)
                def _(t):
                    rows = pl.ds(pl.multiple_of(t * 128, 128), 128)
                    dxacc[rows, :] = dyb[rows, :].astype(F32)

            token_loop(True)

        @pl.when(layer == 0)
        def _():
            token_loop(False)

        @pl.when(g > 0)
        def _():
            to_s2(0, prev)

        for n in range(CH // 256):
            if n == 2:
                @pl.when(g > 0)
                def _():
                    to_s2(1, prev)

                @pl.when(g == 4)
                def _():
                    gather_local().wait()
                    gather2_local().wait()
                    for m in (9, 10, 11):
                        first(m)

            fs = slice(n * 256, n * 256 + 256)
            res = dot(xt[...], dhb[:, fs]).astype(BF16)
            for b in range(8):
                p1[slot, b % 2, b // 4, (b // 2) % 2, :, fs] = res[b * 96:(b + 1) * 96]

        start_s0(0, slot)

        for n in range(CH // 256):
            res = dot(at[n * 256:n * 256 + 256, :], dyb[...]).astype(BF16)
            p2[slot, n // 2, n % 2] = res.reshape(2, SUB, D)

        to_s1(0, slot)
        start_s0(1, slot)

        @pl.when(g > 0)
        def _():
            finish(0, prev, g - 1)
            finish(1, prev, g - 1)

        @pl.when(g == 2)
        def _():
            @pl.loop(0, TOK // TT)
            def _(t):
                rows = pl.ds(pl.multiple_of(t * TT, TT), TT)
                dyb[rows, :] = dxacc[rows, :].astype(BF16)

        @pl.when(g == 3)
        def _():
            settle(lamb_loads(1))
            lamb_moments(1, 0)
            lamb_moments(1, 1)

    to_s1(1, 1)
    to_s2(0, 1)
    to_s2(1, 1)
    first(6)
    settle(lamb_loads(0))
    finish(0, 1, 5)
    lamb_moments(0, 0)
    finish(1, 1, 5)
    lamb_moments(0, 1)
    lamb_apply(0, 0)
    first(0)
    lamb_apply(0, 1)
    first(1)
    second(0)
    first(2)
    second(1)
    first(3)
    first(4)
    third(0)
    second(2)
    first(5)
    third(9)
    loads[3].wait()
    settle(lamb_outs(0, (0, 1), (1, 2)))
    third(1)
    done(0)
    done(1)

    def chunk_load(k, kind):
        if kind == 0:
            return pltpu.make_async_copy(wg1.at[k], w1b.at[k], f_sem.at[k, 0])
        return pltpu.make_async_copy(wg2.at[k], w2b.at[k], f_sem.at[k, 1])

    def out_copy(t):
        rows = pl.ds(pl.multiple_of(t * 512, 512), 512)
        return pltpu.make_async_copy(dyb.at[rows, :], out.at[rows, :], out_sem.at[t])

    def load(k, kind):
        done(9 + k if kind == 0 else 6 + k)
        chunk_load(k, kind).start()

    def ready(k):
        chunk_load(k, 0).wait()
        chunk_load(k, 1).wait()

    def before_1():
        second(5)
        first(7)
        third(3)
        done(2)
        done(3)
        load(0, 0)

    def before_2():
        third(5)
        done(4)
        done(5)
        second(7)
        first(8)
        second(11)

    def before_3():
        load(0, 1)
        third(10)
        ready(0)

    def before_4():
        third(11)
        ready(1)

    def before_5():
        ready(2)

    def f1_t1():
        third(4)
        second(6)

    def f3_t3():
        second(8)
        load(1, 1)

    hooks = {
        (0, 0): lambda: second(3),
        (0, 1): lambda: second(4),
        (0, 3): lambda: third(2),
        (1, 1): f1_t1,
        (1, 2): lambda: second(10),
        (2, 2): lambda: third(6),
        (3, 1): lambda: third(7),
        (3, 2): lambda: load(1, 0),
        (3, 3): f3_t3,
        (4, 1): lambda: load(2, 0),
        (4, 2): lambda: third(8),
        (4, 3): lambda: load(2, 1),
    }

    @pl.loop(0, 6)
    def _(f):
        k = f % 3
        for i, fn in enumerate((before_1, before_2, before_3, before_4, before_5)):
            pl.when(f == i + 1)(fn)

        @pl.when(k == 0)
        def _():
            @pl.loop(0, TOK // 128)
            def _(t):
                rows = pl.ds(pl.multiple_of(t * 128, 128), 128)
                dxacc[rows, :] = xb[1, rows, :].astype(F32)

        @pl.loop(0, TOK // (2 * TT))
        def _(t):
            for (hf, ht), fn in hooks.items():
                pl.when((f == hf) & (t == ht))(fn)
            base = pl.multiple_of(t * (2 * TT), 2 * TT)
            spans = [pl.ds(base + i * TT, TT) for i in range(2)]
            for rows in spans:
                xv = xb[1, rows, :]
                for n in range(CH // 256):
                    cs = slice(n * 256, n * 256 + 256)
                    h = dot(xv, w1b[k, :, :, :, :, cs].reshape(D, 256))
                    s = 0.5 * jnp.tanh(h * (C0 + C1 * (h * h))) + 0.5
                    dhb[rows, cs] = (h * s).astype(BF16)
            for rows in spans:
                dxacc[rows, :] += dot(dhb[rows, :], w2b[k].reshape(CH, D))

            pair = pl.ds(base, 2 * TT)

            @pl.when(f == 2)
            def _():
                xb[1, pair, :] = dxacc[pair, :].astype(BF16)

            @pl.when(f == 5)
            def _():
                dyb[pair, :] = dxacc[pair, :].astype(BF16)
                out_copy(t).start()

    settle(lamb_outs(0, (0, 1), (0,)))
    for t in range(4):
        out_copy(t).wait()


def run_step(*args):
    any_spec = pl.BlockSpec(memory_space=pl.ANY)
    vm = pltpu.VMEM
    dma = pltpu.SemaphoreType.DMA
    up, down = jax.ShapeDtypeStruct((2, 96, FF), F32), jax.ShapeDtypeStruct((2, 384, D), F32)
    return pl.pallas_call(
        step_kernel,
        out_shape=(up, down, up, down, up, down, jax.ShapeDtypeStruct((TOK, D), BF16),
                   jax.ShapeDtypeStruct((3, 2, 2, 2, 96, CH), BF16), jax.ShapeDtypeStruct((3, 2, 2, 2, SUB, D), BF16)),
        in_specs=[any_spec] * 13,
        out_specs=(any_spec,) * 9,
        scratch_shapes=[
            vm((2, TOK, D), BF16), vm((TOK, D), BF16), vm((D, TOK), BF16), vm((3 * 768, D), F32),
            vm((3, 2, 2, 2, 96, CH), BF16), vm((3, 2, 2, 2, SUB, D), BF16), vm((CH, TOK), BF16), vm((TOK, CH), BF16),
            vm((2, 2, 2, 2, 96, CH), BF16), vm((2, 2, 2, 2, SUB, D), BF16),
            vm((2, 2, 2, 96, CH), BF16), vm((2, 2, 2, SUB, D), BF16),
            vm((2, 2, 48, CH), BF16), vm((2, 2, 48, CH), BF16), vm((2, 2, 64, D), BF16), vm((2, 2, 64, D), BF16),
            vm((2, 48, CH), BF16), vm((2, 48, CH), BF16), vm((2, 64, D), BF16), vm((2, 64, D), BF16),
            vm((96, FF), F32), vm((384, D), F32), vm((768, 768), F32), vm((2, 2, 2, 8, 128), F32), vm((2, 2, 8, 128), F32), vm((2, 2, 8, 8, 128), F32), vm((8, 128), F32),
            vm((3, 96, CH), BF16), vm((3, SUB, D), BF16),
            dma((6,)), dma((3, 10)), dma((2, 2, 5)), dma((2, 2, 5)), dma((4, 5)), dma((3, 5)),
            dma((2, 2, 7)), dma((2, 2, 7)), dma((12, 9)), dma((12, 9)), dma((3, 2)), dma((4,)),
        ],
        compiler_params=pltpu.CompilerParams(collective_id=0, has_side_effects=True, vmem_limit_bytes=VMEM_MAX),
        name='step',
    )(*args)


def copy_kernel(*refs):
    src, dst, buf, (sem_in, sem_out) = refs[:7], refs[7:14], refs[14:21], refs[21:]
    order = [(a, i) for i in range(2) for a in range(7)]

    def part(ref, a, i):
        return ref.at[pl.ds(i * (TOK // 2), TOK // 2)] if a == 6 else ref.at[i]

    ins = [pltpu.make_async_copy(part(src[a], a, i), part(buf[a], a, i), sem_in.at[a, i]) for a, i in order]
    outs = [pltpu.make_async_copy(part(buf[a], a, i), part(dst[a], a, i), sem_out.at[a, i]) for a, i in order]
    for cp in ins:
        cp.start()
    for cp, nxt in zip(ins, outs):
        cp.wait()
        nxt.start()
    for cp in outs:
        cp.wait()


def run_copy(arrays):
    any_spec = pl.BlockSpec(memory_space=pl.ANY)
    return pl.pallas_call(
        copy_kernel,
        out_shape=tuple(jax.ShapeDtypeStruct(a.shape, a.dtype) for a in arrays),
        in_specs=[any_spec] * 7,
        out_specs=(any_spec,) * 7,
        scratch_shapes=[pltpu.VMEM(a.shape, a.dtype) for a in arrays] + [pltpu.SemaphoreType.DMA((7, 2)), pltpu.SemaphoreType.DMA((7, 2))],
        compiler_params=pltpu.CompilerParams(vmem_limit_bytes=VMEM_MAX),
        name='copy_out',
    )(*arrays)


def solution(mesh):
    shard_rows = P(None, 'fsdp')
    shard_batch = P('fsdp')
    spec_whole = P()

    def local_step(x_layers, dy_top, x_next, w_up, w_down, acc_up, acc_down, master_up, master_down, mom_up, mom_down, var_up, var_down):
        res = run_step(x_layers.reshape(2, TOK, D), dy_top.reshape(TOK, D), x_next.reshape(TOK, D),
                       w_up.reshape(2, 2, 2, 2, 96, FF), w_down.reshape(2, 2, 2, 2, 3, SUB, D),
                       acc_up, acc_down, master_up, master_down, mom_up, mom_down, var_up, var_down)
        res = run_copy(res[:7])
        return tuple(res[:6]) + (res[6].reshape(1, TOK, D),)

    return jax.shard_map(local_step, mesh=mesh, in_specs=(shard_rows, shard_batch, shard_batch, spec_whole, spec_whole) + (shard_rows,) * 8, out_specs=(shard_rows,) * 6 + (shard_batch,), check_vma=False)
```

```python
import functools

import jax
import jax.numpy as jnp
from jax import lax
from jax.experimental import pallas as pl
from jax.experimental.pallas import tpu as pltpu
from jax.sharding import PartitionSpec as P

MICRO_STEPS = 2
STEP_COUNT = 3
BETA_MOM = 0.9
BETA_VAR = 0.999
ADAM_EPS = 1e-6
WEIGHT_DECAY = 0.01
LEARN_RATE = 0.06

C0 = 0.7978845608028654
C1 = C0 * 0.044715
MESH = pl.DeviceIdType.MESH
BF16 = jnp.bfloat16
F32 = jnp.float32
VMEM_MAX = 67043328

TOK = 2048
D = 768
FF = 3072
SUB = 128
CH = 8 * SUB
TT = 256
NT_DIMS = (((1,), (1,)), ((), ()))
NN_DIMS = (((1,), (0,)), ((), ()))


def position():
    me = lax.axis_index('fsdp')
    y, x, c = me // 4, (me // 2) % 2, me % 2
    return me, y, x, c, me + 1 - 2 * c, me + 2 - 4 * x, me + 4 - 8 * y


def entry_barrier(targets):
    barrier = pltpu.get_barrier_semaphore()
    for dev in targets:
        pl.semaphore_signal(barrier, inc=1, device_id=(dev,), device_id_type=MESH)
    pl.semaphore_wait(barrier, len(targets))


def dot(a, b, dims=NN_DIMS):
    return lax.dot_general(a, b, dims, preferred_element_type=F32)


def moments(grad_sum, acc, master, mom_prev, var_prev):
    grad = (acc + grad_sum) / MICRO_STEPS
    mom = BETA_MOM * mom_prev + (1.0 - BETA_MOM) * grad
    var = BETA_VAR * var_prev + (1.0 - BETA_VAR) * grad * grad
    upd = (mom / (1.0 - BETA_MOM ** STEP_COUNT)) / (jnp.sqrt(var / (1.0 - BETA_VAR ** STEP_COUNT)) + ADAM_EPS) + WEIGHT_DECAY * master
    return mom, var, upd


def step_kernel(x_hbm, dy_hbm, xn_hbm, w1_hbm, w2_hbm, acc1, acc2, mas1, mas2, mom1, mom2, var1, var2,
                wo1, wo2, mo1, mo2, vo1, vo2, out, wg1, wg2,
                xb, dyb, xt, dxacc, w1b, w2b, at, dhb, p1, p2, r01, r02, r1a1, r1b1, r1a2, r1b2, r2a1, r2b1, r2a2, r2b2,
                g1, g2, mb, sqb, smine, sgot, tot, ws1, ws2,
                ld_sem, w_sem, snd, rcv, l_sem, o_sem, x_snd, x_rcv, b_snd, b_rcv, f_sem, out_sem):
    me, y, x, c, partner, xn, yn = position()
    others = [lax.rem(me + i, 8) for i in range(1, 8)]

    def column(q, cc, k):
        return pl.ds(pl.multiple_of((2 * q + cc) * 384 + k * SUB, SUB), SUB)

    def w_copies(g):
        layer = 1 - g // 3
        k = g % 3
        res = []
        for cc in range(2):
            for q in range(4):
                i = cc * 4 + q
                res.append(pltpu.make_async_copy(w1_hbm.at[layer, :, :, :, :, column(q, cc, k)], w1b.at[k, :, :, :, :, pl.ds(i * SUB, SUB)], w_sem.at[k, i]))
            res.append(pltpu.make_async_copy(w2_hbm.at[layer, :, :, cc, k], w2b.at[k, cc], w_sem.at[k, 8 + cc]))
        return res

    loads = [pltpu.make_async_copy(x_hbm.at[1], xb.at[1], ld_sem.at[0]),
             pltpu.make_async_copy(dy_hbm, dyb, ld_sem.at[1]),
             pltpu.make_async_copy(x_hbm.at[0], xb.at[0], ld_sem.at[2]),
             pltpu.make_async_copy(xn_hbm, xb.at[1], ld_sem.at[3])]
    for cp in loads[:2]:
        cp.start()
    for cp in w_copies(0):
        cp.start()
    sqb[...] = jnp.zeros_like(sqb)
    smine[...] = jnp.zeros_like(smine)
    entry_barrier(others)

    def area(a, kind, j):
        return pl.ds(pl.multiple_of(a * 768 + j * 96, 96), 96) if kind == 0 else pl.ds(pl.multiple_of(a * 768 + 384 + j * SUB, SUB), SUB)

    def shard_pairs(up, down, layer, buf, a):
        res = [(up.at[layer, :, pl.ds(j * 768, 768)], buf.at[pl.ds(a * 768 + j * 96, 96), :]) for j in range(4)]
        res.append((down.at[layer], buf.at[pl.ds(a * 768 + 384, 384), :]))
        return res

    def lamb_loads(layer):
        res = []
        for a, (up, down) in enumerate(((acc1, acc2), (mom1, mom2), (var1, var2), (mas1, mas2))):
            for i, (src, dst) in enumerate(shard_pairs(up, down, layer, dxacc if a < 3 else mb, a % 3)):
                res.append(pltpu.make_async_copy(src, dst, l_sem.at[a, i]))
        return res

    def lamb_outs(layer, kinds, arrays):
        res = []
        for a, (up, down) in ((0, (wo1, wo2)), (1, (mo1, mo2)), (2, (vo1, vo2))):
            for i, (dst, src) in enumerate(shard_pairs(up, down, layer, mb if a == 0 else dxacc, a)):
                if a in arrays and i // 4 in kinds:
                    res.append(pltpu.make_async_copy(src, dst, o_sem.at[a, i]))
        return res

    def run(copies):
        for cp in copies:
            cp.start()

    def settle(copies):
        for cp in copies:
            cp.wait()

    def lamb_moments(layer, kind):
        @pl.loop(0, 4 - kind)
        def _(j):
            spans = [area(a, kind, j) for a in range(3)]
            grad_sum = g1[:, pl.ds(pl.multiple_of(j * 768, 768), 768)] if kind == 0 else g2[pl.ds(pl.multiple_of(j * SUB, SUB), SUB), :]
            master = mb[spans[0], :]
            mom, var, upd = moments(grad_sum, dxacc[spans[0], :], master, dxacc[spans[1], :], dxacc[spans[2], :])
            dxacc[spans[0], :] = upd
            dxacc[spans[1], :] = mom
            dxacc[spans[2], :] = var
            for i, val in enumerate((master, upd)):
                folded = jnp.sum((val * val).reshape(-1, 8, 768), axis=0)
                lanes = folded[:, 0:128]
                for b in range(1, 6):
                    lanes = lanes + folded[:, b * 128:(b + 1) * 128]
                sqb[layer, kind, i] += lanes

        for i in range(2):
            smine[layer, kind, i:i + 1, :] = jnp.sum(sqb[layer, kind, i], axis=0, keepdims=True)
        run(sum_copies(layer, kind))
        run(lamb_outs(layer, (kind,), (1, 2)))

    def sum_copies(layer, kind):
        return [pltpu.make_async_remote_copy(src_ref=smine.at[layer, kind], dst_ref=sgot.at[layer, kind, i], send_sem=x_snd.at[layer, kind, i], recv_sem=x_rcv.at[layer, kind, i], device_id=(dev,), device_id_type=MESH) for i, dev in enumerate(others)]

    def lamb_apply(layer, kind):
        sgot[layer, kind, 7] = smine[layer, kind]
        settle(sum_copies(layer, kind))
        total = sgot[layer, kind, lax.rem(me + 7, 8)]
        for dev in range(1, 8):
            total = total + sgot[layer, kind, lax.rem(me + 7 - dev + 8, 8)]
        tot[...] = jnp.broadcast_to(jnp.sum(total, axis=1, keepdims=True), (8, 128))
        scale = LEARN_RATE * jnp.sqrt(tot[0:1, 0:1] / tot[1:2, 0:1])

        @pl.loop(0, 4 - kind)
        def _(j):
            span = area(0, kind, j)
            new = mb[span, :] - scale * dxacc[span, :]
            mb[span, :] = new
            half = new.astype(BF16)
            if kind == 1:
                if layer == 1:
                    ws2[j] = half
                else:
                    w2b[j, c, y, x] = half
            else:
                for cc in range(2):
                    lanes = pl.ds(pl.multiple_of((cc * 4 + j) * SUB, SUB), SUB)
                    for k in range(3):
                        piece = half[:, cc * 384 + k * SUB:cc * 384 + (k + 1) * SUB]
                        if layer == 1:
                            ws1[k, :, lanes] = piece
                        else:
                            w1b[k, y, x, c, :, lanes] = piece

        run(lamb_outs(layer, (kind,), (0,)))

    def remote_copy(src, dst, s_sem, r_sem, dev):
        return pltpu.make_async_remote_copy(src_ref=src, dst_ref=dst, send_sem=s_sem, recv_sem=r_sem, device_id=(dev,), device_id_type=MESH)

    def gather_local():
        return pltpu.make_async_copy(ws1, wg1.at[:, y, x, c], ld_sem.at[4])

    def gather2_local():
        return pltpu.make_async_copy(ws2, wg2.at[:, c, y, x], ld_sem.at[5])

    groups = {0: 1, 1: 1, 2: 2, 3: 2, 6: 1, 7: 1, 8: 1, 9: 3}

    def piece_parts(m, name):
        if name in ('s1', 'd1'):
            if m not in groups:
                return ()
            span = pl.ds(m // 2 if m < 6 else m % 3, groups[m])
            if m > 8 or (m < 6 and m % 2 == 0):
                ref, h = (w1b if m < 6 else wg1).at[span, y, x, c], 48
            else:
                ref, h = (w2b if m < 6 else wg2).at[span, c, y, x], 64
            if name == 'd1':
                return (remote_copy(ref, ref, b_snd.at[m, 4], b_rcv.at[m, 4], partner),)
            lower, upper = ref.at[:, pl.ds(0, h)], ref.at[:, pl.ds(h, h)]
            return remote_copy(lower, lower, b_snd.at[m, 0], b_rcv.at[m, 0], xn), remote_copy(upper, upper, b_snd.at[m, 1], b_rcv.at[m, 1], yn)
        if m > 8 or (m < 6 and m % 2 == 0):
            ref = w1b.at[m // 2] if m < 6 else wg1.at[m - 9]
            h = 48

            def blk(yy, xx, rows):
                return ref.at[yy, xx, c, rows]
        else:
            ref = w2b.at[m // 2] if m < 6 else wg2.at[m - 6]
            h = 64

            def blk(yy, xx, rows):
                return ref.at[c, yy, xx, rows]
        first, last, both = pl.ds(0, h), pl.ds(h, h), slice(None)

        def go(part, i, dev):
            return remote_copy(part, part, b_snd.at[m, i], b_rcv.at[m, i], dev)
        if name == 's2':
            return go(blk(y, both, first), 2, yn), go(blk(both, x, last), 3, xn)
        if name == 'd2':
            return go(blk(y, 1 - x, first), 5, partner), go(blk(1 - y, x, last), 6, partner)
        return go(blk(1 - y, both, first), 7, partner), go(blk(both, 1 - x, last), 8, partner)

    def first(m):
        run(piece_parts(m, 's1'))
        run(piece_parts(m, 'd1'))

    def second(m):
        settle(piece_parts(m, 's1'))
        run(piece_parts(m, 's2'))
        run(piece_parts(m, 'd2'))

    def third(m):
        settle(piece_parts(m, 's2'))
        run(piece_parts(m, 'd3'))

    def done(m):
        for name in ('d1', 'd2', 'd3'):
            settle(piece_parts(m, name))

    units = ((p1, r01, r1a1, r1b1, r2a1, r2b1, 48), (p2, r02, r1a2, r1b2, r2a2, r2b2, 64))

    def remote(src, dst, u, slot, stage, dev):
        return pltpu.make_async_remote_copy(src_ref=src, dst_ref=dst, send_sem=snd.at[u, slot, stage], recv_sem=rcv.at[u, slot, stage], device_id=(dev,), device_id_type=MESH)

    def s0(u, slot):
        p, r0, r1a, r1b, r2a, r2b, hr = units[u]
        return remote(p.at[slot, 1 - c], r0.at[slot], u, slot, 0, partner)

    def s1(u, slot):
        p, r0, r1a, r1b, r2a, r2b, hr = units[u]
        return (remote(p.at[slot, c, :, 1 - x, pl.ds(0, hr)], r1a.at[slot], u, slot, 1, xn),
                remote(p.at[slot, c, 1 - y, :, pl.ds(hr, hr)], r1b.at[slot], u, slot, 2, yn))

    def s2(u, slot):
        p, r0, r1a, r1b, r2a, r2b, hr = units[u]
        return (remote(p.at[slot, c, 1 - y, x, pl.ds(0, hr)], r2a.at[slot], u, slot, 3, yn),
                remote(p.at[slot, c, y, 1 - x, pl.ds(hr, hr)], r2b.at[slot], u, slot, 4, xn))

    def start_s0(u, slot):
        s0(u, slot).start()

    def to_s1(u, slot):
        p, r0, r1a, r1b, r2a, r2b, hr = units[u]
        s0(u, slot).wait()

        @pl.loop(0, 2)
        def _(yy):
            for xx in range(2):
                p[slot, c, yy, xx] = (p[slot, c, yy, xx].astype(F32) + r0[slot, yy, xx].astype(F32)).astype(BF16)

        for cp in s1(u, slot):
            cp.start()

    def to_s2(u, slot):
        p, r0, r1a, r1b, r2a, r2b, hr = units[u]
        ca, cb = s1(u, slot)
        ca.wait()
        for i in range(2):
            p[slot, c, i, x, 0:hr] = (p[slot, c, i, x, 0:hr].astype(F32) + r1a[slot, i].astype(F32)).astype(BF16)
        cb.wait()
        for i in range(2):
            p[slot, c, y, i, hr:2 * hr] = (p[slot, c, y, i, hr:2 * hr].astype(F32) + r1b[slot, i].astype(F32)).astype(BF16)
        for cp in s2(u, slot):
            cp.start()

    def finish(u, slot, g):
        p, r0, r1a, r1b, r2a, r2b, hr = units[u]
        k = g % 3
        ca, cb = s2(u, slot)
        for half, (cp, r2) in enumerate(((ca, r2a), (cb, r2b))):
            cp.wait()
            rows = slice(half * hr, half * hr + hr)
            total = p[slot, c, y, x, rows].astype(F32) + r2[slot].astype(F32)
            if u == 1:
                g2[pl.ds(pl.multiple_of(k * SUB + half * hr, 64), hr), :] = total
            else:
                for cc in range(2):
                    for q in range(4):
                        i = cc * 4 + q
                        g1[rows, column(q, cc, k)] = total[:, i * SUB:(i + 1) * SUB]

    settle(loads[:2])

    @pl.loop(0, 6)
    def _(g):
        slot = g % 2
        prev = 1 - slot
        layer = 1 - g // 3
        k = g % 3
        settle(w_copies(g))

        @pl.when(g < 5)
        def _():
            run(w_copies(g + 1))

        @pl.when(g == 1)
        def _():
            loads[2].start()

        @pl.when(g == 3)
        def _():
            loads[2].wait()
            loads[3].start()
            run(lamb_loads(1))

        @pl.when(g == 5)
        def _():
            settle(lamb_outs(1, (0, 1), (0, 1, 2)))
            run(lamb_loads(0))

        def tile(rows):
            xv = xb[layer, rows, :]
            dyv = dyb[rows, :]
            xt[:, rows] = xv.T
            for n in range(CH // 256):
                cs = slice(n * 256, n * 256 + 256)
                h = dot(xv, w1b[k, :, :, :, :, cs].reshape(D, 256))
                da = dot(dyv, w2b[k, n // 2, n % 2].reshape(256, D), NT_DIMS)
                sq = h * h
                s = 0.5 * jnp.tanh(h * (C0 + C1 * sq)) + 0.5
                a = h * s
                gp = s + a * (1.0 - s) * (2.0 * C0 + (6.0 * C1) * sq)
                at[cs, rows] = a.astype(BF16).T
                dhb[rows, cs] = (da * gp).astype(BF16)

        def token_loop(with_dx):
            @pl.loop(0, TOK // (4 * TT))
            def _(t):
                @pl.when((g > 0) & (t == 1))
                def _():
                    to_s1(1, prev)

                if not with_dx:
                    @pl.when((g == 5) & (t == 1))
                    def _():
                        second(9)

                    @pl.when((g == 4) & (t == 1))
                    def _():
                        lamb_apply(1, 0)
                        gather_local().start()
                        lamb_apply(1, 1)
                        gather2_local().start()

                base = pl.multiple_of(t * (4 * TT), 4 * TT)
                spans = [pl.ds(base + i * TT, TT) for i in range(4)]
                for rows in spans:
                    tile(rows)
                if with_dx:
                    for rows in spans:
                        dxacc[rows, :] += dot(dhb[rows, :], w1b[k].reshape(D, CH), NT_DIMS)

        @pl.when(layer == 1)
        def _():
            @pl.when(k == 0)
            def _():
                @pl.loop(0, TOK // 128)
                def _(t):
                    rows = pl.ds(pl.multiple_of(t * 128, 128), 128)
                    dxacc[rows, :] = dyb[rows, :].astype(F32)

            token_loop(True)

        @pl.when(layer == 0)
        def _():
            token_loop(False)

        @pl.when(g > 0)
        def _():
            to_s2(0, prev)

        for n in range(CH // 256):
            if n == 2:
                @pl.when(g > 0)
                def _():
                    to_s2(1, prev)

                @pl.when(g == 4)
                def _():
                    gather_local().wait()
                    gather2_local().wait()
                    first(9)

            fs = slice(n * 256, n * 256 + 256)
            res = dot(xt[...], dhb[:, fs]).astype(BF16)
            for b in range(8):
                p1[slot, b % 2, b // 4, (b // 2) % 2, :, fs] = res[b * 96:(b + 1) * 96]

        start_s0(0, slot)

        for n in range(CH // 256):
            res = dot(at[n * 256:n * 256 + 256, :], dyb[...]).astype(BF16)
            p2[slot, n // 2, n % 2] = res.reshape(2, SUB, D)

        to_s1(0, slot)
        start_s0(1, slot)

        @pl.when(g > 0)
        def _():
            finish(0, prev, g - 1)
            finish(1, prev, g - 1)

        @pl.when(g == 2)
        def _():
            @pl.loop(0, TOK // TT)
            def _(t):
                rows = pl.ds(pl.multiple_of(t * TT, TT), TT)
                dyb[rows, :] = dxacc[rows, :].astype(BF16)

        @pl.when(g == 3)
        def _():
            settle(lamb_loads(1))
            lamb_moments(1, 0)
            lamb_moments(1, 1)

    to_s1(1, 1)
    to_s2(0, 1)
    to_s2(1, 1)
    first(6)
    settle(lamb_loads(0))
    finish(0, 1, 5)
    lamb_moments(0, 0)
    finish(1, 1, 5)
    lamb_moments(0, 1)
    lamb_apply(0, 0)
    first(0)
    lamb_apply(0, 1)
    first(1)
    second(0)
    first(2)
    second(1)
    first(3)
    third(0)
    second(2)
    third(9)
    loads[3].wait()
    settle(lamb_outs(0, (0, 1), (1, 2)))
    third(1)
    done(0)
    done(1)

    def chunk_load(k, kind):
        if kind == 0:
            return pltpu.make_async_copy(wg1.at[k], w1b.at[k], f_sem.at[k, 0])
        return pltpu.make_async_copy(wg2.at[k], w2b.at[k], f_sem.at[k, 1])

    def out_copy(t):
        rows = pl.ds(pl.multiple_of(t * 512, 512), 512)
        return pltpu.make_async_copy(dyb.at[rows, :], out.at[rows, :], out_sem.at[t])

    def load(k, kind):
        done(9 + k if kind == 0 else 6 + k)
        chunk_load(k, kind).start()

    def ready(k):
        chunk_load(k, 0).wait()
        chunk_load(k, 1).wait()

    def before_1():
        second(5)
        first(7)
        third(3)
        done(2)
        done(3)
        load(0, 0)

    def before_2():
        third(5)
        done(4)
        done(5)
        second(7)
        first(8)
        second(11)

    def before_3():
        load(0, 1)
        third(10)
        ready(0)

    def before_4():
        third(11)
        ready(1)

    def before_5():
        ready(2)

    def f1_t1():
        third(4)
        second(6)

    def f3_t3():
        second(8)
        load(1, 1)

    hooks = {
        (0, 0): lambda: second(3),
        (0, 1): lambda: second(4),
        (0, 3): lambda: third(2),
        (1, 1): f1_t1,
        (1, 2): lambda: second(10),
        (2, 2): lambda: third(6),
        (3, 1): lambda: third(7),
        (3, 2): lambda: load(1, 0),
        (3, 3): f3_t3,
        (4, 1): lambda: load(2, 0),
        (4, 2): lambda: third(8),
        (4, 3): lambda: load(2, 1),
    }

    @pl.loop(0, 6)
    def _(f):
        k = f % 3
        for i, fn in enumerate((before_1, before_2, before_3, before_4, before_5)):
            pl.when(f == i + 1)(fn)

        @pl.when(k == 0)
        def _():
            @pl.loop(0, TOK // 128)
            def _(t):
                rows = pl.ds(pl.multiple_of(t * 128, 128), 128)
                dxacc[rows, :] = xb[1, rows, :].astype(F32)

        @pl.loop(0, TOK // (2 * TT))
        def _(t):
            for (hf, ht), fn in hooks.items():
                pl.when((f == hf) & (t == ht))(fn)
            base = pl.multiple_of(t * (2 * TT), 2 * TT)
            spans = [pl.ds(base + i * TT, TT) for i in range(2)]
            for rows in spans:
                xv = xb[1, rows, :]
                for n in range(CH // 256):
                    cs = slice(n * 256, n * 256 + 256)
                    h = dot(xv, w1b[k, :, :, :, :, cs].reshape(D, 256))
                    s = 0.5 * jnp.tanh(h * (C0 + C1 * (h * h))) + 0.5
                    dhb[rows, cs] = (h * s).astype(BF16)
            for rows in spans:
                dxacc[rows, :] += dot(dhb[rows, :], w2b[k].reshape(CH, D))

            pair = pl.ds(base, 2 * TT)

            @pl.when(f == 2)
            def _():
                xb[1, pair, :] = dxacc[pair, :].astype(BF16)

            @pl.when(f == 5)
            def _():
                dyb[pair, :] = dxacc[pair, :].astype(BF16)
                out_copy(t).start()

    settle(lamb_outs(0, (0, 1), (0,)))
    for t in range(4):
        out_copy(t).wait()


def run_step(*args):
    any_spec = pl.BlockSpec(memory_space=pl.ANY)
    vm = pltpu.VMEM
    dma = pltpu.SemaphoreType.DMA
    up, down = jax.ShapeDtypeStruct((2, 96, FF), F32), jax.ShapeDtypeStruct((2, 384, D), F32)
    return pl.pallas_call(
        step_kernel,
        out_shape=(up, down, up, down, up, down, jax.ShapeDtypeStruct((TOK, D), BF16),
                   jax.ShapeDtypeStruct((3, 2, 2, 2, 96, CH), BF16), jax.ShapeDtypeStruct((3, 2, 2, 2, SUB, D), BF16)),
        in_specs=[any_spec] * 13,
        out_specs=(any_spec,) * 9,
        scratch_shapes=[
            vm((2, TOK, D), BF16), vm((TOK, D), BF16), vm((D, TOK), BF16), vm((3 * 768, D), F32),
            vm((3, 2, 2, 2, 96, CH), BF16), vm((3, 2, 2, 2, SUB, D), BF16), vm((CH, TOK), BF16), vm((TOK, CH), BF16),
            vm((2, 2, 2, 2, 96, CH), BF16), vm((2, 2, 2, 2, SUB, D), BF16),
            vm((2, 2, 2, 96, CH), BF16), vm((2, 2, 2, SUB, D), BF16),
            vm((2, 2, 48, CH), BF16), vm((2, 2, 48, CH), BF16), vm((2, 2, 64, D), BF16), vm((2, 2, 64, D), BF16),
            vm((2, 48, CH), BF16), vm((2, 48, CH), BF16), vm((2, 64, D), BF16), vm((2, 64, D), BF16),
            vm((96, FF), F32), vm((384, D), F32), vm((768, 768), F32), vm((2, 2, 2, 8, 128), F32), vm((2, 2, 8, 128), F32), vm((2, 2, 8, 8, 128), F32), vm((8, 128), F32),
            vm((3, 96, CH), BF16), vm((3, SUB, D), BF16),
            dma((6,)), dma((3, 10)), dma((2, 2, 5)), dma((2, 2, 5)), dma((4, 5)), dma((3, 5)),
            dma((2, 2, 7)), dma((2, 2, 7)), dma((12, 9)), dma((12, 9)), dma((3, 2)), dma((4,)),
        ],
        compiler_params=pltpu.CompilerParams(collective_id=0, has_side_effects=True, vmem_limit_bytes=VMEM_MAX),
        name='step',
    )(*args)


def copy_kernel(*refs):
    src, dst, buf, (sem_in, sem_out) = refs[:7], refs[7:14], refs[14:21], refs[21:]
    order = [(a, i) for i in range(2) for a in range(7)]

    def part(ref, a, i):
        return ref.at[pl.ds(i * (TOK // 2), TOK // 2)] if a == 6 else ref.at[i]

    ins = [pltpu.make_async_copy(part(src[a], a, i), part(buf[a], a, i), sem_in.at[a, i]) for a, i in order]
    outs = [pltpu.make_async_copy(part(buf[a], a, i), part(dst[a], a, i), sem_out.at[a, i]) for a, i in order]
    for cp in ins:
        cp.start()
    for cp, nxt in zip(ins, outs):
        cp.wait()
        nxt.start()
    for cp in outs:
        cp.wait()


def run_copy(arrays):
    any_spec = pl.BlockSpec(memory_space=pl.ANY)
    return pl.pallas_call(
        copy_kernel,
        out_shape=tuple(jax.ShapeDtypeStruct(a.shape, a.dtype) for a in arrays),
        in_specs=[any_spec] * 7,
        out_specs=(any_spec,) * 7,
        scratch_shapes=[pltpu.VMEM(a.shape, a.dtype) for a in arrays] + [pltpu.SemaphoreType.DMA((7, 2)), pltpu.SemaphoreType.DMA((7, 2))],
        compiler_params=pltpu.CompilerParams(vmem_limit_bytes=VMEM_MAX),
        name='copy_out',
    )(*arrays)


def solution(mesh):
    shard_rows = P(None, 'fsdp')
    shard_batch = P('fsdp')
    spec_whole = P()

    def local_step(x_layers, dy_top, x_next, w_up, w_down, acc_up, acc_down, master_up, master_down, mom_up, mom_down, var_up, var_down):
        res = run_step(x_layers.reshape(2, TOK, D), dy_top.reshape(TOK, D), x_next.reshape(TOK, D),
                       w_up.reshape(2, 2, 2, 2, 96, FF), w_down.reshape(2, 2, 2, 2, 3, SUB, D),
                       acc_up, acc_down, master_up, master_down, mom_up, mom_down, var_up, var_down)
        res = run_copy(res[:7])
        return tuple(res[:6]) + (res[6].reshape(1, TOK, D),)

    return jax.shard_map(local_step, mesh=mesh, in_specs=(shard_rows, shard_batch, shard_batch, spec_whole, spec_whole) + (shard_rows,) * 8, out_specs=(shard_rows,) * 6 + (shard_batch,), check_vma=False)
```
